32 devices in a mesh: grp: 2 (over y), kvp: 4 (over x, core), tp: 4 (over z).
Axes of the slice: x: 2, y: 2, z: 4, core: 2. Of those that a mesh axis runs over, the one named last changes fastest.
Arguments:
- hidden_in: bfloat16 [16, 7168], P('grp'), parts along dimension 0, may hold values from -3 to 3
- queries_nope: bfloat16 [16, 128, 128], P('grp', ('kvp', 'tp')), parts along dimension 0, may hold values from -6 to 6
- queries_rope: bfloat16 [16, 128, 64], P('grp', ('kvp', 'tp')), parts along dimension 0, may hold values from -26 to 26
- cache: bfloat16 [16, 1536, 576], P('grp', 'kvp'), parts along dimension 0, may hold values from -20 to 20
- lengths: int32 [16], P('grp'), parts along dimension 0, may hold values from 128 to 1536, as said below
- w_uk: bfloat16 [128, 128, 512], P(('kvp', 'tp')), may hold values from -0.5 to 0.5
- w_uv: bfloat16 [128, 512, 128], P(('kvp', 'tp')), may hold values from -0.25 to 0.25
- w_out: bfloat16 [16384, 7168], P(('kvp', 'tp')), may hold values from -0.0625 to 0.0625
- norm_gain: float32 [7168], replicated, may hold values from 0.25 to 1.75
- w_gate: bfloat16 [7168, 18432], P(None, ('kvp', 'tp')), may hold values from -0.0625 to 0.0625
- w_up: bfloat16 [7168, 18432], P(None, ('kvp', 'tp')), may hold values from -0.0625 to 0.0625
- w_down: bfloat16 [18432, 7168], P(('kvp', 'tp')), may hold values from -0.0625 to 0.0625
Outputs:
- layer_out: bfloat16 [16, 7168], P('grp', ('kvp', 'tp')), parts along dimension 0
The draws below stay inside these ranges and needn't reach their ends.
There are 2 independent parts, one for each index of `grp`. The reference program is written for one: setup_inputs(seed, part) draws one part's arguments, and reference() takes and returns one part's arrays. A program takes and returns all parts, laid end to end along the dimension named above; an argument that names none is the same for every part. Nothing has to cross between parts.
Inputs may be any that keep to these rules, and one draw needn't show every extreme that they name: `lengths`: every length is a multiple of 128; in every draw some request has the full 1536.
All inputs are finite; a program needn't handle non-finite values.
Results may differ from the reference program's by a relative error of at most 0.04.
Values may be sent and summed in bfloat16 or wider, within the bound.
A program may use at most 128 MiB of HBM per device.

```python
import jax
import jax.numpy as jnp
from jax import lax

D = 7168
FF = 18432
H = 128
LAT = 512
ROPE = 64
HEAD_DIM = 128
BATCH = 8
BLOCK = 128
CTX_DEV = 384
CTX = 1536
N_KVP = 4


def draw_lengths(key, part):
    count_blocks = CTX // BLOCK
    counts = jax.random.randint(key, (BATCH,), 1, count_blocks + 1)
    full_row = jax.random.randint(jax.random.fold_in(key, 3), (), 0, BATCH)
    counts = jnp.where(jnp.arange(BATCH) == full_row, count_blocks, counts)
    return (counts * BLOCK).astype(jnp.int32)


def draw_cache(key, part):
    values = jnp.clip(jax.random.normal(jax.random.fold_in(key, 11), (BATCH, CTX, LAT + ROPE), jnp.float32), -6.0, 6.0)
    return values.astype(jnp.bfloat16)


def draw_queries_rope(key, part):
    values = jnp.clip(jax.random.normal(jax.random.fold_in(key, 21), (BATCH, H, ROPE), jnp.float32), -6.0, 6.0)
    return values.astype(jnp.bfloat16)


def strengthened(drawn, key, source, target, shards_of, factor):
    def block_of(position):
        return (jnp.arange(drawn.shape[position]) // (drawn.shape[position] // shards_of)).reshape((-1,) + (1,) * (drawn.ndim - 1 - position))

    first = jax.random.permutation(key, shards_of)[block_of(target)]
    far = (block_of(target) + shards_of // 2) % shards_of
    return jnp.where((block_of(source) == first) | (block_of(source) == far), factor * drawn, drawn)


def block_scale(own_key, shape, pieces, smallest, largest):
    level = 1.0
    for position, shards_of in pieces:
        heights = jax.random.uniform(jax.random.fold_in(jax.random.fold_in(own_key, 6), position), (shards_of,), jnp.float32, smallest / len(pieces), largest / len(pieces))
        level = level * jnp.repeat(jnp.exp(heights), shape[position] // shards_of).reshape((-1,) + (1,) * (len(shape) - 1 - position))
    return level


def centred(own_key, extent, scale, most, shards=(), kind=jnp.bfloat16):
    result = jax.random.normal(own_key, extent, jnp.float32) * scale
    if len(shards) > 0:
        result = block_scale(own_key, extent, shards, -0.22, 0.18) * result
    return jnp.clip(result, min=-most, max=most).astype(kind)


def heavy_noise(own_key, extent, deviation, bound, cuts, heavy, kind=jnp.bfloat16):
    entries = deviation * jax.random.normal(own_key, extent, jnp.float32)
    if cuts:
        entries = entries * block_scale(own_key, extent, cuts, -0.22, 0.18)
    return jnp.clip(strengthened(entries, jax.random.fold_in(own_key, 3), *heavy), -bound, bound).astype(kind)


def setup_inputs(seed: int = 0, part: int = 0) -> dict:
    key_of = jax.random.split(jax.random.key(seed), 13)
    own_keys = jax.random.split(jax.random.fold_in(key_of[12], part), 13)
    hidden_in = centred(own_keys[0], (BATCH, D), 0.5, 3.0)
    queries_nope = centred(own_keys[1], (BATCH, H, HEAD_DIM), 1.0, 6.0, ((1, 16),))
    queries_rope = draw_queries_rope(jax.random.fold_in(jax.random.fold_in(key_of[12], part), 71), part)
    cache = draw_cache(jax.random.fold_in(jax.random.fold_in(key_of[12], part), 71), part)
    lengths = draw_lengths(jax.random.fold_in(jax.random.fold_in(key_of[12], part), 71), part)
    w_uk = centred(key_of[5], (H, HEAD_DIM, LAT), HEAD_DIM ** -0.5, 0.5, ((0, 16),))
    w_uv = centred(key_of[6], (H, LAT, HEAD_DIM), LAT ** -0.5, 0.25, ((0, 16),))
    w_out = heavy_noise(key_of[7], (H * HEAD_DIM, D), (H * HEAD_DIM) ** -0.5, 0.0625, ((0, 16),), (0, 1, 16, 2.0))
    norm_gain = jnp.clip(1.0 + 0.15 * jax.random.normal(key_of[8], (D,), jnp.float32), 0.25, 1.75)
    w_gate = centred(key_of[9], (D, FF), D ** -0.5, 0.0625, ((1, 16),))
    w_up = centred(key_of[10], (D, FF), D ** -0.5, 0.0625, ((1, 16),))
    w_down = heavy_noise(key_of[11], (FF, D), FF ** -0.5, 0.0625, ((0, 16),), (0, 1, 16, 2.0))
    return {"hidden_in": hidden_in, "queries_nope": queries_nope, "queries_rope": queries_rope, "cache": cache, "lengths": lengths, "w_uk": w_uk, "w_uv": w_uv, "w_out": w_out, "norm_gain": norm_gain, "w_gate": w_gate, "w_up": w_up, "w_down": w_down}


def reference(hidden_in, queries_nope, queries_rope, cache, lengths, w_uk, w_uv, w_out, norm_gain, w_gate, w_up, w_down):
    score_scale = float(HEAD_DIM + ROPE) ** (-0.5)
    q_lat = jnp.einsum('bhd,hdl->bhl', queries_nope.astype(jnp.float32), w_uk.astype(jnp.float32)).astype(jnp.bfloat16)
    q_full = jnp.concatenate([q_lat, queries_rope], axis=2).astype(jnp.float32)
    cache_wide = cache.astype(jnp.float32)
    scores = jnp.einsum('bhc,btc->bht', q_full, cache_wide) * score_scale
    visible = jnp.arange(CTX, dtype=jnp.int32)[None, :] < lengths[:, None]
    visible = jnp.broadcast_to(visible[:, None, :], scores.shape).reshape(BATCH, H, N_KVP, CTX_DEV)
    blocks = scores.reshape(BATCH, H, N_KVP, CTX_DEV)
    masked = jnp.where(visible, blocks, jnp.float32(-1e+30))
    block_max = lax.optimization_barrier(jnp.max(masked, axis=3))
    exponent = jnp.where(visible, jnp.exp(masked - block_max[..., None]), jnp.float32(0.0))
    block_sum = lax.optimization_barrier(jnp.sum(exponent, axis=3))
    guarded = jnp.maximum(block_sum, 1.0)
    log_total = block_max + jnp.log(guarded)
    weights = (exponent / guarded[..., None]).astype(jnp.bfloat16)
    cache_blocks = cache_wide.reshape(BATCH, N_KVP, CTX_DEV, LAT + ROPE)
    partial_value = jnp.einsum('bhkt,bktc->bhkc', weights.astype(jnp.float32), cache_blocks)[..., :LAT]
    highest = lax.optimization_barrier(jnp.max(log_total, axis=2))
    overall = highest + jnp.log(lax.optimization_barrier(jnp.sum(jnp.exp(log_total - highest[..., None]), axis=2)))
    o_lat = lax.optimization_barrier(jnp.sum(jnp.exp(log_total - overall[..., None])[..., None] * partial_value, axis=2)).astype(jnp.bfloat16)
    head_out = jnp.einsum('bhl,hle->bhe', o_lat.astype(jnp.float32), w_uv.astype(jnp.float32)).astype(jnp.bfloat16)
    attention = jnp.dot(head_out.reshape(BATCH, H * HEAD_DIM), w_out, preferred_element_type=jnp.float32)
    residual = hidden_in.astype(jnp.float32) + attention
    mean_square = lax.optimization_barrier(jnp.mean(residual * residual, axis=1))
    normed = (residual * lax.rsqrt(mean_square + 1e-06)[:, None] * norm_gain.astype(jnp.float32)[None, :]).astype(jnp.bfloat16)
    gate_proj = jnp.dot(normed, w_gate, preferred_element_type=jnp.float32)
    up_proj = jnp.dot(normed, w_up, preferred_element_type=jnp.float32)
    act = (jax.nn.silu(gate_proj) * up_proj).astype(jnp.bfloat16)
    ffn_out = jnp.dot(act, w_down, preferred_element_type=jnp.float32)
    return (residual + ffn_out).astype(jnp.bfloat16)
```

```python
import functools

import jax
import jax.numpy as jnp
from jax import lax
from jax.experimental import pallas as pl
from jax.experimental.pallas import tpu as pltpu
from jax.sharding import PartitionSpec as P


def project(o_lat, w_uv, w_out):
    head_out = jnp.einsum("bhl,hle->bhe", o_lat, w_uv, preferred_element_type=jnp.float32).astype(
        jnp.bfloat16
    )
    return jnp.dot(
        head_out.reshape(head_out.shape[0], -1), w_out, preferred_element_type=jnp.float32
    )


def plain_device(
    hidden_in,
    queries_nope,
    queries_rope,
    cache,
    lengths,
    w_uk,
    w_uv,
    w_out,
    norm_gain,
    w_gate,
    w_up,
    w_down,
):
    batch, heads_dev, head_dim = queries_nope.shape
    latent = w_uk.shape[2]
    ctx_dev = cache.shape[1]
    groups = lax.axis_size("kvp")
    score_scale = float(head_dim + queries_rope.shape[2]) ** (-0.5)
    q_lat = jnp.einsum(
        "bhd,hdl->bhl", queries_nope, w_uk, preferred_element_type=jnp.float32
    ).astype(jnp.bfloat16)
    q_lat_all, rope_all = (
        lax.all_gather(q_lat, "kvp", axis=1, tiled=True),
        lax.all_gather(queries_rope, "kvp", axis=1, tiled=True),
    )
    q_full = jnp.concatenate([q_lat_all, rope_all], axis=2)
    scores = (
        jnp.einsum("bhc,btc->bht", q_full, cache, preferred_element_type=jnp.float32) * score_scale
    )
    offset = lax.axis_index("kvp") * ctx_dev
    visible = ((offset + jnp.arange(ctx_dev, dtype=jnp.int32))[None, :] < lengths[:, None])[
        :, None, :
    ]
    masked = jnp.where(visible, scores, jnp.float32(-1e30))
    block_max = jnp.max(masked, axis=2)
    exponent = jnp.where(visible, jnp.exp(masked - block_max[..., None]), jnp.float32(0.0))
    guarded = jnp.maximum(jnp.sum(exponent, axis=2), 1.0)
    log_total = block_max + jnp.log(guarded)
    weights = (exponent / guarded[..., None]).astype(jnp.bfloat16)
    partial_value = jnp.einsum("bht,btc->bhc", weights, cache, preferred_element_type=jnp.float32)[
        ..., :latent
    ]
    blocks = partial_value.reshape(batch, groups, heads_dev, latent)
    block_logs = log_total.reshape(batch, groups, heads_dev)
    part_blocks = lax.all_to_all(
        blocks.astype(jnp.bfloat16), "kvp", split_axis=1, concat_axis=1, tiled=True
    ).astype(blocks.dtype)
    part_logs = lax.all_to_all(block_logs, "kvp", split_axis=1, concat_axis=1, tiled=True)
    highest = jnp.max(part_logs, axis=1)
    overall = highest + jnp.log(jnp.sum(jnp.exp(part_logs - highest[:, None, :]), axis=1))
    scaled = jnp.exp(part_logs - overall[:, None, :])[..., None] * part_blocks
    o_lat = jnp.sum(scaled, axis=1).astype(jnp.bfloat16)
    attention = project(o_lat, w_uv, w_out)
    model_width = norm_gain.shape[0]
    share_width = model_width // lax.axis_size(("kvp", "tp"))
    share_start = lax.axis_index(("kvp", "tp")) * share_width
    attn_whole = lax.psum(attention, ("kvp", "tp"))
    residual = hidden_in.astype(jnp.float32) + attn_whole
    mean_square = jnp.mean(residual * residual, axis=1)
    normed = (residual * lax.rsqrt(mean_square + 1e-06)[:, None] * norm_gain[None, :]).astype(
        jnp.bfloat16
    )
    residual_share = lax.dynamic_slice_in_dim(residual, share_start, share_width, 1)
    gate_proj = jnp.dot(normed, w_gate, preferred_element_type=jnp.float32)
    up_proj = jnp.dot(normed, w_up, preferred_element_type=jnp.float32)
    act = (jax.nn.silu(gate_proj) * up_proj).astype(jnp.bfloat16)
    ffn_terms = jnp.dot(act, w_down, preferred_element_type=jnp.float32)
    ffn_share = lax.psum_scatter(ffn_terms, ("kvp", "tp"), scatter_dimension=1, tiled=True)
    return (residual_share + ffn_share).astype(jnp.bfloat16)


MESH = pl.DeviceIdType.MESH
F32 = jnp.float32
BF16 = jnp.bfloat16
VMEM_BYTES = 67043328


SPAN = 4


def layer_kernel(
    groups, tps, share, chunk, out_rows, span,
    hidden_hbm, nope_hbm, rope_hbm, len_hbm, gain_hbm,
    cache_hbm, uk_hbm, uv_hbm, wo_hbm, wg_hbm, wu_hbm, wd_hbm,
    out_ref,
    hidden_v, nope_v, rope_v, len_v, gain_v, gain_s,
    cache_v, uk_v, uv_v, big_v, gu_v,
    nope_s, qlat_s, score_s, weight_s, q_send, q_all, part_send, part_all, log_send, log_all,
    olat_s, head_s, own_s, rs_send, rs_all, ag_send, ag_all, fs_send, fs_all,
    in_sem, uk_sem, cache_sem, uv_sem, wo_sem, gu_sem, wd_sem,
    q_ss, q_rs, part_ss, part_rs, log_ss, log_rs, rs_ss, rs_rs, ag_ss, ag_rs, fs_ss, fs_rs,
):
    count = groups * tps
    kvp = lax.axis_index("kvp")
    tp = lax.axis_index("tp")
    me = kvp * tps + tp
    batch, heads, head_dim = nope_v.shape
    latent = uk_v.shape[2]
    rope = rope_v.shape[2]
    ctx = cache_v.shape[2]
    width = hidden_v.shape[1]
    chunks = width // chunk
    hidden_units = gu_v.shape[1] // 2
    parts = batch // span
    halves = tps // 2
    half = tp // 2
    chips = groups // 2

    def peer(index):
        return {"kvp": index // tps, "tp": lax.rem(index, tps)}

    def target_of(i):
        return lax.rem(kvp // 2 + i // 2, chips) * 2 + lax.rem(kvp + i, 2)

    def source_of(i):
        return lax.rem(kvp // 2 + chips - i // 2, chips) * 2 + lax.rem(kvp + i, 2)

    def owner_tp(h):
        return 2 * h + 1 - (4 * h + 2) // tps

    near = [
        (target_of(i), lax.rem(half + e, halves)) for e in range(halves) for i in range(groups)
    ]
    far = near[::-1]
    mine = kvp * halves + half
    owns = tp == owner_tp(half)

    def load(source, target, sem):
        return pltpu.make_async_copy(source, target, sem)

    def cols(j):
        return pl.ds(pl.multiple_of(j * chunk, 128), chunk)

    def side(t):
        return pl.ds((t % 2) * chunk, chunk)

    def load_wo(t):
        k, h = far[t]
        return load(
            wo_hbm.at[:, cols(k * halves + h)],
            big_v.at[t // 2, pl.ds(0, out_rows), side(t)],
            wo_sem.at[t],
        )

    def load_wd(t):
        k, h = far[t]
        return load(wd_hbm.at[:, cols(k * halves + h)], big_v.at[t // 2, :, side(t)], wd_sem.at[t])

    def load_gu(t, n):
        k, h = near[t]
        return load(
            (wg_hbm, wu_hbm)[n].at[cols(k * halves + h)],
            gu_v.at[pl.ds(t * chunk, chunk), pl.ds(n * hidden_units, hidden_units)],
            gu_sem.at[n, t],
        )

    small = [
        load(nope_hbm, nope_v, in_sem.at[0]),
        load(rope_hbm, rope_v, in_sem.at[1]),
        load(len_hbm, len_v, in_sem.at[2]),
        load(hidden_hbm, hidden_v, in_sem.at[3]),
        load(gain_hbm, gain_v.at[:, pl.ds(0, width)], in_sem.at[4]),
    ]
    uk_load = load(uk_hbm, uk_v, uk_sem)
    cache_load = load(cache_hbm, cache_v, cache_sem)
    uv_load = load(uv_hbm, uv_v, uv_sem)

    barrier = pltpu.get_barrier_semaphore()
    small[0].start()
    uk_load.start()
    small[1].start()

    @pl.loop(1, count)
    def _(d):
        pl.semaphore_signal(
            barrier, inc=1, device_id=peer(lax.rem(me + d, count)), device_id_type=MESH
        )

    cache_load.start()
    for copy in small[2:]:
        copy.start()

    small[0].wait()
    nope_s[...] = nope_v[...].astype(F32)
    small[1].wait()
    base = 2 * latent
    for b in range(batch):
        first = base + (b % 2) * rope
        q_send[b // 2, :, first : first + rope] = rope_v[b]
    uk_load.wait()
    for i in range(heads):
        qlat_s[:, i, :] = jnp.dot(
            nope_s[:, i, :].astype(BF16), uk_v[i], preferred_element_type=F32
        )
    for b in range(batch):
        first = (b % 2) * latent
        q_send[b // 2, :, first : first + latent] = qlat_s[b].astype(BF16)
    pl.semaphore_wait(barrier, count - 1)

    def q_copy(i, u, ahead):
        other = target_of(i) if ahead else source_of(i)
        return pltpu.make_async_remote_copy(
            src_ref=q_send.at[pl.ds(u * span // 2, span // 2)],
            dst_ref=q_all.at[kvp if ahead else other, pl.ds(u * span // 2, span // 2)],
            send_sem=q_ss.at[i, u],
            recv_sem=q_rs.at[kvp if ahead else other, u],
            device_id={"kvp": other, "tp": tp},
            device_id_type=MESH,
        )

    def part_copy(i, u, ahead):
        other = target_of(i) if ahead else source_of(i)
        slot = kvp if ahead else other
        some = pl.ds(u * span, span)
        return pltpu.make_async_remote_copy(
            src_ref=part_send.at[other, some],
            dst_ref=part_all.at[slot, some],
            send_sem=part_ss.at[i, u],
            recv_sem=part_rs.at[slot, u],
            device_id={"kvp": other, "tp": tp},
            device_id_type=MESH,
        )

    def log_copy(i, ahead):
        other = target_of(i) if ahead else source_of(i)
        slot = kvp if ahead else other
        return pltpu.make_async_remote_copy(
            src_ref=log_send.at[other],
            dst_ref=log_all.at[slot],
            send_sem=log_ss.at[i],
            recv_sem=log_rs.at[slot],
            device_id={"kvp": other, "tp": tp},
            device_id_type=MESH,
        )

    outward = list(range(2, groups)) + [1]
    for u in range(parts):
        for i in outward:
            q_copy(i, u, True).start()
    uv_load.start(priority=1)
    for t in range(chunks):
        load_wo(t).start(priority=1)
    for t in range(chunks):
        load_gu(t, 0).start(priority=1)
        load_gu(t, 1).start(priority=1)
    q_all[kvp] = q_send[...]
    for copy in small[2:]:
        copy.wait()
    for j in range(chunks):
        gain_s[j] = jnp.broadcast_to(gain_v[:, j * chunk : (j + 1) * chunk], (batch, chunk))
    cache_load.wait()

    scale = float(head_dim + rope) ** (-0.5)
    rows = groups * heads
    position = kvp * ctx + lax.broadcasted_iota(jnp.int32, (rows, ctx), 1)
    lane = lax.broadcasted_iota(jnp.int32, (rows, 128), 1)
    logs_acc = jnp.zeros((rows, 128), F32)
    lengths = len_v[...]
    for u in range(parts):
        for i in range(1, groups):
            q_copy(i, u, False).wait_recv()
        some = range(u * span, (u + 1) * span)
        for b in some:
            lat = (b % 2) * latent
            rot = base + (b % 2) * rope
            q_lat = q_all[:, b // 2, :, lat : lat + latent].astype(F32).reshape(rows, latent)
            q_rot = q_all[:, b // 2, :, rot : rot + rope].astype(F32).reshape(rows, rope)
            score_s[b] = (
                jnp.dot(q_lat.astype(BF16), cache_v[b, :latent], preferred_element_type=F32)
                + jnp.dot(q_rot.astype(BF16), cache_v[b, latent:], preferred_element_type=F32)
            ) * scale
        for b in some:
            visible = position < lengths[:, b : b + 1]
            masked = jnp.where(visible, score_s[b], F32(-1e30))
            top = jnp.max(masked, axis=1, keepdims=True)
            exps = jnp.where(visible, jnp.exp(masked - top), F32(0.0))
            guarded = jnp.maximum(jnp.sum(exps, axis=1, keepdims=True), 1.0)
            logs_acc = jnp.where(lane == b, top + jnp.log(guarded), logs_acc)
            weight_s[b] = (exps / guarded).astype(BF16)
        for b in some:
            part = lax.dot_general(
                weight_s[b], cache_v[b, :latent], (((1,), (1,)), ((), ())),
                preferred_element_type=F32,
            )
            for g in range(groups):
                part_send[g, b] = part[g * heads : (g + 1) * heads].astype(BF16)
        for i in outward:
            part_copy(i, u, True).start()
    for g in range(groups):
        log_send[g] = logs_acc[g * heads : (g + 1) * heads]
    for i in outward:
        log_copy(i, True).start()
    part_all[kvp] = part_send[kvp]
    log_all[kvp] = log_send[kvp]
    uv_load.wait()
    for t in range(chunks):
        load_wo(t).wait()
    for i in range(1, groups):
        log_copy(i, False).wait_recv()
    logs = [log_all[g] for g in range(groups)]
    highest = functools.reduce(jnp.maximum, logs)
    overall = highest + jnp.log(sum(jnp.exp(x - highest) for x in logs))
    factors = [jnp.exp(x - overall) for x in logs]
    for u in range(parts):
        for i in range(1, groups):
            part_copy(i, u, False).wait_recv()
        for b in range(u * span, (u + 1) * span):
            olat_s[b] = sum(
                factors[g][:, b : b + 1] * part_all[g, b].astype(F32) for g in range(groups)
            )
    for i in range(heads):
        head_s[:, i * head_dim : (i + 1) * head_dim] = jnp.dot(
            olat_s[:, i, :].astype(BF16), uv_v[i], preferred_element_type=F32
        ).astype(BF16)

    def rs_copy(t, slot, k, z):
        return pltpu.make_async_remote_copy(
            src_ref=rs_send.at[t],
            dst_ref=rs_all.at[slot],
            send_sem=rs_ss.at[t],
            recv_sem=rs_rs.at[slot],
            device_id={"kvp": k, "tp": z},
            device_id_type=MESH,
        )

    for s in range(chunks // 2):
        both = jnp.dot(head_s[...], big_v[s, :out_rows], preferred_element_type=F32)
        for t in (2 * s, 2 * s + 1):
            k, h = far[t]
            load_wd(t).start(priority=1)
            term = both[:, (t % 2) * chunk : (t % 2 + 1) * chunk]
            rs_send[t] = term.astype(BF16)
            if t < chunks - 1:
                rs_copy(t, me, k, owner_tp(h)).start()
            else:
                own_s[...] = term

                @pl.when(jnp.logical_not(owns))
                def _():
                    rs_copy(t, me, k, owner_tp(h)).start()

    def ag_copy(d, slot, dest):
        return pltpu.make_async_remote_copy(
            src_ref=ag_send,
            dst_ref=ag_all.at[slot],
            send_sem=ag_ss.at[d],
            recv_sem=ag_rs.at[slot],
            device_id=peer(dest),
            device_id_type=MESH,
        )

    @pl.when(owns)
    def _():
        residual = hidden_v[:, cols(mine)].astype(F32) + own_s[...]
        for d in range(1, count):
            source = lax.rem(me + d, count)
            rs_copy(0, source, source // tps, lax.rem(source, tps)).wait_recv()
        total = residual
        for d in range(1, count):
            total = total + rs_all[lax.rem(me + d, count)].astype(F32)
        ag_send[...] = total.astype(BF16)

        @pl.loop(1, count)
        def _(d):
            ag_copy(d, mine, lax.rem(me + d, count)).start()

        ag_all[mine] = ag_send[...]

    square = jnp.zeros((batch, 1), F32)
    for t in range(chunks):
        load_gu(t, 0).wait()
        load_gu(t, 1).wait()
    products = jnp.zeros((batch, 2 * hidden_units), F32)
    for s in range(chunks // 2):
        x = []
        for t in (2 * s, 2 * s + 1):
            k, h = near[t]
            j = k * halves + h
            if t == 0:
                @pl.when(jnp.logical_not(owns))
                def _():
                    ag_copy(0, j, k * tps + owner_tp(h)).wait_recv()
            else:
                ag_copy(0, j, k * tps + owner_tp(h)).wait_recv()
        for t in (2 * s, 2 * s + 1):
            k, h = near[t]
            j = k * halves + h
            value = ag_all[j].astype(F32)
            square = square + jnp.sum(value * value, axis=1, keepdims=True)
            x.append((value * gain_s[j]).astype(BF16))
        products = products + jnp.dot(
            jnp.concatenate(x, axis=1),
            gu_v[2 * s * chunk : 2 * (s + 1) * chunk],
            preferred_element_type=F32,
        )
    products = products * lax.rsqrt(square / width + 1e-06)
    gate, up = products[:, :hidden_units], products[:, hidden_units:]
    act = (gate / (1.0 + jnp.exp(-gate)) * up).astype(BF16)

    def fs_copy(n, slot, k, z):
        return pltpu.make_async_remote_copy(
            src_ref=fs_send.at[n],
            dst_ref=fs_all.at[slot],
            send_sem=fs_ss.at[n],
            recv_sem=fs_rs.at[slot],
            device_id={"kvp": k, "tp": z},
            device_id_type=MESH,
        )

    pair = ag_all[mine].astype(F32)
    total = jnp.where(lax.rem(tp, 2) == 0, pair[:, :share], pair[:, share:])
    for t in range(chunks):
        load_wd(t).wait()
    for s in range(chunks // 2):
        both = jnp.dot(act, big_v[s], preferred_element_type=F32)
        for n in range(4 * s, 4 * s + 4):
            k, h = far[n // 2]
            p = n % 2
            piece = both[:, (n % 4) * share : (n % 4 + 1) * share]
            fs_send[n] = piece.astype(BF16)
            if n < count - 2:
                fs_copy(n, me, k, 2 * h + p).start()
            else:
                total = total + jnp.where(lax.rem(tp, 2) == p, piece, F32(0.0))

                @pl.when(lax.rem(tp, 2) != p)
                def _():
                    fs_copy(n, me, k, 2 * h + p).start()

    for d in range(1, count):
        source = lax.rem(me + d, count)
        fs_copy(0, source, source // tps, lax.rem(source, tps)).wait_recv()
    for d in range(1, count):
        total = total + fs_all[lax.rem(me + d, count)].astype(F32)
    out_ref[...] = total.astype(BF16)

    for i in range(1, groups):
        for u in range(parts):
            q_copy(i, u, True).wait_send()
            part_copy(i, u, True).wait_send()
        log_copy(i, True).wait_send()
    for t, (k, h) in enumerate(far):
        if t < chunks - 1:
            rs_copy(t, me, k, owner_tp(h)).wait_send()
            fs_copy(2 * t, me, k, 2 * h).wait_send()
            fs_copy(2 * t + 1, me, k, 2 * h + 1).wait_send()
        else:
            @pl.when(jnp.logical_not(owns))
            def _():
                rs_copy(t, me, k, owner_tp(h)).wait_send()

            for p in range(2):
                @pl.when(lax.rem(tp, 2) != p)
                def _():
                    fs_copy(2 * t + p, me, k, 2 * h + p).wait_send()

    @pl.when(owns)
    def _():
        @pl.loop(1, count)
        def _(d):
            ag_copy(d, mine, lax.rem(me + d, count)).wait_send()


def per_device(*operands):
    (hidden_in, queries_nope, queries_rope, cache, lengths, w_uk, w_uv, w_out, norm_gain,
     w_gate, w_up, w_down) = operands
    groups, tps = lax.axis_size("kvp"), lax.axis_size("tp")
    count = groups * tps
    batch, heads, head_dim = queries_nope.shape
    latent, rope, ctx = w_uk.shape[2], queries_rope.shape[2], cache.shape[1]
    width = hidden_in.shape[1]
    share = width // count
    ff = w_gate.shape[1]
    rows = w_out.shape[0]
    chunk = 2 * share
    held = (w_gate.size + w_up.size + max(rows, ff) * width + cache.size + w_uk.size + w_uv.size) * 2
    fits = (
        batch % 8 == 0
        and heads % 8 == 0
        and all(size % 128 == 0 for size in (head_dim, latent, 2 * rope, ctx, chunk, ff))
        and groups % 2 == 0
        and tps % 2 == 0
        and batch <= 128
        and rows <= ff
        and held < VMEM_BYTES - 8 * 2**20
    )
    if not fits:
        return plain_device(*operands)
    chunks = width // chunk
    pairs = batch // 2
    parts = batch // SPAN
    dma = pltpu.SemaphoreType.DMA
    vmem = pl.BlockSpec(memory_space=pltpu.VMEM)
    anywhere = pl.BlockSpec(memory_space=pl.ANY)
    packed = 2 * (latent + rope)
    scratch = [
        pltpu.VMEM((batch, width), BF16),
        pltpu.VMEM((batch, heads, head_dim), BF16),
        pltpu.VMEM((batch, heads, rope), BF16),
        pltpu.VMEM((1, batch), jnp.int32),
        pltpu.VMEM((1, width + 1024), F32),
        pltpu.VMEM((chunks, batch, chunk), F32),
        pltpu.VMEM((batch, latent + rope, ctx), BF16),
        pltpu.VMEM(w_uk.shape, BF16),
        pltpu.VMEM(w_uv.shape, BF16),
        pltpu.VMEM((chunks // 2, ff, 2 * chunk), BF16),
        pltpu.VMEM((width, 2 * ff), BF16),
        pltpu.VMEM((batch, heads, head_dim), F32),
        pltpu.VMEM((batch, heads, latent), F32),
        pltpu.VMEM((batch, groups * heads, ctx), F32),
        pltpu.VMEM((batch, groups * heads, ctx), BF16),
        pltpu.VMEM((pairs, heads, packed), BF16),
        pltpu.VMEM((groups, pairs, heads, packed), BF16),
        pltpu.VMEM((groups, batch, heads, latent), BF16),
        pltpu.VMEM((groups, batch, heads, latent), BF16),
        pltpu.VMEM((groups, heads, 128), F32),
        pltpu.VMEM((groups, heads, 128), F32),
        pltpu.VMEM((batch, heads, latent), F32),
        pltpu.VMEM((batch, heads * head_dim), BF16),
        pltpu.VMEM((batch, chunk), F32),
        pltpu.VMEM((chunks, batch, chunk), BF16),
        pltpu.VMEM((count, batch, chunk), BF16),
        pltpu.VMEM((batch, chunk), BF16),
        pltpu.VMEM((chunks, batch, chunk), BF16),
        pltpu.VMEM((count, batch, share), BF16),
        pltpu.VMEM((count, batch, share), BF16),
        dma((5,)), dma, dma, dma,
        dma((chunks,)), dma((2, chunks)), dma((chunks,)),
        dma((groups, parts)), dma((groups, parts)), dma((groups, parts)), dma((groups, parts)),
        dma((groups,)), dma((groups,)),
        dma((chunks,)), dma((count,)), dma((count,)), dma((chunks,)), dma((count,)), dma((count,)),
    ]
    return pl.pallas_call(
        functools.partial(layer_kernel, groups, tps, share, chunk, rows, SPAN),
        out_shape=jax.ShapeDtypeStruct((batch, share), BF16),
        in_specs=[anywhere] * 12,
        out_specs=vmem,
        scratch_shapes=scratch,
        compiler_params=pltpu.CompilerParams(
            collective_id=0, has_side_effects=True, vmem_limit_bytes=VMEM_BYTES
        ),
    )(
        hidden_in, queries_nope, queries_rope, lengths.reshape(1, batch), norm_gain.reshape(1, width),
        jnp.swapaxes(cache, 1, 2), w_uk, w_uv, w_out, w_gate, w_up, w_down,
    )


def solution(mesh):
    placed = (
        P("grp", None),
        P("grp", ("kvp", "tp"), None),
        P("grp", ("kvp", "tp"), None),
        P("grp", "kvp", None),
        P("grp"),
        P(("kvp", "tp"), None, None),
        P(("kvp", "tp"), None, None),
        P(("kvp", "tp"), None),
        P(),
        P(None, ("kvp", "tp")),
        P(None, ("kvp", "tp")),
        P(("kvp", "tp"), None),
    )
    return jax.shard_map(
        per_device, mesh=mesh, in_specs=placed, out_specs=P("grp", ("kvp", "tp")), check_vma=False
    )
```

```python
import functools

import jax
import jax.numpy as jnp
from jax import lax
from jax.experimental import pallas as pl
from jax.experimental.pallas import tpu as pltpu
from jax.sharding import PartitionSpec as P


def project(o_lat, w_uv, w_out):
    head_out = jnp.einsum("bhl,hle->bhe", o_lat, w_uv, preferred_element_type=jnp.float32).astype(
        jnp.bfloat16
    )
    return jnp.dot(
        head_out.reshape(head_out.shape[0], -1), w_out, preferred_element_type=jnp.float32
    )


def plain_device(
    hidden_in,
    queries_nope,
    queries_rope,
    cache,
    lengths,
    w_uk,
    w_uv,
    w_out,
    norm_gain,
    w_gate,
    w_up,
    w_down,
):
    batch, heads_dev, head_dim = queries_nope.shape
    latent = w_uk.shape[2]
    ctx_dev = cache.shape[1]
    groups = lax.axis_size("kvp")
    score_scale = float(head_dim + queries_rope.shape[2]) ** (-0.5)
    q_lat = jnp.einsum(
        "bhd,hdl->bhl", queries_nope, w_uk, preferred_element_type=jnp.float32
    ).astype(jnp.bfloat16)
    q_lat_all, rope_all = (
        lax.all_gather(q_lat, "kvp", axis=1, tiled=True),
        lax.all_gather(queries_rope, "kvp", axis=1, tiled=True),
    )
    q_full = jnp.concatenate([q_lat_all, rope_all], axis=2)
    scores = (
        jnp.einsum("bhc,btc->bht", q_full, cache, preferred_element_type=jnp.float32) * score_scale
    )
    offset = lax.axis_index("kvp") * ctx_dev
    visible = ((offset + jnp.arange(ctx_dev, dtype=jnp.int32))[None, :] < lengths[:, None])[
        :, None, :
    ]
    masked = jnp.where(visible, scores, jnp.float32(-1e30))
    block_max = jnp.max(masked, axis=2)
    exponent = jnp.where(visible, jnp.exp(masked - block_max[..., None]), jnp.float32(0.0))
    guarded = jnp.maximum(jnp.sum(exponent, axis=2), 1.0)
    log_total = block_max + jnp.log(guarded)
    weights = (exponent / guarded[..., None]).astype(jnp.bfloat16)
    partial_value = jnp.einsum("bht,btc->bhc", weights, cache, preferred_element_type=jnp.float32)[
        ..., :latent
    ]
    blocks = partial_value.reshape(batch, groups, heads_dev, latent)
    block_logs = log_total.reshape(batch, groups, heads_dev)
    part_blocks = lax.all_to_all(
        blocks.astype(jnp.bfloat16), "kvp", split_axis=1, concat_axis=1, tiled=True
    ).astype(blocks.dtype)
    part_logs = lax.all_to_all(block_logs, "kvp", split_axis=1, concat_axis=1, tiled=True)
    highest = jnp.max(part_logs, axis=1)
    overall = highest + jnp.log(jnp.sum(jnp.exp(part_logs - highest[:, None, :]), axis=1))
    scaled = jnp.exp(part_logs - overall[:, None, :])[..., None] * part_blocks
    o_lat = jnp.sum(scaled, axis=1).astype(jnp.bfloat16)
    attention = project(o_lat, w_uv, w_out)
    model_width = norm_gain.shape[0]
    share_width = model_width // lax.axis_size(("kvp", "tp"))
    share_start = lax.axis_index(("kvp", "tp")) * share_width
    attn_whole = lax.psum(attention, ("kvp", "tp"))
    residual = hidden_in.astype(jnp.float32) + attn_whole
    mean_square = jnp.mean(residual * residual, axis=1)
    normed = (residual * lax.rsqrt(mean_square + 1e-06)[:, None] * norm_gain[None, :]).astype(
        jnp.bfloat16
    )
    residual_share = lax.dynamic_slice_in_dim(residual, share_start, share_width, 1)
    gate_proj = jnp.dot(normed, w_gate, preferred_element_type=jnp.float32)
    up_proj = jnp.dot(normed, w_up, preferred_element_type=jnp.float32)
    act = (jax.nn.silu(gate_proj) * up_proj).astype(jnp.bfloat16)
    ffn_terms = jnp.dot(act, w_down, preferred_element_type=jnp.float32)
    ffn_share = lax.psum_scatter(ffn_terms, ("kvp", "tp"), scatter_dimension=1, tiled=True)
    return (residual_share + ffn_share).astype(jnp.bfloat16)


MESH = pl.DeviceIdType.MESH
F32 = jnp.float32
BF16 = jnp.bfloat16
VMEM_BYTES = 67043328


SPAN = 4


def layer_kernel(
    groups, tps, share, chunk, out_rows, span,
    hidden_hbm, nope_hbm, rope_hbm, len_hbm, gain_hbm,
    cache_hbm, uk_hbm, uv_hbm, wo_hbm, wg_hbm, wu_hbm, wd_hbm,
    out_ref,
    hidden_v, nope_v, rope_v, len_v, gain_v, gain_s,
    cache_v, uk_v, uv_v, big_v, gu_v,
    nope_s, qlat_s, score_s, weight_s, q_send, q_all, part_send, part_all, log_send, log_all,
    olat_s, head_s, own_s, rs_send, rs_all, ag_send, ag_all, fs_send, fs_all,
    in_sem, uk_sem, cache_sem, uv_sem, wo_sem, gu_sem, wd_sem,
    q_ss, q_rs, part_ss, part_rs, log_ss, log_rs, rs_ss, rs_rs, ag_ss, ag_rs, fs_ss, fs_rs,
):
    count = groups * tps
    kvp = lax.axis_index("kvp")
    tp = lax.axis_index("tp")
    me = kvp * tps + tp
    batch, heads, head_dim = nope_v.shape
    latent = uk_v.shape[2]
    rope = rope_v.shape[2]
    ctx = cache_v.shape[2]
    width = hidden_v.shape[1]
    chunks = width // chunk
    hidden_units = gu_v.shape[1] // 2
    parts = batch // span
    halves = tps // 2
    half = tp // 2
    chips = groups // 2

    def peer(index):
        return {"kvp": index // tps, "tp": lax.rem(index, tps)}

    def target_of(i):
        return lax.rem(kvp // 2 + i // 2, chips) * 2 + lax.rem(kvp + i, 2)

    def owner_tp(h):
        return 2 * h + 1 - (4 * h + 2) // tps

    near = [
        (target_of(i), lax.rem(half + e, halves)) for e in range(halves) for i in range(groups)
    ]
    far = near[::-1]
    mine = kvp * halves + half
    owns = tp == owner_tp(half)

    def load(source, target, sem):
        return pltpu.make_async_copy(source, target, sem)

    def cols(j):
        return pl.ds(pl.multiple_of(j * chunk, 128), chunk)

    def side(t):
        return pl.ds((t % 2) * chunk, chunk)

    def load_wo(t):
        k, h = far[t]
        return load(
            wo_hbm.at[:, cols(k * halves + h)],
            big_v.at[t // 2, pl.ds(0, out_rows), side(t)],
            wo_sem,
        )

    def load_wd(t):
        k, h = far[t]
        return load(wd_hbm.at[:, cols(k * halves + h)], big_v.at[t // 2, :, side(t)], wd_sem.at[2 * t // chunks])

    def load_gu(t, n):
        k, h = near[t]
        return load(
            (wg_hbm, wu_hbm)[n].at[cols(k * halves + h)],
            gu_v.at[pl.ds(t * chunk, chunk), pl.ds(n * hidden_units, hidden_units)],
            gu_sem.at[t // 2],
        )

    def landed(ref, sem):
        pltpu.make_async_copy(ref, ref, sem).wait()

    def load_step(s):
        for t in (2 * s, 2 * s + 1):
            load_gu(t, 0).start(priority=1)
            load_gu(t, 1).start(priority=1)

    small = [
        load(nope_hbm, nope_v, in_sem.at[0]),
        load(rope_hbm, rope_v, in_sem.at[1]),
        load(len_hbm, len_v, in_sem.at[2]),
        load(hidden_hbm, hidden_v, in_sem.at[3]),
        load(gain_hbm, gain_v.at[:, pl.ds(0, width)], in_sem.at[4]),
    ]
    uk_load = load(uk_hbm, uk_v, uk_sem)
    cache_load = load(cache_hbm, cache_v, cache_sem)
    uv_load = load(uv_hbm, uv_v, uv_sem)

    barrier = pltpu.get_barrier_semaphore()
    small[0].start()
    uk_load.start()
    small[1].start()

    @pl.loop(1, count)
    def _(d):
        pl.semaphore_signal(
            barrier, inc=1, device_id=peer(lax.rem(me + d, count)), device_id_type=MESH
        )

    cache_load.start()
    for copy in small[2:]:
        copy.start()

    small[0].wait()
    nope_s[...] = nope_v[...].astype(F32)
    small[1].wait()
    base = 2 * latent
    for b in range(batch):
        first = base + (b % 2) * rope
        q_send[b // 2, :, first : first + rope] = rope_v[b]
    uk_load.wait()
    uv_load.start()
    for t in range(chunks):
        load_wo(t).start()
    for i in range(heads):
        qlat_s[:, i, :] = jnp.dot(
            nope_s[:, i, :].astype(BF16), uk_v[i], preferred_element_type=F32
        )
    for b in range(batch):
        first = (b % 2) * latent
        q_send[b // 2, :, first : first + latent] = qlat_s[b].astype(BF16)
    pl.semaphore_wait(barrier, count - 1)

    def q_copy(i, u):
        other = target_of(i)
        return pltpu.make_async_remote_copy(
            src_ref=q_send.at[pl.ds(u * span // 2, span // 2)],
            dst_ref=q_all.at[kvp, pl.ds(u * span // 2, span // 2)],
            send_sem=q_ss,
            recv_sem=q_rs.at[u],
            device_id={"kvp": other, "tp": tp},
            device_id_type=MESH,
        )

    def part_copy(i, u):
        other = target_of(i)
        some = pl.ds(u * span, span)
        return pltpu.make_async_remote_copy(
            src_ref=part_send.at[other, some],
            dst_ref=part_all.at[kvp, some],
            send_sem=part_ss,
            recv_sem=part_rs.at[u],
            device_id={"kvp": other, "tp": tp},
            device_id_type=MESH,
        )

    def log_copy(i):
        other = target_of(i)
        return pltpu.make_async_remote_copy(
            src_ref=log_send.at[other],
            dst_ref=log_all.at[kvp],
            send_sem=log_ss,
            recv_sem=log_rs,
            device_id={"kvp": other, "tp": tp},
            device_id_type=MESH,
        )

    outward = list(range(2, groups)) + [1]
    for u in range(parts):
        for i in outward:
            q_copy(i, u).start()
    steps = chunks // 2
    for s in range(steps // 2):
        load_step(s)
    q_all[kvp] = q_send[...]
    for copy in small[2:]:
        copy.wait()
    for j in range(chunks):
        gain_s[j] = jnp.broadcast_to(gain_v[:, j * chunk : (j + 1) * chunk], (batch, chunk))
    cache_load.wait()

    scale = float(head_dim + rope) ** (-0.5)
    rows = groups * heads
    position = kvp * ctx + lax.broadcasted_iota(jnp.int32, (rows, ctx), 1)
    lane = lax.broadcasted_iota(jnp.int32, (rows, 128), 1)
    logs_acc = jnp.zeros((rows, 128), F32)
    lengths = len_v[...]
    for u in range(parts):
        landed(q_all.at[pl.ds(0, groups - 1), pl.ds(u * span // 2, span // 2)], q_rs.at[u])
        some = range(u * span, (u + 1) * span)
        for b in some:
            lat = (b % 2) * latent
            rot = base + (b % 2) * rope
            q_lat = q_all[:, b // 2, :, lat : lat + latent].astype(F32).reshape(rows, latent)
            q_rot = q_all[:, b // 2, :, rot : rot + rope].astype(F32).reshape(rows, rope)
            score_s[b] = (
                jnp.dot(q_lat.astype(BF16), cache_v[b, :latent], preferred_element_type=F32)
                + jnp.dot(q_rot.astype(BF16), cache_v[b, latent:], preferred_element_type=F32)
            ) * scale
        for b in some:
            visible = position < lengths[:, b : b + 1]
            masked = jnp.where(visible, score_s[b], F32(-1e30))
            top = jnp.max(masked, axis=1, keepdims=True)
            exps = jnp.where(visible, jnp.exp(masked - top), F32(0.0))
            guarded = jnp.maximum(jnp.sum(exps, axis=1, keepdims=True), 1.0)
            logs_acc = jnp.where(lane == b, top + jnp.log(guarded), logs_acc)
            weight_s[b] = (exps / guarded).astype(BF16)
        for b in some:
            part = lax.dot_general(
                weight_s[b], cache_v[b, :latent], (((1,), (1,)), ((), ())),
                preferred_element_type=F32,
            )
            for g in range(groups):
                part_send[g, b] = part[g * heads : (g + 1) * heads].astype(BF16)
        for i in outward:
            part_copy(i, u).start()
    for g in range(groups):
        log_send[g] = logs_acc[g * heads : (g + 1) * heads]
    for i in outward:
        log_copy(i).start()
    for s in range(steps // 2, steps):
        load_step(s)
    part_all[kvp] = part_send[kvp]
    log_all[kvp] = log_send[kvp]
    uv_load.wait()
    landed(big_v.at[:, pl.ds(0, out_rows)], wo_sem)
    landed(log_all.at[pl.ds(0, groups - 1)], log_rs)
    logs = [log_all[g] for g in range(groups)]
    highest = functools.reduce(jnp.maximum, logs)
    overall = highest + jnp.log(sum(jnp.exp(x - highest) for x in logs))
    factors = [jnp.exp(x - overall) for x in logs]
    for u in range(parts):
        landed(part_all.at[pl.ds(0, groups - 1), pl.ds(u * span, span)], part_rs.at[u])
        for b in range(u * span, (u + 1) * span):
            olat_s[b] = sum(
                factors[g][:, b : b + 1] * part_all[g, b].astype(F32) for g in range(groups)
            )
    for i in range(heads):
        head_s[:, i * head_dim : (i + 1) * head_dim] = jnp.dot(
            olat_s[:, i, :].astype(BF16), uv_v[i], preferred_element_type=F32
        ).astype(BF16)

    def rs_copy(t, slot, k, z):
        return pltpu.make_async_remote_copy(
            src_ref=rs_send.at[t],
            dst_ref=rs_all.at[slot],
            send_sem=rs_ss,
            recv_sem=rs_rs,
            device_id={"kvp": k, "tp": z},
            device_id_type=MESH,
        )

    for s in range(steps):
        both = jnp.dot(head_s[...], big_v[s, :out_rows], preferred_element_type=F32)
        for t in (2 * s, 2 * s + 1):
            k, h = far[t]
            load_wd(t).start(priority=1)
            term = both[:, (t % 2) * chunk : (t % 2 + 1) * chunk]
            rs_send[t] = term.astype(BF16)
            if t < chunks - 1:
                rs_copy(t, me, k, owner_tp(h)).start()
            else:
                own_s[...] = term

                @pl.when(jnp.logical_not(owns))
                def _():
                    rs_copy(t, me, k, owner_tp(h)).start()

    def ag_copy(d, slot, dest):
        return pltpu.make_async_remote_copy(
            src_ref=ag_send,
            dst_ref=ag_all.at[slot],
            send_sem=ag_ss,
            recv_sem=ag_rs.at[slot],
            device_id=peer(dest),
            device_id_type=MESH,
        )

    @pl.when(owns)
    def _():
        residual = hidden_v[:, cols(mine)].astype(F32) + own_s[...]
        landed(rs_all.at[pl.ds(0, count - 1)], rs_rs)
        total = residual
        for d in range(1, count):
            total = total + rs_all[lax.rem(me + d, count)].astype(F32)
        ag_send[...] = total.astype(BF16)

        @pl.loop(1, count)
        def _(d):
            ag_copy(d, mine, lax.rem(me + d, count)).start()

        ag_all[mine] = ag_send[...]

    square = jnp.zeros((batch, 1), F32)
    for s in range(steps):
        landed(gu_v.at[pl.ds(2 * s * chunk, 2 * chunk)], gu_sem.at[s])
    products = jnp.zeros((batch, 2 * hidden_units), F32)
    for s in range(steps):
        x = []
        for t in (2 * s, 2 * s + 1):
            k, h = near[t]
            j = k * halves + h
            if t == 0:
                @pl.when(jnp.logical_not(owns))
                def _():
                    ag_copy(0, j, k * tps + owner_tp(h)).wait_recv()
            else:
                ag_copy(0, j, k * tps + owner_tp(h)).wait_recv()
        for t in (2 * s, 2 * s + 1):
            k, h = near[t]
            j = k * halves + h
            value = ag_all[j].astype(F32)
            square = square + jnp.sum(value * value, axis=1, keepdims=True)
            x.append((value * gain_s[j]).astype(BF16))
        products = products + jnp.dot(
            jnp.concatenate(x, axis=1),
            gu_v[2 * s * chunk : 2 * (s + 1) * chunk],
            preferred_element_type=F32,
        )
    products = products * lax.rsqrt(square / width + 1e-06)
    gate, up = products[:, :hidden_units], products[:, hidden_units:]
    act = (gate / (1.0 + jnp.exp(-gate)) * up).astype(BF16)

    def fs_copy(n, slot, k, z):
        return pltpu.make_async_remote_copy(
            src_ref=fs_send.at[n],
            dst_ref=fs_all.at[slot],
            send_sem=fs_ss,
            recv_sem=fs_rs,
            device_id={"kvp": k, "tp": z},
            device_id_type=MESH,
        )

    pair = ag_all[mine].astype(F32)
    total = jnp.where(lax.rem(tp, 2) == 0, pair[:, :share], pair[:, share:])
    for s in range(2):
        landed(big_v.at[pl.ds(s * steps // 2, steps // 2)], wd_sem.at[s])
    for s in range(steps):
        both = jnp.dot(act, big_v[s], preferred_element_type=F32)
        for n in range(4 * s, 4 * s + 4):
            k, h = far[n // 2]
            p = n % 2
            piece = both[:, (n % 4) * share : (n % 4 + 1) * share]
            fs_send[n] = piece.astype(BF16)
            if n < count - 2:
                fs_copy(n, me, k, 2 * h + p).start()
            else:
                total = total + jnp.where(lax.rem(tp, 2) == p, piece, F32(0.0))

                @pl.when(lax.rem(tp, 2) != p)
                def _():
                    fs_copy(n, me, k, 2 * h + p).start()

    landed(fs_all.at[pl.ds(0, count - 1)], fs_rs)
    for d in range(1, count):
        total = total + fs_all[lax.rem(me + d, count)].astype(F32)
    out_ref[...] = total.astype(BF16)

    others = pl.ds(0, groups - 1)
    landed(q_all.at[others], q_ss)
    landed(part_all.at[others], part_ss)
    landed(log_all.at[others], log_ss)
    landed(fs_all.at[pl.ds(0, count - 1)], fs_ss)

    @pl.when(owns)
    def _():
        landed(rs_all.at[pl.ds(0, chunks - 1)], rs_ss)
        landed(rs_all.at[pl.ds(0, count - 1)], ag_ss)

    @pl.when(jnp.logical_not(owns))
    def _():
        landed(rs_all.at[pl.ds(0, chunks)], rs_ss)


def per_device(*operands):
    (hidden_in, queries_nope, queries_rope, cache, lengths, w_uk, w_uv, w_out, norm_gain,
     w_gate, w_up, w_down) = operands
    groups, tps = lax.axis_size("kvp"), lax.axis_size("tp")
    count = groups * tps
    batch, heads, head_dim = queries_nope.shape
    latent, rope, ctx = w_uk.shape[2], queries_rope.shape[2], cache.shape[1]
    width = hidden_in.shape[1]
    share = width // count
    ff = w_gate.shape[1]
    rows = w_out.shape[0]
    chunk = 2 * share
    held = (w_gate.size + w_up.size + max(rows, ff) * width + cache.size + w_uk.size + w_uv.size) * 2
    fits = (
        batch % 8 == 0
        and heads % 8 == 0
        and all(size % 128 == 0 for size in (head_dim, latent, 2 * rope, ctx, chunk, ff))
        and groups % 2 == 0
        and tps % 4 == 0
        and batch <= 128
        and rows <= ff
        and held < VMEM_BYTES - 8 * 2**20
    )
    if not fits:
        return plain_device(*operands)
    chunks = width // chunk
    pairs = batch // 2
    parts = batch // SPAN
    dma = pltpu.SemaphoreType.DMA
    vmem = pl.BlockSpec(memory_space=pltpu.VMEM)
    anywhere = pl.BlockSpec(memory_space=pl.ANY)
    packed = 2 * (latent + rope)
    scratch = [
        pltpu.VMEM((batch, width), BF16),
        pltpu.VMEM((batch, heads, head_dim), BF16),
        pltpu.VMEM((batch, heads, rope), BF16),
        pltpu.VMEM((1, batch), jnp.int32),
        pltpu.VMEM((1, width + 1024), F32),
        pltpu.VMEM((chunks, batch, chunk), F32),
        pltpu.VMEM((batch, latent + rope, ctx), BF16),
        pltpu.VMEM(w_uk.shape, BF16),
        pltpu.VMEM(w_uv.shape, BF16),
        pltpu.VMEM((chunks // 2, ff, 2 * chunk), BF16),
        pltpu.VMEM((width, 2 * ff), BF16),
        pltpu.VMEM((batch, heads, head_dim), F32),
        pltpu.VMEM((batch, heads, latent), F32),
        pltpu.VMEM((batch, groups * heads, ctx), F32),
        pltpu.VMEM((batch, groups * heads, ctx), BF16),
        pltpu.VMEM((pairs, heads, packed), BF16),
        pltpu.VMEM((groups, pairs, heads, packed), BF16),
        pltpu.VMEM((groups, batch, heads, latent), BF16),
        pltpu.VMEM((groups, batch, heads, latent), BF16),
        pltpu.VMEM((groups, heads, 128), F32),
        pltpu.VMEM((groups, heads, 128), F32),
        pltpu.VMEM((batch, heads, latent), F32),
        pltpu.VMEM((batch, heads * head_dim), BF16),
        pltpu.VMEM((batch, chunk), F32),
        pltpu.VMEM((chunks, batch, chunk), BF16),
        pltpu.VMEM((count, batch, chunk), BF16),
        pltpu.VMEM((batch, chunk), BF16),
        pltpu.VMEM((chunks, batch, chunk), BF16),
        pltpu.VMEM((count, batch, share), BF16),
        pltpu.VMEM((count, batch, share), BF16),
        dma((5,)), dma, dma, dma,
        dma, dma((chunks // 2,)), dma((2,)),
        dma, dma((parts,)), dma, dma((parts,)), dma, dma,
        dma, dma, dma, dma((chunks,)), dma, dma,
    ]
    return pl.pallas_call(
        functools.partial(layer_kernel, groups, tps, share, chunk, rows, SPAN),
        out_shape=jax.ShapeDtypeStruct((batch, share), BF16),
        in_specs=[anywhere] * 12,
        out_specs=vmem,
        scratch_shapes=scratch,
        compiler_params=pltpu.CompilerParams(
            collective_id=0, has_side_effects=True, vmem_limit_bytes=VMEM_BYTES
        ),
    )(
        hidden_in, queries_nope, queries_rope, lengths.reshape(1, batch), norm_gain.reshape(1, width),
        jnp.swapaxes(cache, 1, 2), w_uk, w_uv, w_out, w_gate, w_up, w_down,
    )


def solution(mesh):
    placed = (
        P("grp", None),
        P("grp", ("kvp", "tp"), None),
        P("grp", ("kvp", "tp"), None),
        P("grp", "kvp", None),
        P("grp"),
        P(("kvp", "tp"), None, None),
        P(("kvp", "tp"), None, None),
        P(("kvp", "tp"), None),
        P(),
        P(None, ("kvp", "tp")),
        P(None, ("kvp", "tp")),
        P(("kvp", "tp"), None),
    )
    return jax.shard_map(
        per_device, mesh=mesh, in_specs=placed, out_specs=P("grp", ("kvp", "tp")), check_vma=False
    )
```

```python
import functools

import jax
import jax.numpy as jnp
from jax import lax
from jax.experimental import pallas as pl
from jax.experimental.pallas import tpu as pltpu
from jax.sharding import PartitionSpec as P


def project(o_lat, w_uv, w_out):
    head_out = jnp.einsum("bhl,hle->bhe", o_lat, w_uv, preferred_element_type=jnp.float32).astype(
        jnp.bfloat16
    )
    return jnp.dot(
        head_out.reshape(head_out.shape[0], -1), w_out, preferred_element_type=jnp.float32
    )


def plain_device(
    hidden_in,
    queries_nope,
    queries_rope,
    cache,
    lengths,
    w_uk,
    w_uv,
    w_out,
    norm_gain,
    w_gate,
    w_up,
    w_down,
):
    batch, heads_dev, head_dim = queries_nope.shape
    latent = w_uk.shape[2]
    ctx_dev = cache.shape[1]
    groups = lax.axis_size("kvp")
    score_scale = float(head_dim + queries_rope.shape[2]) ** (-0.5)
    q_lat = jnp.einsum(
        "bhd,hdl->bhl", queries_nope, w_uk, preferred_element_type=jnp.float32
    ).astype(jnp.bfloat16)
    q_lat_all, rope_all = (
        lax.all_gather(q_lat, "kvp", axis=1, tiled=True),
        lax.all_gather(queries_rope, "kvp", axis=1, tiled=True),
    )
    q_full = jnp.concatenate([q_lat_all, rope_all], axis=2)
    scores = (
        jnp.einsum("bhc,btc->bht", q_full, cache, preferred_element_type=jnp.float32) * score_scale
    )
    offset = lax.axis_index("kvp") * ctx_dev
    visible = ((offset + jnp.arange(ctx_dev, dtype=jnp.int32))[None, :] < lengths[:, None])[
        :, None, :
    ]
    masked = jnp.where(visible, scores, jnp.float32(-1e30))
    block_max = jnp.max(masked, axis=2)
    exponent = jnp.where(visible, jnp.exp(masked - block_max[..., None]), jnp.float32(0.0))
    guarded = jnp.maximum(jnp.sum(exponent, axis=2), 1.0)
    log_total = block_max + jnp.log(guarded)
    weights = (exponent / guarded[..., None]).astype(jnp.bfloat16)
    partial_value = jnp.einsum("bht,btc->bhc", weights, cache, preferred_element_type=jnp.float32)[
        ..., :latent
    ]
    blocks = partial_value.reshape(batch, groups, heads_dev, latent)
    block_logs = log_total.reshape(batch, groups, heads_dev)
    part_blocks = lax.all_to_all(
        blocks.astype(jnp.bfloat16), "kvp", split_axis=1, concat_axis=1, tiled=True
    ).astype(blocks.dtype)
    part_logs = lax.all_to_all(block_logs, "kvp", split_axis=1, concat_axis=1, tiled=True)
    highest = jnp.max(part_logs, axis=1)
    overall = highest + jnp.log(jnp.sum(jnp.exp(part_logs - highest[:, None, :]), axis=1))
    scaled = jnp.exp(part_logs - overall[:, None, :])[..., None] * part_blocks
    o_lat = jnp.sum(scaled, axis=1).astype(jnp.bfloat16)
    attention = project(o_lat, w_uv, w_out)
    model_width = norm_gain.shape[0]
    share_width = model_width // lax.axis_size(("kvp", "tp"))
    share_start = lax.axis_index(("kvp", "tp")) * share_width
    attn_whole = lax.psum(attention, ("kvp", "tp"))
    residual = hidden_in.astype(jnp.float32) + attn_whole
    mean_square = jnp.mean(residual * residual, axis=1)
    normed = (residual * lax.rsqrt(mean_square + 1e-06)[:, None] * norm_gain[None, :]).astype(
        jnp.bfloat16
    )
    residual_share = lax.dynamic_slice_in_dim(residual, share_start, share_width, 1)
    gate_proj = jnp.dot(normed, w_gate, preferred_element_type=jnp.float32)
    up_proj = jnp.dot(normed, w_up, preferred_element_type=jnp.float32)
    act = (jax.nn.silu(gate_proj) * up_proj).astype(jnp.bfloat16)
    ffn_terms = jnp.dot(act, w_down, preferred_element_type=jnp.float32)
    ffn_share = lax.psum_scatter(ffn_terms, ("kvp", "tp"), scatter_dimension=1, tiled=True)
    return (residual_share + ffn_share).astype(jnp.bfloat16)


MESH = pl.DeviceIdType.MESH
F32 = jnp.float32
BF16 = jnp.bfloat16
VMEM_BYTES = 67043328


SPAN = 2


def layer_kernel(
    groups, tps, share, chunk, out_rows, span,
    hidden_hbm, nope_hbm, rope_hbm, len_hbm, gain_hbm,
    cache_hbm, uk_hbm, uv_hbm, wo_hbm, wg_hbm, wu_hbm, wd_hbm,
    out_ref,
    hidden_v, nope_v, rope_v, len_v, gain_v, gain_s,
    cache_v, uk_v, uv_v, big_v, gu_v,
    nope_s, qlat_s, score_s, weight_s, q_send, q_all, part_send, part_all, log_send, log_all,
    olat_s, head_s, own_s, rp_send, rp_all, rs_send, rs_all, ag_send, ag_all, fp_send, fp_all, fs_send, fs_all,
    in_sem, uk_sem, cache_sem, uv_sem, wo_sem, gu_sem, wd_sem,
    q_ss, q_rs, part_ss, part_rs, log_ss, log_rs, rp_ss, rp_rs, rs_ss, rs_rs, ag_ss, ag_rs, fp_ss, fp_rs, fs_ss, fs_rs,
):
    count = groups * tps
    kvp = lax.axis_index("kvp")
    tp = lax.axis_index("tp")
    me = kvp * tps + tp
    batch, heads, head_dim = nope_v.shape
    latent = uk_v.shape[2]
    rope = rope_v.shape[2]
    ctx = cache_v.shape[2]
    width = hidden_v.shape[1]
    chunks = width // chunk
    hidden_units = gu_v.shape[1] // 2
    parts = batch // span
    halves = tps // 2
    half = tp // 2
    chips = groups // 2

    def peer(index):
        return {"kvp": index // tps, "tp": lax.rem(index, tps)}

    def target_of(i):
        return lax.rem(kvp // 2 + i // 2, chips) * 2 + lax.rem(kvp + i, 2)

    def owner_tp(h):
        return 2 * h + 1 - (4 * h + 2) // tps

    near = [
        (target_of(i), lax.rem(half + e, halves)) for e in range(halves) for i in range(groups)
    ]
    reach = [(e, i) for e in range(halves) for i in range(groups)][::-1]
    order = [near[e * groups + i] for e, i in reach if i % 2 == 1]
    order += [near[e * groups + i] for e, i in reach if i % 2 == 0]
    sibling = {"kvp": target_of(1), "tp": tp}
    sources = chips * tps
    slot = (kvp // 2) * tps + tp
    mine = kvp * halves + half
    owns = tp == owner_tp(half)

    def load(source, target, sem):
        return pltpu.make_async_copy(source, target, sem)

    def cols(j):
        return pl.ds(pl.multiple_of(j * chunk, 128), chunk)

    def side(t):
        return pl.ds((t % 2) * chunk, chunk)

    def load_wo(t):
        k, h = order[t]
        return load(
            wo_hbm.at[:, cols(k * halves + h)],
            big_v.at[t // 2, pl.ds(0, out_rows), side(t)],
            wo_sem,
        )

    def load_wd(t):
        k, h = order[t]
        return load(wd_hbm.at[:, cols(k * halves + h)], big_v.at[t // 2, :, side(t)], wd_sem.at[2 * t // chunks])

    def load_gu(t, n):
        k, h = near[t]
        return load(
            (wg_hbm, wu_hbm)[n].at[cols(k * halves + h)],
            gu_v.at[pl.ds(t * chunk, chunk), pl.ds(n * hidden_units, hidden_units)],
            gu_sem.at[t // 2],
        )

    def landed(ref, sem):
        pltpu.make_async_copy(ref, ref, sem).wait()

    def load_step(s):
        for t in (2 * s, 2 * s + 1):
            load_gu(t, 0).start(priority=1)
            load_gu(t, 1).start(priority=1)

    small = [
        load(nope_hbm, nope_v, in_sem.at[0]),
        load(rope_hbm, rope_v, in_sem.at[1]),
        load(len_hbm, len_v, in_sem.at[2]),
        load(hidden_hbm, hidden_v, in_sem.at[3]),
        load(gain_hbm, gain_v.at[:, pl.ds(0, width)], in_sem.at[4]),
    ]
    uk_load = load(uk_hbm, uk_v, uk_sem)
    cache_load = load(cache_hbm, cache_v, cache_sem)
    uv_load = load(uv_hbm, uv_v, uv_sem)

    barrier = pltpu.get_barrier_semaphore()
    small[0].start()
    uk_load.start()
    small[1].start()

    @pl.loop(1, count)
    def _(d):
        pl.semaphore_signal(
            barrier, inc=1, device_id=peer(lax.rem(me + d, count)), device_id_type=MESH
        )

    cache_load.start()
    for copy in small[2:]:
        copy.start()

    small[0].wait()
    nope_s[...] = nope_v[...].astype(F32)
    small[1].wait()
    base = 2 * latent
    for b in range(batch):
        first = base + (b % 2) * rope
        q_send[b // 2, :, first : first + rope] = rope_v[b]
    uk_load.wait()
    uv_load.start()
    for t in range(chunks):
        load_wo(t).start()
    for i in range(heads):
        qlat_s[:, i, :] = jnp.dot(
            nope_s[:, i, :].astype(BF16), uk_v[i], preferred_element_type=F32
        )
    for b in range(batch):
        first = (b % 2) * latent
        q_send[b // 2, :, first : first + latent] = qlat_s[b].astype(BF16)
    pl.semaphore_wait(barrier, count - 1)

    def q_copy(i, u):
        other = target_of(i)
        return pltpu.make_async_remote_copy(
            src_ref=q_send.at[pl.ds(u * span // 2, span // 2)],
            dst_ref=q_all.at[kvp, pl.ds(u * span // 2, span // 2)],
            send_sem=q_ss,
            recv_sem=q_rs.at[u],
            device_id={"kvp": other, "tp": tp},
            device_id_type=MESH,
        )

    def part_copy(i, u):
        other = target_of(i)
        some = pl.ds(u * span, span)
        return pltpu.make_async_remote_copy(
            src_ref=part_send.at[other, some],
            dst_ref=part_all.at[kvp, some],
            send_sem=part_ss,
            recv_sem=part_rs.at[u],
            device_id={"kvp": other, "tp": tp},
            device_id_type=MESH,
        )

    def log_copy(i):
        other = target_of(i)
        return pltpu.make_async_remote_copy(
            src_ref=log_send.at[other],
            dst_ref=log_all.at[kvp],
            send_sem=log_ss,
            recv_sem=log_rs,
            device_id={"kvp": other, "tp": tp},
            device_id_type=MESH,
        )

    outward = list(range(2, groups)) + [1]
    for u in range(parts):
        for i in outward:
            q_copy(i, u).start()
    steps = chunks // 2
    for s in range(steps // 2):
        load_step(s)
    q_all[kvp] = q_send[...]
    for copy in small[2:]:
        copy.wait()
    for j in range(chunks):
        gain_s[j] = jnp.broadcast_to(gain_v[:, j * chunk : (j + 1) * chunk], (batch, chunk))
    cache_load.wait()

    scale = float(head_dim + rope) ** (-0.5)
    rows = groups * heads
    position = kvp * ctx + lax.broadcasted_iota(jnp.int32, (rows, ctx), 1)
    lane = lax.broadcasted_iota(jnp.int32, (rows, 128), 1)
    logs_acc = jnp.zeros((rows, 128), F32)
    lengths = len_v[...]
    for u in range(parts):
        landed(q_all.at[pl.ds(0, groups - 1), pl.ds(u * span // 2, span // 2)], q_rs.at[u])
        some = range(u * span, (u + 1) * span)
        for b in some:
            lat = (b % 2) * latent
            rot = base + (b % 2) * rope
            q_lat = q_all[:, b // 2, :, lat : lat + latent].astype(F32).reshape(rows, latent)
            q_rot = q_all[:, b // 2, :, rot : rot + rope].astype(F32).reshape(rows, rope)
            score_s[b] = (
                jnp.dot(q_lat.astype(BF16), cache_v[b, :latent], preferred_element_type=F32)
                + jnp.dot(q_rot.astype(BF16), cache_v[b, latent:], preferred_element_type=F32)
            ) * scale
        for b in some:
            visible = position < lengths[:, b : b + 1]
            masked = jnp.where(visible, score_s[b], F32(-1e30))
            top = jnp.max(masked, axis=1, keepdims=True)
            exps = jnp.where(visible, jnp.exp(masked - top), F32(0.0))
            guarded = jnp.maximum(jnp.sum(exps, axis=1, keepdims=True), 1.0)
            logs_acc = jnp.where(lane == b, top + jnp.log(guarded), logs_acc)
            weight_s[b] = (exps / guarded).astype(BF16)
        for b in some:
            part = lax.dot_general(
                weight_s[b], cache_v[b, :latent], (((1,), (1,)), ((), ())),
                preferred_element_type=F32,
            )
            for g in range(groups):
                part_send[g, b] = part[g * heads : (g + 1) * heads].astype(BF16)
        for i in outward:
            part_copy(i, u).start()
    for g in range(groups):
        log_send[g] = logs_acc[g * heads : (g + 1) * heads]
    for i in outward:
        log_copy(i).start()
    for s in range(steps // 2, steps):
        load_step(s)
    part_all[kvp] = part_send[kvp]
    log_all[kvp] = log_send[kvp]
    uv_load.wait()
    landed(big_v.at[:, pl.ds(0, out_rows)], wo_sem)
    landed(log_all.at[pl.ds(0, groups - 1)], log_rs)
    logs = [log_all[g] for g in range(groups)]
    highest = functools.reduce(jnp.maximum, logs)
    overall = highest + jnp.log(sum(jnp.exp(x - highest) for x in logs))
    factors = [jnp.exp(x - overall) for x in logs]
    for u in range(parts):
        landed(part_all.at[pl.ds(0, groups - 1), pl.ds(u * span, span)], part_rs.at[u])
        for b in range(u * span, (u + 1) * span):
            olat_s[b] = sum(
                factors[g][:, b : b + 1] * part_all[g, b].astype(F32) for g in range(groups)
            )
    for i in range(heads):
        head_s[:, i * head_dim : (i + 1) * head_dim] = jnp.dot(
            olat_s[:, i, :].astype(BF16), uv_v[i], preferred_element_type=F32
        ).astype(BF16)

    def pair_copy(b, source, target, ss, rs):
        return pltpu.make_async_remote_copy(
            src_ref=source.at[pl.ds(2 * b, 2)],
            dst_ref=target.at[pl.ds(2 * b, 2)],
            send_sem=ss,
            recv_sem=rs.at[b],
            device_id=sibling,
            device_id_type=MESH,
        )

    def rs_copy(n, k, h):
        return pltpu.make_async_remote_copy(
            src_ref=rs_send.at[n],
            dst_ref=rs_all.at[slot],
            send_sem=rs_ss,
            recv_sem=rs_rs,
            device_id={"kvp": k, "tp": owner_tp(h)},
            device_id_type=MESH,
        )

    first_own = steps // 2
    for s in range(steps):
        both = jnp.dot(head_s[...], big_v[s, :out_rows], preferred_element_type=F32)
        load_wd(2 * s).start(priority=1)
        load_wd(2 * s + 1).start(priority=1)
        b = s % first_own
        if s < first_own:
            for q in range(2):
                rp_send[2 * b + q] = both[:, q * chunk : (q + 1) * chunk].astype(BF16)
            pair_copy(b, rp_send, rp_all, rp_ss, rp_rs).start()
        else:
            landed(rp_all.at[pl.ds(2 * b, 2)], rp_rs.at[b])
            for q in range(2):
                n = 2 * b + q
                k, h = order[chunks // 2 + n]
                term = both[:, q * chunk : (q + 1) * chunk] + rp_all[n].astype(F32)
                rs_send[n] = term.astype(BF16)
                if n < chunks // 2 - 1:
                    rs_copy(n, k, h).start()
                else:
                    own_s[...] = term

                    @pl.when(jnp.logical_not(owns))
                    def _():
                        rs_copy(n, k, h).start()

    def ag_copy(d, j, dest):
        return pltpu.make_async_remote_copy(
            src_ref=ag_send,
            dst_ref=ag_all.at[j],
            send_sem=ag_ss,
            recv_sem=ag_rs.at[j],
            device_id=peer(dest),
            device_id_type=MESH,
        )

    @pl.when(owns)
    def _():
        residual = hidden_v[:, cols(mine)].astype(F32) + own_s[...]
        landed(rs_all.at[pl.ds(0, sources - 1)], rs_rs)
        total = residual
        for d in range(1, sources):
            total = total + rs_all[lax.rem(slot + d, sources)].astype(F32)
        ag_send[...] = total.astype(BF16)

        @pl.loop(1, count)
        def _(d):
            ag_copy(d, mine, lax.rem(me + d, count)).start()

        ag_all[mine] = ag_send[...]

    square = jnp.zeros((batch, 1), F32)
    for s in range(steps):
        landed(gu_v.at[pl.ds(2 * s * chunk, 2 * chunk)], gu_sem.at[s])
    products = jnp.zeros((batch, 2 * hidden_units), F32)
    for s in range(steps):
        x = []
        for t in (2 * s, 2 * s + 1):
            k, h = near[t]
            j = k * halves + h
            if t == 0:
                @pl.when(jnp.logical_not(owns))
                def _():
                    ag_copy(0, j, k * tps + owner_tp(h)).wait_recv()
            else:
                ag_copy(0, j, k * tps + owner_tp(h)).wait_recv()
        for t in (2 * s, 2 * s + 1):
            k, h = near[t]
            j = k * halves + h
            value = ag_all[j].astype(F32)
            square = square + jnp.sum(value * value, axis=1, keepdims=True)
            x.append((value * gain_s[j]).astype(BF16))
        products = products + jnp.dot(
            jnp.concatenate(x, axis=1),
            gu_v[2 * s * chunk : 2 * (s + 1) * chunk],
            preferred_element_type=F32,
        )
    products = products * lax.rsqrt(square / width + 1e-06)
    gate, up = products[:, :hidden_units], products[:, hidden_units:]
    act = (gate / (1.0 + jnp.exp(-gate)) * up).astype(BF16)

    def fs_copy(n, k, z):
        return pltpu.make_async_remote_copy(
            src_ref=fs_send.at[n],
            dst_ref=fs_all.at[slot],
            send_sem=fs_ss,
            recv_sem=fs_rs,
            device_id={"kvp": k, "tp": z},
            device_id_type=MESH,
        )

    pair = ag_all[mine].astype(F32)
    total = jnp.where(lax.rem(tp, 2) == 0, pair[:, :share], pair[:, share:])
    for s in range(2):
        landed(big_v.at[pl.ds(s * steps // 2, steps // 2)], wd_sem.at[s])
    for s in range(steps):
        both = jnp.dot(act, big_v[s], preferred_element_type=F32)
        b = s % first_own
        if s < first_own:
            for q in range(2):
                fp_send[2 * b + q] = both[:, q * chunk : (q + 1) * chunk].astype(BF16)
            pair_copy(b, fp_send, fp_all, fp_ss, fp_rs).start()
        else:
            landed(fp_all.at[pl.ds(2 * b, 2)], fp_rs.at[b])
            for q in range(2):
                k, h = order[chunks // 2 + 2 * b + q]
                term = both[:, q * chunk : (q + 1) * chunk] + fp_all[2 * b + q].astype(F32)
                for p in range(2):
                    n = 4 * b + 2 * q + p
                    piece = term[:, p * share : (p + 1) * share]
                    fs_send[n] = piece.astype(BF16)
                    if n < chunks - 2:
                        fs_copy(n, k, 2 * h + p).start()
                    else:
                        total = total + jnp.where(lax.rem(tp, 2) == p, piece, F32(0.0))

                        @pl.when(lax.rem(tp, 2) != p)
                        def _():
                            fs_copy(n, k, 2 * h + p).start()

    landed(fs_all.at[pl.ds(0, sources - 1)], fs_rs)
    for d in range(1, sources):
        total = total + fs_all[lax.rem(slot + d, sources)].astype(F32)
    out_ref[...] = total.astype(BF16)

    others = pl.ds(0, groups - 1)
    landed(q_all.at[others], q_ss)
    landed(part_all.at[others], part_ss)
    landed(log_all.at[others], log_ss)
    landed(fs_all.at[pl.ds(0, sources - 1)], fs_ss)
    landed(rp_all, rp_ss)
    landed(fp_all, fp_ss)

    @pl.when(owns)
    def _():
        landed(rp_all.at[pl.ds(0, chunks // 2 - 1)], rs_ss)
        rows_sent = (count - 1) * batch * chunk // 128
        landed(gu_v.at[pl.ds(0, rows_sent), pl.ds(0, 128)], ag_ss)

    @pl.when(jnp.logical_not(owns))
    def _():
        landed(rp_all, rs_ss)


def per_device(*operands):
    (hidden_in, queries_nope, queries_rope, cache, lengths, w_uk, w_uv, w_out, norm_gain,
     w_gate, w_up, w_down) = operands
    groups, tps = lax.axis_size("kvp"), lax.axis_size("tp")
    count = groups * tps
    batch, heads, head_dim = queries_nope.shape
    latent, rope, ctx = w_uk.shape[2], queries_rope.shape[2], cache.shape[1]
    width = hidden_in.shape[1]
    share = width // count
    ff = w_gate.shape[1]
    rows = w_out.shape[0]
    chunk = 2 * share
    held = (w_gate.size + w_up.size + max(rows, ff) * width + cache.size + w_uk.size + w_uv.size) * 2
    fits = (
        batch % 8 == 0
        and heads % 8 == 0
        and all(size % 128 == 0 for size in (head_dim, latent, 2 * rope, ctx, chunk, ff))
        and groups % 2 == 0
        and tps % 4 == 0
        and batch <= 128
        and rows <= ff
        and held < VMEM_BYTES - 8 * 2**20
    )
    if not fits:
        return plain_device(*operands)
    chunks = width // chunk
    pairs = batch // 2
    parts = batch // SPAN
    dma = pltpu.SemaphoreType.DMA
    vmem = pl.BlockSpec(memory_space=pltpu.VMEM)
    anywhere = pl.BlockSpec(memory_space=pl.ANY)
    packed = 2 * (latent + rope)
    half_set = pltpu.VMEM((chunks // 2, batch, chunk), BF16)
    scratch = [
        pltpu.VMEM((batch, width), BF16),
        pltpu.VMEM((batch, heads, head_dim), BF16),
        pltpu.VMEM((batch, heads, rope), BF16),
        pltpu.VMEM((1, batch), jnp.int32),
        pltpu.VMEM((1, width + 1024), F32),
        pltpu.VMEM((chunks, batch, chunk), F32),
        pltpu.VMEM((batch, latent + rope, ctx), BF16),
        pltpu.VMEM(w_uk.shape, BF16),
        pltpu.VMEM(w_uv.shape, BF16),
        pltpu.VMEM((chunks // 2, ff, 2 * chunk), BF16),
        pltpu.VMEM((width, 2 * ff), BF16),
        pltpu.VMEM((batch, heads, head_dim), F32),
        pltpu.VMEM((batch, heads, latent), F32),
        pltpu.VMEM((batch, groups * heads, ctx), F32),
        pltpu.VMEM((batch, groups * heads, ctx), BF16),
        pltpu.VMEM((pairs, heads, packed), BF16),
        pltpu.VMEM((groups, pairs, heads, packed), BF16),
        pltpu.VMEM((groups, batch, heads, latent), BF16),
        pltpu.VMEM((groups, batch, heads, latent), BF16),
        pltpu.VMEM((groups, heads, 128), F32),
        pltpu.VMEM((groups, heads, 128), F32),
        pltpu.VMEM((batch, heads, latent), F32),
        pltpu.VMEM((batch, heads * head_dim), BF16),
        pltpu.VMEM((batch, chunk), F32),
        half_set, half_set, half_set,
        pltpu.VMEM((count // 2, batch, chunk), BF16),
        pltpu.VMEM((batch, chunk), BF16),
        pltpu.VMEM((chunks, batch, chunk), BF16),
        half_set, half_set,
        pltpu.VMEM((count // 2, batch, share), BF16),
        pltpu.VMEM((count // 2, batch, share), BF16),
        dma((5,)), dma, dma, dma,
        dma, dma((chunks // 2,)), dma((2,)),
        dma, dma((parts,)), dma, dma((parts,)), dma, dma,
        dma, dma((chunks // 4,)), dma, dma, dma, dma((chunks,)), dma, dma((chunks // 4,)), dma, dma,
    ]
    return pl.pallas_call(
        functools.partial(layer_kernel, groups, tps, share, chunk, rows, SPAN),
        out_shape=pltpu.VMEM((batch, share), BF16),
        in_specs=[anywhere] * 12,
        out_specs=vmem,
        scratch_shapes=scratch,
        compiler_params=pltpu.CompilerParams(
            collective_id=0, has_side_effects=True, vmem_limit_bytes=VMEM_BYTES - 640 * 1024
        ),
    )(
        hidden_in, queries_nope, queries_rope, lengths.reshape(1, batch), norm_gain.reshape(1, width),
        jnp.swapaxes(cache, 1, 2), w_uk, w_uv, w_out, w_gate, w_up, w_down,
    )


def solution(mesh):
    placed = (
        P("grp", None),
        P("grp", ("kvp", "tp"), None),
        P("grp", ("kvp", "tp"), None),
        P("grp", "kvp", None),
        P("grp"),
        P(("kvp", "tp"), None, None),
        P(("kvp", "tp"), None, None),
        P(("kvp", "tp"), None),
        P(),
        P(None, ("kvp", "tp")),
        P(None, ("kvp", "tp")),
        P(("kvp", "tp"), None),
    )
    return jax.shard_map(
        per_device, mesh=mesh, in_specs=placed, out_specs=P("grp", ("kvp", "tp")), check_vma=False
    )
```

```python
import functools

import jax
import jax.numpy as jnp
from jax import lax
from jax.experimental import pallas as pl
from jax.experimental.pallas import tpu as pltpu
from jax.sharding import PartitionSpec as P


def project(o_lat, w_uv, w_out):
    head_out = jnp.einsum("bhl,hle->bhe", o_lat, w_uv, preferred_element_type=jnp.float32).astype(
        jnp.bfloat16
    )
    return jnp.dot(
        head_out.reshape(head_out.shape[0], -1), w_out, preferred_element_type=jnp.float32
    )


def plain_device(
    hidden_in,
    queries_nope,
    queries_rope,
    cache,
    lengths,
    w_uk,
    w_uv,
    w_out,
    norm_gain,
    w_gate,
    w_up,
    w_down,
):
    batch, heads_dev, head_dim = queries_nope.shape
    latent = w_uk.shape[2]
    ctx_dev = cache.shape[1]
    groups = lax.axis_size("kvp")
    score_scale = float(head_dim + queries_rope.shape[2]) ** (-0.5)
    q_lat = jnp.einsum(
        "bhd,hdl->bhl", queries_nope, w_uk, preferred_element_type=jnp.float32
    ).astype(jnp.bfloat16)
    q_lat_all, rope_all = (
        lax.all_gather(q_lat, "kvp", axis=1, tiled=True),
        lax.all_gather(queries_rope, "kvp", axis=1, tiled=True),
    )
    q_full = jnp.concatenate([q_lat_all, rope_all], axis=2)
    scores = (
        jnp.einsum("bhc,btc->bht", q_full, cache, preferred_element_type=jnp.float32) * score_scale
    )
    offset = lax.axis_index("kvp") * ctx_dev
    visible = ((offset + jnp.arange(ctx_dev, dtype=jnp.int32))[None, :] < lengths[:, None])[
        :, None, :
    ]
    masked = jnp.where(visible, scores, jnp.float32(-1e30))
    block_max = jnp.max(masked, axis=2)
    exponent = jnp.where(visible, jnp.exp(masked - block_max[..., None]), jnp.float32(0.0))
    guarded = jnp.maximum(jnp.sum(exponent, axis=2), 1.0)
    log_total = block_max + jnp.log(guarded)
    weights = (exponent / guarded[..., None]).astype(jnp.bfloat16)
    partial_value = jnp.einsum("bht,btc->bhc", weights, cache, preferred_element_type=jnp.float32)[
        ..., :latent
    ]
    blocks = partial_value.reshape(batch, groups, heads_dev, latent)
    block_logs = log_total.reshape(batch, groups, heads_dev)
    part_blocks = lax.all_to_all(
        blocks.astype(jnp.bfloat16), "kvp", split_axis=1, concat_axis=1, tiled=True
    ).astype(blocks.dtype)
    part_logs = lax.all_to_all(block_logs, "kvp", split_axis=1, concat_axis=1, tiled=True)
    highest = jnp.max(part_logs, axis=1)
    overall = highest + jnp.log(jnp.sum(jnp.exp(part_logs - highest[:, None, :]), axis=1))
    scaled = jnp.exp(part_logs - overall[:, None, :])[..., None] * part_blocks
    o_lat = jnp.sum(scaled, axis=1).astype(jnp.bfloat16)
    attention = project(o_lat, w_uv, w_out)
    model_width = norm_gain.shape[0]
    share_width = model_width // lax.axis_size(("kvp", "tp"))
    share_start = lax.axis_index(("kvp", "tp")) * share_width
    attn_whole = lax.psum(attention, ("kvp", "tp"))
    residual = hidden_in.astype(jnp.float32) + attn_whole
    mean_square = jnp.mean(residual * residual, axis=1)
    normed = (residual * lax.rsqrt(mean_square + 1e-06)[:, None] * norm_gain[None, :]).astype(
        jnp.bfloat16
    )
    residual_share = lax.dynamic_slice_in_dim(residual, share_start, share_width, 1)
    gate_proj = jnp.dot(normed, w_gate, preferred_element_type=jnp.float32)
    up_proj = jnp.dot(normed, w_up, preferred_element_type=jnp.float32)
    act = (jax.nn.silu(gate_proj) * up_proj).astype(jnp.bfloat16)
    ffn_terms = jnp.dot(act, w_down, preferred_element_type=jnp.float32)
    ffn_share = lax.psum_scatter(ffn_terms, ("kvp", "tp"), scatter_dimension=1, tiled=True)
    return (residual_share + ffn_share).astype(jnp.bfloat16)


MESH = pl.DeviceIdType.MESH
F32 = jnp.float32
BF16 = jnp.bfloat16
VMEM_BYTES = 67043328


SPAN = 2


def layer_kernel(
    groups, tps, share, chunk, out_rows, span,
    hidden_hbm, nope_hbm, rope_hbm, len_hbm, gain_hbm,
    cache_hbm, uk_hbm, uv_hbm, wo_hbm, wg_hbm, wu_hbm, wd_hbm,
    out_ref,
    hidden_v, nope_v, rope_v, len_v, gain_v, gain_s,
    cache_v, uk_v, uv_v, big_v, gu_v,
    nope_s, qlat_s, score_s, weight_s, q_send, q_all, part_send, part_all, log_send, log_all,
    olat_s, head_s, own_s, rp_send, rp_all, rs_send, rs_all, ag_send, ag_all, fp_send, fp_all, fs_send, fs_all,
    in_sem, uk_sem, cache_sem, uv_sem, wo_sem, gu_sem, wd_sem,
    q_ss, q_rs, part_ss, part_rs, log_ss, log_rs, rp_ss, rp_rs, rs_ss, rs_rs, ag_ss, ag_rs, fp_ss, fp_rs, fs_ss, fs_rs, up_sem, down_sem,
):
    count = groups * tps
    kvp = lax.axis_index("kvp")
    tp = lax.axis_index("tp")
    me = kvp * tps + tp
    batch, heads, head_dim = nope_v.shape
    latent = uk_v.shape[2]
    rope = rope_v.shape[2]
    ctx = cache_v.shape[2]
    width = hidden_v.shape[1]
    chunks = width // chunk
    hidden_units = gu_v.shape[1] // 2
    parts = batch // span
    halves = tps // 2
    half = tp // 2
    chips = groups // 2

    def peer(index):
        return {"kvp": index // tps, "tp": lax.rem(index, tps)}

    def target_of(i):
        return lax.rem(kvp // 2 + i // 2, chips) * 2 + lax.rem(kvp + i, 2)

    def owner_tp(h):
        return 2 * h + 1 - (4 * h + 2) // tps

    near = [
        (target_of(i), lax.rem(half + e, halves)) for e in range(halves) for i in range(groups)
    ]
    reach = [(e, i) for e in range(halves) for i in range(groups)][::-1]
    order = [near[e * groups + i] for e, i in reach if i % 2 == 1]
    order += [near[e * groups + i] for e, i in reach if i % 2 == 0]
    sibling = {"kvp": target_of(1), "tp": tp}
    sources = chips * tps
    slot = (kvp // 2) * tps + tp
    mine = kvp * halves + half
    owns = tp == owner_tp(half)

    def load(source, target, sem):
        return pltpu.make_async_copy(source, target, sem)

    def cols(j):
        return pl.ds(pl.multiple_of(j * chunk, 128), chunk)

    def side(t):
        return pl.ds((t % 2) * chunk, chunk)

    def load_wo(t):
        k, h = order[t]
        return load(
            wo_hbm.at[:, cols(k * halves + h)],
            big_v.at[t // 2, pl.ds(0, out_rows), side(t)],
            wo_sem,
        )

    def load_wd(t):
        k, h = order[t]
        return load(wd_hbm.at[:, cols(k * halves + h)], big_v.at[t // 2, :, side(t)], wd_sem.at[2 * t // chunks])

    def load_gu(t, n):
        k, h = near[t]
        return load(
            (wg_hbm, wu_hbm)[n].at[cols(k * halves + h)],
            gu_v.at[pl.ds(t * chunk, chunk), pl.ds(n * hidden_units, hidden_units)],
            gu_sem.at[t // 2],
        )

    def landed(ref, sem):
        pltpu.make_async_copy(ref, ref, sem).wait()

    def load_step(s):
        for t in (2 * s, 2 * s + 1):
            load_gu(t, 0).start(priority=1)
            load_gu(t, 1).start(priority=1)

    small = [
        load(nope_hbm, nope_v, in_sem.at[0]),
        load(rope_hbm, rope_v, in_sem.at[1]),
        load(len_hbm, len_v, in_sem.at[2]),
        load(hidden_hbm, hidden_v, in_sem.at[3]),
        load(gain_hbm, gain_v.at[:, pl.ds(0, width)], in_sem.at[4]),
    ]
    uk_load = load(uk_hbm, uk_v, uk_sem)
    cache_load = load(cache_hbm, cache_v, cache_sem)
    uv_load = load(uv_hbm, uv_v, uv_sem)

    barrier = pltpu.get_barrier_semaphore()
    small[0].start()
    uk_load.start()
    small[1].start()

    below = {"kvp": kvp, "tp": lax.rem(tp + tps - 1, tps)}
    above = {"kvp": kvp, "tp": lax.rem(tp + 1, tps)}
    has_below, has_above = tp > 0, tp < tps - 1

    def greet(sem, device):
        pl.semaphore_signal(sem, inc=1, device_id=device, device_id_type=MESH)

    for i in range(1, groups):
        greet(barrier, {"kvp": target_of(i), "tp": tp})

    @pl.when(has_below)
    def _():
        greet(barrier, below)

    @pl.when(has_above)
    def _():
        greet(barrier, above)

    cache_load.start()
    for copy in small[2:]:
        copy.start()

    small[0].wait()
    nope_s[...] = nope_v[...].astype(F32)
    small[1].wait()
    base = 2 * latent
    for b in range(batch):
        first = base + (b % 2) * rope
        q_send[b // 2, :, first : first + rope] = rope_v[b]
    uk_load.wait()
    uv_load.start()
    for t in range(chunks):
        load_wo(t).start()
    for i in range(heads):
        qlat_s[:, i, :] = jnp.dot(
            nope_s[:, i, :].astype(BF16), uk_v[i], preferred_element_type=F32
        )
    for b in range(batch):
        first = (b % 2) * latent
        q_send[b // 2, :, first : first + latent] = qlat_s[b].astype(BF16)
    edges = (tps - tp - 1) // (tps - 1) + tp // (tps - 1)
    pl.semaphore_wait(barrier, groups + 1 - edges)

    def q_copy(i, u):
        other = target_of(i)
        return pltpu.make_async_remote_copy(
            src_ref=q_send.at[pl.ds(u * span // 2, span // 2)],
            dst_ref=q_all.at[kvp, pl.ds(u * span // 2, span // 2)],
            send_sem=q_ss,
            recv_sem=q_rs.at[u],
            device_id={"kvp": other, "tp": tp},
            device_id_type=MESH,
        )

    def part_copy(i, u):
        other = target_of(i)
        some = pl.ds(u * span, span)
        return pltpu.make_async_remote_copy(
            src_ref=part_send.at[other, some],
            dst_ref=part_all.at[kvp, some],
            send_sem=part_ss,
            recv_sem=part_rs.at[u],
            device_id={"kvp": other, "tp": tp},
            device_id_type=MESH,
        )

    def log_copy(i):
        other = target_of(i)
        return pltpu.make_async_remote_copy(
            src_ref=log_send.at[other],
            dst_ref=log_all.at[kvp],
            send_sem=log_ss,
            recv_sem=log_rs,
            device_id={"kvp": other, "tp": tp},
            device_id_type=MESH,
        )

    outward = list(range(2, groups)) + [1]
    for u in range(parts):
        for i in outward:
            q_copy(i, u).start()
    steps = chunks // 2
    for s in range(steps // 2):
        load_step(s)
    def token(sem, arrives, leaves, device):
        @pl.when(arrives)
        def _():
            pl.semaphore_wait(sem, 1)

        @pl.when(leaves)
        def _():
            greet(sem, device)

    up = functools.partial(token, up_sem, has_below, has_above, above)
    down = functools.partial(token, down_sem, has_above, has_below, below)

    @pl.when(half < halves // 2)
    def _():
        up()
        down()

    @pl.when(half >= halves // 2)
    def _():
        down()
        up()

    q_all[kvp] = q_send[...]
    for copy in small[2:]:
        copy.wait()
    for j in range(chunks):
        gain_s[j] = jnp.broadcast_to(gain_v[:, j * chunk : (j + 1) * chunk], (batch, chunk))
    cache_load.wait()

    scale = float(head_dim + rope) ** (-0.5)
    rows = groups * heads
    position = kvp * ctx + lax.broadcasted_iota(jnp.int32, (rows, ctx), 1)
    lane = lax.broadcasted_iota(jnp.int32, (rows, 128), 1)
    logs_acc = jnp.zeros((rows, 128), F32)
    lengths = len_v[...]
    for u in range(parts):
        landed(q_all.at[pl.ds(0, groups - 1), pl.ds(u * span // 2, span // 2)], q_rs.at[u])
        some = range(u * span, (u + 1) * span)
        for b in some:
            lat = (b % 2) * latent
            rot = base + (b % 2) * rope
            q_lat = q_all[:, b // 2, :, lat : lat + latent].astype(F32).reshape(rows, latent)
            q_rot = q_all[:, b // 2, :, rot : rot + rope].astype(F32).reshape(rows, rope)
            score_s[b] = (
                jnp.dot(q_lat.astype(BF16), cache_v[b, :latent], preferred_element_type=F32)
                + jnp.dot(q_rot.astype(BF16), cache_v[b, latent:], preferred_element_type=F32)
            ) * scale
        for b in some:
            visible = position < lengths[:, b : b + 1]
            masked = jnp.where(visible, score_s[b], F32(-1e30))
            top = jnp.max(masked, axis=1, keepdims=True)
            exps = jnp.where(visible, jnp.exp(masked - top), F32(0.0))
            guarded = jnp.maximum(jnp.sum(exps, axis=1, keepdims=True), 1.0)
            logs_acc = jnp.where(lane == b, top + jnp.log(guarded), logs_acc)
            weight_s[b] = (exps / guarded).astype(BF16)
        for b in some:
            part = lax.dot_general(
                weight_s[b], cache_v[b, :latent], (((1,), (1,)), ((), ())),
                preferred_element_type=F32,
            )
            for g in range(groups):
                part_send[g, b] = part[g * heads : (g + 1) * heads].astype(BF16)
        for i in outward:
            part_copy(i, u).start()
    for g in range(groups):
        log_send[g] = logs_acc[g * heads : (g + 1) * heads]
    for i in outward:
        log_copy(i).start()
    for s in range(steps // 2, steps):
        load_step(s)
    part_all[kvp] = part_send[kvp]
    log_all[kvp] = log_send[kvp]
    uv_load.wait()
    landed(big_v.at[:, pl.ds(0, out_rows)], wo_sem)
    landed(log_all.at[pl.ds(0, groups - 1)], log_rs)
    logs = [log_all[g] for g in range(groups)]
    highest = functools.reduce(jnp.maximum, logs)
    overall = highest + jnp.log(sum(jnp.exp(x - highest) for x in logs))
    factors = [jnp.exp(x - overall) for x in logs]
    for u in range(parts):
        landed(part_all.at[pl.ds(0, groups - 1), pl.ds(u * span, span)], part_rs.at[u])
        for b in range(u * span, (u + 1) * span):
            olat_s[b] = sum(
                factors[g][:, b : b + 1] * part_all[g, b].astype(F32) for g in range(groups)
            )
    for i in range(heads):
        head_s[:, i * head_dim : (i + 1) * head_dim] = jnp.dot(
            olat_s[:, i, :].astype(BF16), uv_v[i], preferred_element_type=F32
        ).astype(BF16)

    def pair_copy(b, source, target, ss, rs):
        return pltpu.make_async_remote_copy(
            src_ref=source.at[pl.ds(2 * b, 2)],
            dst_ref=target.at[pl.ds(2 * b, 2)],
            send_sem=ss,
            recv_sem=rs.at[b],
            device_id=sibling,
            device_id_type=MESH,
        )

    def rs_copy(n, k, h):
        return pltpu.make_async_remote_copy(
            src_ref=rs_send.at[n],
            dst_ref=rs_all.at[slot],
            send_sem=rs_ss,
            recv_sem=rs_rs,
            device_id={"kvp": k, "tp": owner_tp(h)},
            device_id_type=MESH,
        )

    first_own = steps // 2
    for s in range(steps):
        both = jnp.dot(head_s[...], big_v[s, :out_rows], preferred_element_type=F32)
        load_wd(2 * s).start(priority=1)
        load_wd(2 * s + 1).start(priority=1)
        b = s % first_own
        if s < first_own:
            for q in range(2):
                rp_send[2 * b + q] = both[:, q * chunk : (q + 1) * chunk].astype(BF16)
            pair_copy(b, rp_send, rp_all, rp_ss, rp_rs).start()
        else:
            landed(rp_all.at[pl.ds(2 * b, 2)], rp_rs.at[b])
            for q in range(2):
                n = 2 * b + q
                k, h = order[chunks // 2 + n]
                term = both[:, q * chunk : (q + 1) * chunk] + rp_all[n].astype(F32)
                rs_send[n] = term.astype(BF16)
                if n < chunks // 2 - 1:
                    rs_copy(n, k, h).start()
                else:
                    own_s[...] = term

                    @pl.when(jnp.logical_not(owns))
                    def _():
                        rs_copy(n, k, h).start()

    def ag_copy(d, j, dest):
        return pltpu.make_async_remote_copy(
            src_ref=ag_send,
            dst_ref=ag_all.at[j],
            send_sem=ag_ss,
            recv_sem=ag_rs.at[j],
            device_id=peer(dest),
            device_id_type=MESH,
        )

    @pl.when(owns)
    def _():
        residual = hidden_v[:, cols(mine)].astype(F32) + own_s[...]
        landed(rs_all.at[pl.ds(0, sources - 1)], rs_rs)
        total = residual
        for d in range(1, sources):
            total = total + rs_all[lax.rem(slot + d, sources)].astype(F32)
        ag_send[...] = total.astype(BF16)

        @pl.loop(1, count)
        def _(d):
            ag_copy(d, mine, lax.rem(me + d, count)).start()

        ag_all[mine] = ag_send[...]

    square = jnp.zeros((batch, 1), F32)
    for s in range(steps):
        landed(gu_v.at[pl.ds(2 * s * chunk, 2 * chunk)], gu_sem.at[s])
    products = jnp.zeros((batch, 2 * hidden_units), F32)
    for s in range(steps):
        x = []
        for t in (2 * s, 2 * s + 1):
            k, h = near[t]
            j = k * halves + h
            if t == 0:
                @pl.when(jnp.logical_not(owns))
                def _():
                    ag_copy(0, j, k * tps + owner_tp(h)).wait_recv()
            else:
                ag_copy(0, j, k * tps + owner_tp(h)).wait_recv()
        for t in (2 * s, 2 * s + 1):
            k, h = near[t]
            j = k * halves + h
            value = ag_all[j].astype(F32)
            square = square + jnp.sum(value * value, axis=1, keepdims=True)
            x.append((value * gain_s[j]).astype(BF16))
        products = products + jnp.dot(
            jnp.concatenate(x, axis=1),
            gu_v[2 * s * chunk : 2 * (s + 1) * chunk],
            preferred_element_type=F32,
        )
    products = products * lax.rsqrt(square / width + 1e-06)
    gate, up = products[:, :hidden_units], products[:, hidden_units:]
    act = (gate / (1.0 + jnp.exp(-gate)) * up).astype(BF16)

    def fs_copy(n, k, z):
        return pltpu.make_async_remote_copy(
            src_ref=fs_send.at[n],
            dst_ref=fs_all.at[slot],
            send_sem=fs_ss,
            recv_sem=fs_rs,
            device_id={"kvp": k, "tp": z},
            device_id_type=MESH,
        )

    pair = ag_all[mine].astype(F32)
    total = jnp.where(lax.rem(tp, 2) == 0, pair[:, :share], pair[:, share:])
    for s in range(2):
        landed(big_v.at[pl.ds(s * steps // 2, steps // 2)], wd_sem.at[s])
    for s in range(steps):
        both = jnp.dot(act, big_v[s], preferred_element_type=F32)
        b = s % first_own
        if s < first_own:
            for q in range(2):
                fp_send[2 * b + q] = both[:, q * chunk : (q + 1) * chunk].astype(BF16)
            pair_copy(b, fp_send, fp_all, fp_ss, fp_rs).start()
        else:
            landed(fp_all.at[pl.ds(2 * b, 2)], fp_rs.at[b])
            for q in range(2):
                k, h = order[chunks // 2 + 2 * b + q]
                term = both[:, q * chunk : (q + 1) * chunk] + fp_all[2 * b + q].astype(F32)
                for p in range(2):
                    n = 4 * b + 2 * q + p
                    piece = term[:, p * share : (p + 1) * share]
                    fs_send[n] = piece.astype(BF16)
                    if n < chunks - 2:
                        fs_copy(n, k, 2 * h + p).start()
                    else:
                        total = total + jnp.where(lax.rem(tp, 2) == p, piece, F32(0.0))

                        @pl.when(lax.rem(tp, 2) != p)
                        def _():
                            fs_copy(n, k, 2 * h + p).start()

    landed(fs_all.at[pl.ds(0, sources - 1)], fs_rs)
    for d in range(1, sources):
        total = total + fs_all[lax.rem(slot + d, sources)].astype(F32)
    out_ref[...] = total.astype(BF16)

    others = pl.ds(0, groups - 1)
    landed(q_all.at[others], q_ss)
    landed(part_all.at[others], part_ss)
    landed(log_all.at[others], log_ss)
    landed(fs_all.at[pl.ds(0, sources - 1)], fs_ss)
    landed(rp_all, rp_ss)
    landed(fp_all, fp_ss)

    @pl.when(owns)
    def _():
        landed(rp_all.at[pl.ds(0, chunks // 2 - 1)], rs_ss)
        rows_sent = (count - 1) * batch * chunk // 128
        landed(gu_v.at[pl.ds(0, rows_sent), pl.ds(0, 128)], ag_ss)

    @pl.when(jnp.logical_not(owns))
    def _():
        landed(rp_all, rs_ss)


def per_device(*operands):
    (hidden_in, queries_nope, queries_rope, cache, lengths, w_uk, w_uv, w_out, norm_gain,
     w_gate, w_up, w_down) = operands
    groups, tps = lax.axis_size("kvp"), lax.axis_size("tp")
    count = groups * tps
    batch, heads, head_dim = queries_nope.shape
    latent, rope, ctx = w_uk.shape[2], queries_rope.shape[2], cache.shape[1]
    width = hidden_in.shape[1]
    share = width // count
    ff = w_gate.shape[1]
    rows = w_out.shape[0]
    chunk = 2 * share
    held = (w_gate.size + w_up.size + max(rows, ff) * width + cache.size + w_uk.size + w_uv.size) * 2
    fits = (
        batch % 8 == 0
        and heads % 8 == 0
        and all(size % 128 == 0 for size in (head_dim, latent, 2 * rope, ctx, chunk, ff))
        and groups % 2 == 0
        and tps % 4 == 0
        and batch <= 128
        and rows <= ff
        and held < VMEM_BYTES - 8 * 2**20
    )
    if not fits:
        return plain_device(*operands)
    chunks = width // chunk
    pairs = batch // 2
    parts = batch // SPAN
    dma = pltpu.SemaphoreType.DMA
    vmem = pl.BlockSpec(memory_space=pltpu.VMEM)
    anywhere = pl.BlockSpec(memory_space=pl.ANY)
    packed = 2 * (latent + rope)
    half_set = pltpu.VMEM((chunks // 2, batch, chunk), BF16)
    scratch = [
        pltpu.VMEM((batch, width), BF16),
        pltpu.VMEM((batch, heads, head_dim), BF16),
        pltpu.VMEM((batch, heads, rope), BF16),
        pltpu.VMEM((1, batch), jnp.int32),
        pltpu.VMEM((1, width + 1024), F32),
        pltpu.VMEM((chunks, batch, chunk), F32),
        pltpu.VMEM((batch, latent + rope, ctx), BF16),
        pltpu.VMEM(w_uk.shape, BF16),
        pltpu.VMEM(w_uv.shape, BF16),
        pltpu.VMEM((chunks // 2, ff, 2 * chunk), BF16),
        pltpu.VMEM((width, 2 * ff), BF16),
        pltpu.VMEM((batch, heads, head_dim), F32),
        pltpu.VMEM((batch, heads, latent), F32),
        pltpu.VMEM((batch, groups * heads, ctx), F32),
        pltpu.VMEM((batch, groups * heads, ctx), BF16),
        pltpu.VMEM((pairs, heads, packed), BF16),
        pltpu.VMEM((groups, pairs, heads, packed), BF16),
        pltpu.VMEM((groups, batch, heads, latent), BF16),
        pltpu.VMEM((groups, batch, heads, latent), BF16),
        pltpu.VMEM((groups, heads, 128), F32),
        pltpu.VMEM((groups, heads, 128), F32),
        pltpu.VMEM((batch, heads, latent), F32),
        pltpu.VMEM((batch, heads * head_dim), BF16),
        pltpu.VMEM((batch, chunk), F32),
        half_set, half_set, half_set,
        pltpu.VMEM((count // 2, batch, chunk), BF16),
        pltpu.VMEM((batch, chunk), BF16),
        pltpu.VMEM((chunks, batch, chunk), BF16),
        half_set, half_set,
        pltpu.VMEM((count // 2, batch, share), BF16),
        pltpu.VMEM((count // 2, batch, share), BF16),
        dma((5,)), dma, dma, dma,
        dma, dma((chunks // 2,)), dma((2,)),
        dma, dma((parts,)), dma, dma((parts,)), dma, dma,
        dma, dma((chunks // 4,)), dma, dma, dma, dma((chunks,)), dma, dma((chunks // 4,)), dma, dma,
        pltpu.SemaphoreType.REGULAR, pltpu.SemaphoreType.REGULAR,
    ]
    return pl.pallas_call(
        functools.partial(layer_kernel, groups, tps, share, chunk, rows, SPAN),
        out_shape=pltpu.VMEM((batch, share), BF16),
        in_specs=[anywhere] * 12,
        out_specs=vmem,
        scratch_shapes=scratch,
        compiler_params=pltpu.CompilerParams(
            collective_id=0, has_side_effects=True, vmem_limit_bytes=VMEM_BYTES - 640 * 1024
        ),
    )(
        hidden_in, queries_nope, queries_rope, lengths.reshape(1, batch), norm_gain.reshape(1, width),
        jnp.swapaxes(cache, 1, 2), w_uk, w_uv, w_out, w_gate, w_up, w_down,
    )


def solution(mesh):
    placed = (
        P("grp", None),
        P("grp", ("kvp", "tp"), None),
        P("grp", ("kvp", "tp"), None),
        P("grp", "kvp", None),
        P("grp"),
        P(("kvp", "tp"), None, None),
        P(("kvp", "tp"), None, None),
        P(("kvp", "tp"), None),
        P(),
        P(None, ("kvp", "tp")),
        P(None, ("kvp", "tp")),
        P(("kvp", "tp"), None),
    )
    return jax.shard_map(
        per_device, mesh=mesh, in_specs=placed, out_specs=P("grp", ("kvp", "tp")), check_vma=False
    )
```

```python
import functools
import math

import jax
import jax.numpy as jnp
from jax import lax
from jax.experimental import pallas as pl
from jax.experimental.pallas import tpu as pltpu
from jax.sharding import PartitionSpec as P


def project(o_lat, w_uv, w_out):
    head_out = jnp.einsum("bhl,hle->bhe", o_lat, w_uv, preferred_element_type=jnp.float32).astype(
        jnp.bfloat16
    )
    return jnp.dot(
        head_out.reshape(head_out.shape[0], -1), w_out, preferred_element_type=jnp.float32
    )


def plain_device(
    hidden_in,
    queries_nope,
    queries_rope,
    cache,
    lengths,
    w_uk,
    w_uv,
    w_out,
    norm_gain,
    w_gate,
    w_up,
    w_down,
):
    batch, heads_dev, head_dim = queries_nope.shape
    latent = w_uk.shape[2]
    ctx_dev = cache.shape[1]
    groups = lax.axis_size("kvp")
    score_scale = float(head_dim + queries_rope.shape[2]) ** (-0.5)
    q_lat = jnp.einsum(
        "bhd,hdl->bhl", queries_nope, w_uk, preferred_element_type=jnp.float32
    ).astype(jnp.bfloat16)
    q_lat_all, rope_all = (
        lax.all_gather(q_lat, "kvp", axis=1, tiled=True),
        lax.all_gather(queries_rope, "kvp", axis=1, tiled=True),
    )
    q_full = jnp.concatenate([q_lat_all, rope_all], axis=2)
    scores = (
        jnp.einsum("bhc,btc->bht", q_full, cache, preferred_element_type=jnp.float32) * score_scale
    )
    offset = lax.axis_index("kvp") * ctx_dev
    visible = ((offset + jnp.arange(ctx_dev, dtype=jnp.int32))[None, :] < lengths[:, None])[
        :, None, :
    ]
    masked = jnp.where(visible, scores, jnp.float32(-1e30))
    block_max = jnp.max(masked, axis=2)
    exponent = jnp.where(visible, jnp.exp(masked - block_max[..., None]), jnp.float32(0.0))
    guarded = jnp.maximum(jnp.sum(exponent, axis=2), 1.0)
    log_total = block_max + jnp.log(guarded)
    weights = (exponent / guarded[..., None]).astype(jnp.bfloat16)
    partial_value = jnp.einsum("bht,btc->bhc", weights, cache, preferred_element_type=jnp.float32)[
        ..., :latent
    ]
    blocks = partial_value.reshape(batch, groups, heads_dev, latent)
    block_logs = log_total.reshape(batch, groups, heads_dev)
    part_blocks = lax.all_to_all(
        blocks.astype(jnp.bfloat16), "kvp", split_axis=1, concat_axis=1, tiled=True
    ).astype(blocks.dtype)
    part_logs = lax.all_to_all(block_logs, "kvp", split_axis=1, concat_axis=1, tiled=True)
    highest = jnp.max(part_logs, axis=1)
    overall = highest + jnp.log(jnp.sum(jnp.exp(part_logs - highest[:, None, :]), axis=1))
    scaled = jnp.exp(part_logs - overall[:, None, :])[..., None] * part_blocks
    o_lat = jnp.sum(scaled, axis=1).astype(jnp.bfloat16)
    attention = project(o_lat, w_uv, w_out)
    model_width = norm_gain.shape[0]
    share_width = model_width // lax.axis_size(("kvp", "tp"))
    share_start = lax.axis_index(("kvp", "tp")) * share_width
    attn_whole = lax.psum(attention, ("kvp", "tp"))
    residual = hidden_in.astype(jnp.float32) + attn_whole
    mean_square = jnp.mean(residual * residual, axis=1)
    normed = (residual * lax.rsqrt(mean_square + 1e-06)[:, None] * norm_gain[None, :]).astype(
        jnp.bfloat16
    )
    residual_share = lax.dynamic_slice_in_dim(residual, share_start, share_width, 1)
    gate_proj = jnp.dot(normed, w_gate, preferred_element_type=jnp.float32)
    up_proj = jnp.dot(normed, w_up, preferred_element_type=jnp.float32)
    act = (jax.nn.silu(gate_proj) * up_proj).astype(jnp.bfloat16)
    ffn_terms = jnp.dot(act, w_down, preferred_element_type=jnp.float32)
    ffn_share = lax.psum_scatter(ffn_terms, ("kvp", "tp"), scatter_dimension=1, tiled=True)
    return (residual_share + ffn_share).astype(jnp.bfloat16)


MESH = pl.DeviceIdType.MESH
F32 = jnp.float32
BF16 = jnp.bfloat16
VMEM_BYTES = 67043328


SPAN = 2


def layer_kernel(
    groups, tps, share, chunk, out_rows, span,
    hidden_hbm, nope_hbm, rope_hbm, len_hbm, gain_hbm,
    cache_hbm, uk_hbm, uv_hbm, wo_hbm, wg_hbm, wu_hbm, wd_hbm,
    out_ref,
    hidden_v, nope_v, rope_v, len_v, gain_v, gain_s, hid_s,
    cache_v, uk_v, uv_v, big_v, gu_v,
    nope_s, qlat_s, score_s, weight_s, q_send, q_all, part_send, part_all, log_send, log_all,
    olat_s, head_s, own_s, rs_send, rs_all, ag_send, ag_all, fs_send, fs_all,
    in_sem, uk_sem, cache_sem, uv_sem, wo_sem, gu_sem, wd_sem,
    q_ss, q_rs, part_ss, part_rs, log_ss, log_rs, rs_ss, rs_rs, ag_ss, ag_rs, fs_ss, fs_rs, up_sem, down_sem,
):
    count = groups * tps
    kvp = lax.axis_index("kvp")
    tp = lax.axis_index("tp")
    me = kvp * tps + tp
    batch, heads, head_dim = nope_v.shape
    latent = uk_v.shape[2]
    rope = rope_v.shape[2]
    ctx = cache_v.shape[2]
    width = hidden_v.shape[1]
    chunks = width // chunk
    hidden_units = gu_v.shape[1] // 2
    parts = batch // span
    halves = tps // 2
    half = tp // 2
    chips = groups // 2

    def peer(index):
        return {"kvp": index // tps, "tp": lax.rem(index, tps)}

    def target_of(i):
        return lax.rem(kvp // 2 + i // 2, chips) * 2 + lax.rem(kvp + i, 2)

    near = [
        (target_of(i), lax.rem(half + e, halves)) for e in range(halves) for i in range(groups)
    ]
    far = near[::-1]
    planes = [tp, tp + 1 - 2 * lax.rem(tp, 2)]
    for e in range(1, halves):
        h = lax.rem(half + e, halves)
        p = (half - h + halves - 1) // halves
        planes += [2 * h + p, 2 * h + 1 - p]
    shares = [(target_of(i), z) for z in planes for i in range(groups)]
    bounds = [0, 2] + list(range(groups, count + 1, groups))
    segments = list(zip(bounds[:-1], bounds[1:]))

    def load(source, target, sem):
        return pltpu.make_async_copy(source, target, sem)

    def cols(j):
        return pl.ds(pl.multiple_of(j * chunk, 128), chunk)

    def side(t):
        return pl.ds((t % 2) * chunk, chunk)

    def load_wo(t):
        k, h = far[t]
        return load(
            wo_hbm.at[:, cols(k * halves + h)],
            big_v.at[t // 2, pl.ds(0, out_rows), side(t)],
            wo_sem,
        )

    def load_wd(t):
        k, h = far[t]
        return load(wd_hbm.at[:, cols(k * halves + h)], big_v.at[t // 2, :, side(t)], wd_sem.at[2 * t // chunks])

    def load_gu(n, t, segment):
        k, z = shares[t]
        rows = pl.ds(pl.multiple_of((k * tps + z) * share, math.gcd(share, 128)), share)
        return load(
            (wg_hbm, wu_hbm)[n].at[rows],
            gu_v.at[pl.ds(t * share, share), pl.ds(n * hidden_units, hidden_units)],
            gu_sem.at[segment],
        )

    def landed(ref, sem):
        pltpu.make_async_copy(ref, ref, sem).wait()

    def load_segment(segment):
        for t in range(*segments[segment]):
            load_gu(0, t, segment).start(priority=1)
            load_gu(1, t, segment).start(priority=1)

    small = [
        load(nope_hbm, nope_v, in_sem.at[0]),
        load(rope_hbm, rope_v, in_sem.at[1]),
        load(len_hbm, len_v, in_sem.at[2]),
        load(hidden_hbm, hidden_v, in_sem.at[3]),
        load(gain_hbm, gain_v.at[:, pl.ds(0, width)], in_sem.at[4]),
    ]
    uk_load = load(uk_hbm, uk_v, uk_sem)
    cache_load = load(cache_hbm, cache_v, cache_sem)
    uv_load = load(uv_hbm, uv_v, uv_sem)

    barrier = pltpu.get_barrier_semaphore()
    small[0].start()
    uk_load.start()
    small[1].start()

    below = {"kvp": kvp, "tp": lax.rem(tp + tps - 1, tps)}
    above = {"kvp": kvp, "tp": lax.rem(tp + 1, tps)}
    has_below, has_above = tp > 0, tp < tps - 1

    def greet(sem, device):
        pl.semaphore_signal(sem, inc=1, device_id=device, device_id_type=MESH)

    for i in range(1, groups):
        greet(barrier, {"kvp": target_of(i), "tp": tp})

    @pl.when(has_below)
    def _():
        greet(barrier, below)

    @pl.when(has_above)
    def _():
        greet(barrier, above)

    cache_load.start()
    for copy in small[2:]:
        copy.start()

    small[0].wait()
    nope_s[...] = nope_v[...].astype(F32)
    small[1].wait()
    base = 2 * latent
    for b in range(batch):
        first = base + (b % 2) * rope
        q_send[b // 2, :, first : first + rope] = rope_v[b]
    uk_load.wait()
    uv_load.start()
    for t in range(chunks):
        load_wo(t).start()
    for i in range(heads):
        qlat_s[:, i, :] = jnp.dot(
            nope_s[:, i, :].astype(BF16), uk_v[i], preferred_element_type=F32
        )
    for b in range(batch):
        first = (b % 2) * latent
        q_send[b // 2, :, first : first + latent] = qlat_s[b].astype(BF16)
    edges = (tps - tp - 1) // (tps - 1) + tp // (tps - 1)
    pl.semaphore_wait(barrier, groups + 1 - edges)

    def q_copy(i, u):
        other = target_of(i)
        return pltpu.make_async_remote_copy(
            src_ref=q_send.at[pl.ds(u * span // 2, span // 2)],
            dst_ref=q_all.at[kvp, pl.ds(u * span // 2, span // 2)],
            send_sem=q_ss,
            recv_sem=q_rs.at[u],
            device_id={"kvp": other, "tp": tp},
            device_id_type=MESH,
        )

    def part_copy(i, u):
        other = target_of(i)
        some = pl.ds(u * span, span)
        return pltpu.make_async_remote_copy(
            src_ref=part_send.at[other, some],
            dst_ref=part_all.at[kvp, some],
            send_sem=part_ss,
            recv_sem=part_rs.at[u],
            device_id={"kvp": other, "tp": tp},
            device_id_type=MESH,
        )

    def log_copy(i):
        other = target_of(i)
        return pltpu.make_async_remote_copy(
            src_ref=log_send.at[other],
            dst_ref=log_all.at[kvp],
            send_sem=log_ss,
            recv_sem=log_rs,
            device_id={"kvp": other, "tp": tp},
            device_id_type=MESH,
        )

    outward = list(range(2, groups)) + [1]
    for u in range(parts):
        for i in outward:
            q_copy(i, u).start()
    steps = chunks // 2
    early = len(segments) // 2 + 1
    for segment in range(early):
        load_segment(segment)
    def token(sem, arrives, leaves, device):
        @pl.when(arrives)
        def _():
            pl.semaphore_wait(sem, 1)

        @pl.when(leaves)
        def _():
            greet(sem, device)

    up = functools.partial(token, up_sem, has_below, has_above, above)
    down = functools.partial(token, down_sem, has_above, has_below, below)

    @pl.when(half < halves // 2)
    def _():
        up()
        down()

    @pl.when(half >= halves // 2)
    def _():
        down()
        up()

    q_all[kvp] = q_send[...]
    for copy in small[2:]:
        copy.wait()
    for n in range(count):
        piece = slice(n * share, (n + 1) * share)
        gain_s[n] = jnp.broadcast_to(gain_v[:, piece], (batch, share))
        hid_s[n] = hidden_v[:, piece].astype(F32)
    cache_load.wait()

    scale = float(head_dim + rope) ** (-0.5)
    rows = groups * heads
    position = kvp * ctx + lax.broadcasted_iota(jnp.int32, (rows, ctx), 1)
    lane = lax.broadcasted_iota(jnp.int32, (rows, 128), 1)
    logs_acc = jnp.zeros((rows, 128), F32)
    lengths = len_v[...]
    for u in range(parts):
        landed(q_all.at[pl.ds(0, groups - 1), pl.ds(u * span // 2, span // 2)], q_rs.at[u])
        some = range(u * span, (u + 1) * span)
        for b in some:
            lat = (b % 2) * latent
            rot = base + (b % 2) * rope
            q_lat = q_all[:, b // 2, :, lat : lat + latent].astype(F32).reshape(rows, latent)
            q_rot = q_all[:, b // 2, :, rot : rot + rope].astype(F32).reshape(rows, rope)
            score_s[b] = (
                jnp.dot(q_lat.astype(BF16), cache_v[b, :latent], preferred_element_type=F32)
                + jnp.dot(q_rot.astype(BF16), cache_v[b, latent:], preferred_element_type=F32)
            ) * scale
        for b in some:
            visible = position < lengths[:, b : b + 1]
            masked = jnp.where(visible, score_s[b], F32(-1e30))
            top = jnp.max(masked, axis=1, keepdims=True)
            exps = jnp.where(visible, jnp.exp(masked - top), F32(0.0))
            guarded = jnp.maximum(jnp.sum(exps, axis=1, keepdims=True), 1.0)
            logs_acc = jnp.where(lane == b, top + jnp.log(guarded), logs_acc)
            weight_s[b] = (exps / guarded).astype(BF16)
        for b in some:
            part = lax.dot_general(
                weight_s[b], cache_v[b, :latent], (((1,), (1,)), ((), ())),
                preferred_element_type=F32,
            )
            for g in range(groups):
                part_send[g, b] = part[g * heads : (g + 1) * heads].astype(BF16)
        for i in outward:
            part_copy(i, u).start()
    for g in range(groups):
        log_send[g] = logs_acc[g * heads : (g + 1) * heads]
    for i in outward:
        log_copy(i).start()
    for segment in range(early, len(segments)):
        load_segment(segment)
    part_all[kvp] = part_send[kvp]
    log_all[kvp] = log_send[kvp]
    uv_load.wait()
    landed(big_v.at[:, pl.ds(0, out_rows)], wo_sem)
    landed(log_all.at[pl.ds(0, groups - 1)], log_rs)
    logs = [log_all[g] for g in range(groups)]
    highest = functools.reduce(jnp.maximum, logs)
    overall = highest + jnp.log(sum(jnp.exp(x - highest) for x in logs))
    factors = [jnp.exp(x - overall) for x in logs]
    for u in range(parts):
        landed(part_all.at[pl.ds(0, groups - 1), pl.ds(u * span, span)], part_rs.at[u])
        for b in range(u * span, (u + 1) * span):
            olat_s[b] = sum(
                factors[g][:, b : b + 1] * part_all[g, b].astype(F32) for g in range(groups)
            )
    for i in range(heads):
        head_s[:, i * head_dim : (i + 1) * head_dim] = jnp.dot(
            olat_s[:, i, :].astype(BF16), uv_v[i], preferred_element_type=F32
        ).astype(BF16)

    def scatter_sum(lhs, depth, total, send, arrived, ss, rs, after):
        def copy(n, k, z):
            return pltpu.make_async_remote_copy(
                src_ref=send.at[n],
                dst_ref=arrived.at[me],
                send_sem=ss,
                recv_sem=rs,
                device_id={"kvp": k, "tp": z},
                device_id_type=MESH,
            )

        for s in range(steps):
            both = jnp.dot(lhs, big_v[s, :depth], preferred_element_type=F32)
            after(s)
            for t in (2 * s, 2 * s + 1):
                k, h = far[t]
                pieces = [
                    both[:, n * share : (n + 1) * share] for n in (2 * (t % 2), 2 * (t % 2) + 1)
                ]
                for p in range(2):
                    send[2 * t + p] = pieces[p].astype(BF16)
                if t < chunks - 1:
                    p = (h - half + halves) // halves
                    copy(2 * t + p, k, 2 * h + p).start()
                    copy(2 * t + 1 - p, k, 2 * h + 1 - p).start()
                else:
                    for p in range(2):
                        total = total + jnp.where(lax.rem(tp, 2) == p, pieces[p], F32(0.0))

                        @pl.when(lax.rem(tp, 2) != p)
                        def _():
                            copy(2 * t + p, k, 2 * h + p).start()

        landed(arrived.at[pl.ds(0, count - 1)], rs)
        for d in range(1, count):
            total = total + arrived[lax.rem(me + d, count)].astype(F32)
        return total

    def reload(s):
        load_wd(2 * s).start(priority=1)
        load_wd(2 * s + 1).start(priority=1)

    residual = scatter_sum(
        head_s[...], out_rows, hid_s[me], rs_send, rs_all, rs_ss, rs_rs, reload
    )
    own_s[...] = residual
    ag_send[...] = residual.astype(BF16)
    for t in range(1, count):
        k, z = shares[t]
        pltpu.make_async_remote_copy(
            src_ref=ag_send,
            dst_ref=ag_all.at[me],
            send_sem=ag_ss,
            recv_sem=ag_rs.at[0 if t < 2 else 1 if t < groups else 2 + tp],
            device_id={"kvp": k, "tp": z},
            device_id_type=MESH,
        ).start()
    ag_all[me] = ag_send[...]

    square = jnp.zeros((batch, 1), F32)
    for segment in range(len(segments)):
        landed(
            gu_v.at[pl.ds(segments[segment][0] * share, (segments[segment][1] - segments[segment][0]) * share)],
            gu_sem.at[segment],
        )
    products = jnp.zeros((batch, 2 * hidden_units), F32)
    for segment, (low, high) in enumerate(segments):
        came = high - low - (segment == 0)
        landed(
            ag_all.at[pl.ds(0, came)],
            ag_rs.at[segment if segment < 2 else 2 + planes[segment - 1]],
        )
        x = []
        for k, z in shares[low:high]:
            value = ag_all[k * tps + z].astype(F32)
            square = square + jnp.sum(value * value, axis=1, keepdims=True)
            x.append((value * gain_s[k * tps + z]).astype(BF16))
        products = products + jnp.dot(
            jnp.concatenate(x, axis=1),
            gu_v[low * share : high * share],
            preferred_element_type=F32,
        )
    products = products * lax.rsqrt(square / width + 1e-06)
    gate, up = products[:, :hidden_units], products[:, hidden_units:]
    act = (gate / (1.0 + jnp.exp(-gate)) * up).astype(BF16)

    for s in range(2):
        landed(big_v.at[pl.ds(s * steps // 2, steps // 2)], wd_sem.at[s])
    total = scatter_sum(
        act, big_v.shape[1], own_s[...], fs_send, fs_all, fs_ss, fs_rs, lambda s: None
    )
    out_ref[...] = total.astype(BF16)

    others = pl.ds(0, groups - 1)
    landed(q_all.at[others], q_ss)
    landed(part_all.at[others], part_ss)
    landed(log_all.at[others], log_ss)
    everyone = pl.ds(0, count - 1)
    landed(rs_all.at[everyone], rs_ss)
    landed(ag_all.at[everyone], ag_ss)
    landed(fs_all.at[everyone], fs_ss)


def per_device(*operands):
    (hidden_in, queries_nope, queries_rope, cache, lengths, w_uk, w_uv, w_out, norm_gain,
     w_gate, w_up, w_down) = operands
    groups, tps = lax.axis_size("kvp"), lax.axis_size("tp")
    count = groups * tps
    batch, heads, head_dim = queries_nope.shape
    latent, rope, ctx = w_uk.shape[2], queries_rope.shape[2], cache.shape[1]
    width = hidden_in.shape[1]
    share = width // count
    ff = w_gate.shape[1]
    rows = w_out.shape[0]
    chunk = 2 * share
    held = (w_gate.size + w_up.size + max(rows, ff) * width + cache.size + w_uk.size + w_uv.size) * 2
    fits = (
        batch % 8 == 0
        and heads % 8 == 0
        and all(size % 128 == 0 for size in (head_dim, latent, 2 * rope, ctx, chunk, ff))
        and groups % 2 == 0
        and tps % 4 == 0
        and batch <= 128
        and rows <= ff
        and held < VMEM_BYTES - 8 * 2**20
    )
    if not fits:
        return plain_device(*operands)
    chunks = width // chunk
    pairs = batch // 2
    parts = batch // SPAN
    dma = pltpu.SemaphoreType.DMA
    vmem = pl.BlockSpec(memory_space=pltpu.VMEM)
    anywhere = pl.BlockSpec(memory_space=pl.ANY)
    packed = 2 * (latent + rope)
    spread = pltpu.VMEM((count, batch, share), BF16)
    scratch = [
        pltpu.VMEM((batch, width), BF16),
        pltpu.VMEM((batch, heads, head_dim), BF16),
        pltpu.VMEM((batch, heads, rope), BF16),
        pltpu.VMEM((1, batch), jnp.int32),
        pltpu.VMEM((1, width + 1024), F32),
        pltpu.VMEM((count, batch, share), F32),
        pltpu.VMEM((count, batch, share), F32),
        pltpu.VMEM((batch, latent + rope, ctx), BF16),
        pltpu.VMEM(w_uk.shape, BF16),
        pltpu.VMEM(w_uv.shape, BF16),
        pltpu.VMEM((chunks // 2, ff, 2 * chunk), BF16),
        pltpu.VMEM((width, 2 * ff), BF16),
        pltpu.VMEM((batch, heads, head_dim), F32),
        pltpu.VMEM((batch, heads, latent), F32),
        pltpu.VMEM((batch, groups * heads, ctx), F32),
        pltpu.VMEM((batch, groups * heads, ctx), BF16),
        pltpu.VMEM((pairs, heads, packed), BF16),
        pltpu.VMEM((groups, pairs, heads, packed), BF16),
        pltpu.VMEM((groups, batch, heads, latent), BF16),
        pltpu.VMEM((groups, batch, heads, latent), BF16),
        pltpu.VMEM((groups, heads, 128), F32),
        pltpu.VMEM((groups, heads, 128), F32),
        pltpu.VMEM((batch, heads, latent), F32),
        pltpu.VMEM((batch, heads * head_dim), BF16),
        pltpu.VMEM((batch, share), F32),
        spread, spread, pltpu.VMEM((batch, share), BF16), spread, spread, spread,
        dma((5,)), dma, dma, dma,
        dma, dma((tps + 1,)), dma((2,)),
        dma, dma((parts,)), dma, dma((parts,)), dma, dma,
        dma, dma, dma, dma((tps + 2,)), dma, dma,
        pltpu.SemaphoreType.REGULAR, pltpu.SemaphoreType.REGULAR,
    ]
    return pl.pallas_call(
        functools.partial(layer_kernel, groups, tps, share, chunk, rows, SPAN),
        out_shape=pltpu.VMEM((batch, share), BF16),
        in_specs=[anywhere] * 12,
        out_specs=vmem,
        scratch_shapes=scratch,
        compiler_params=pltpu.CompilerParams(
            collective_id=0, has_side_effects=True, vmem_limit_bytes=VMEM_BYTES - 640 * 1024
        ),
    )(
        hidden_in, queries_nope, queries_rope, lengths.reshape(1, batch), norm_gain.reshape(1, width),
        jnp.swapaxes(cache, 1, 2), w_uk, w_uv, w_out, w_gate, w_up, w_down,
    )


def solution(mesh):
    placed = (
        P("grp", None),
        P("grp", ("kvp", "tp"), None),
        P("grp", ("kvp", "tp"), None),
        P("grp", "kvp", None),
        P("grp"),
        P(("kvp", "tp"), None, None),
        P(("kvp", "tp"), None, None),
        P(("kvp", "tp"), None),
        P(),
        P(None, ("kvp", "tp")),
        P(None, ("kvp", "tp")),
        P(("kvp", "tp"), None),
    )
    return jax.shard_map(
        per_device, mesh=mesh, in_specs=placed, out_specs=P("grp", ("kvp", "tp")), check_vma=False
    )
```

```python
import functools
import math

import jax
import jax.numpy as jnp
from jax import lax
from jax.experimental import pallas as pl
from jax.experimental.pallas import tpu as pltpu
from jax.sharding import PartitionSpec as P


def project(o_lat, w_uv, w_out):
    head_out = jnp.einsum("bhl,hle->bhe", o_lat, w_uv, preferred_element_type=jnp.float32).astype(
        jnp.bfloat16
    )
    return jnp.dot(
        head_out.reshape(head_out.shape[0], -1), w_out, preferred_element_type=jnp.float32
    )


def plain_device(
    hidden_in,
    queries_nope,
    queries_rope,
    cache,
    lengths,
    w_uk,
    w_uv,
    w_out,
    norm_gain,
    w_gate,
    w_up,
    w_down,
):
    batch, heads_dev, head_dim = queries_nope.shape
    latent = w_uk.shape[2]
    ctx_dev = cache.shape[1]
    groups = lax.axis_size("kvp")
    score_scale = float(head_dim + queries_rope.shape[2]) ** (-0.5)
    q_lat = jnp.einsum(
        "bhd,hdl->bhl", queries_nope, w_uk, preferred_element_type=jnp.float32
    ).astype(jnp.bfloat16)
    q_lat_all, rope_all = (
        lax.all_gather(q_lat, "kvp", axis=1, tiled=True),
        lax.all_gather(queries_rope, "kvp", axis=1, tiled=True),
    )
    q_full = jnp.concatenate([q_lat_all, rope_all], axis=2)
    scores = (
        jnp.einsum("bhc,btc->bht", q_full, cache, preferred_element_type=jnp.float32) * score_scale
    )
    offset = lax.axis_index("kvp") * ctx_dev
    visible = ((offset + jnp.arange(ctx_dev, dtype=jnp.int32))[None, :] < lengths[:, None])[
        :, None, :
    ]
    masked = jnp.where(visible, scores, jnp.float32(-1e30))
    block_max = jnp.max(masked, axis=2)
    exponent = jnp.where(visible, jnp.exp(masked - block_max[..., None]), jnp.float32(0.0))
    guarded = jnp.maximum(jnp.sum(exponent, axis=2), 1.0)
    log_total = block_max + jnp.log(guarded)
    weights = (exponent / guarded[..., None]).astype(jnp.bfloat16)
    partial_value = jnp.einsum("bht,btc->bhc", weights, cache, preferred_element_type=jnp.float32)[
        ..., :latent
    ]
    blocks = partial_value.reshape(batch, groups, heads_dev, latent)
    block_logs = log_total.reshape(batch, groups, heads_dev)
    part_blocks = lax.all_to_all(
        blocks.astype(jnp.bfloat16), "kvp", split_axis=1, concat_axis=1, tiled=True
    ).astype(blocks.dtype)
    part_logs = lax.all_to_all(block_logs, "kvp", split_axis=1, concat_axis=1, tiled=True)
    highest = jnp.max(part_logs, axis=1)
    overall = highest + jnp.log(jnp.sum(jnp.exp(part_logs - highest[:, None, :]), axis=1))
    scaled = jnp.exp(part_logs - overall[:, None, :])[..., None] * part_blocks
    o_lat = jnp.sum(scaled, axis=1).astype(jnp.bfloat16)
    attention = project(o_lat, w_uv, w_out)
    model_width = norm_gain.shape[0]
    share_width = model_width // lax.axis_size(("kvp", "tp"))
    share_start = lax.axis_index(("kvp", "tp")) * share_width
    attn_whole = lax.psum(attention, ("kvp", "tp"))
    residual = hidden_in.astype(jnp.float32) + attn_whole
    mean_square = jnp.mean(residual * residual, axis=1)
    normed = (residual * lax.rsqrt(mean_square + 1e-06)[:, None] * norm_gain[None, :]).astype(
        jnp.bfloat16
    )
    residual_share = lax.dynamic_slice_in_dim(residual, share_start, share_width, 1)
    gate_proj = jnp.dot(normed, w_gate, preferred_element_type=jnp.float32)
    up_proj = jnp.dot(normed, w_up, preferred_element_type=jnp.float32)
    act = (jax.nn.silu(gate_proj) * up_proj).astype(jnp.bfloat16)
    ffn_terms = jnp.dot(act, w_down, preferred_element_type=jnp.float32)
    ffn_share = lax.psum_scatter(ffn_terms, ("kvp", "tp"), scatter_dimension=1, tiled=True)
    return (residual_share + ffn_share).astype(jnp.bfloat16)


MESH = pl.DeviceIdType.MESH
F32 = jnp.float32
BF16 = jnp.bfloat16
VMEM_BYTES = 67043328


SPAN = 2


def layer_kernel(
    groups, tps, share, chunk, out_rows, span,
    hidden_hbm, nope_hbm, rope_hbm, len_hbm, gain_hbm,
    cache_hbm, uk_hbm, uv_hbm, wo_hbm, wg_hbm, wu_hbm, wd_hbm,
    out_ref,
    hidden_v, nope_v, rope_v, len_v, gain_v, gain_s, hid_s,
    cache_v, uk_v, uv_v, big_v, gu_v,
    nope_s, qlat_s, score_s, weight_s, q_send, q_all, part_send, part_all, log_send, log_all,
    olat_s, head_s, own_s, rs_send, rs_all, ag_send, ag_all, fs_send, fs_all,
    in_sem, uk_sem, cache_sem, uv_sem, wo_sem, gu_sem, wd_sem,
    q_ss, q_rs, part_ss, part_rs, log_ss, log_rs, rs_ss, rs_rs, ag_ss, ag_rs, fs_ss, fs_rs, up_sem, down_sem,
):
    count = groups * tps
    kvp = lax.axis_index("kvp")
    tp = lax.axis_index("tp")
    me = kvp * tps + tp
    batch, heads, head_dim = nope_v.shape
    latent = uk_v.shape[2]
    rope = rope_v.shape[2]
    ctx = cache_v.shape[2]
    width = hidden_v.shape[1]
    chunks = width // chunk
    hidden_units = gu_v.shape[1] // 2
    parts = batch // span
    halves = tps // 2
    half = tp // 2
    chips = groups // 2

    def peer(index):
        return {"kvp": index // tps, "tp": lax.rem(index, tps)}

    def target_of(i):
        return lax.rem(kvp // 2 + i // 2, chips) * 2 + lax.rem(kvp + i, 2)

    near = [
        (target_of(i), lax.rem(half + e, halves)) for e in range(halves) for i in range(groups)
    ]
    far = near[::-1]
    planes = [tp, tp + 1 - 2 * lax.rem(tp, 2)]
    for e in range(1, halves):
        h = lax.rem(half + e, halves)
        p = (half - h + halves - 1) // halves
        planes += [2 * h + p, 2 * h + 1 - p]
    shares = [(target_of(i), z) for z in planes for i in range(groups)]
    bounds = [0, 2] + list(range(2 * groups, count + 1, 2 * groups))
    segments = list(zip(bounds[:-1], bounds[1:]))

    def load(source, target, sem):
        return pltpu.make_async_copy(source, target, sem)

    def cols(j):
        return pl.ds(pl.multiple_of(j * chunk, 128), chunk)

    def side(t):
        return pl.ds((t % 2) * chunk, chunk)

    def load_wo(t):
        k, h = far[t]
        return load(
            wo_hbm.at[:, cols(k * halves + h)],
            big_v.at[t // 2, pl.ds(0, out_rows), side(t)],
            wo_sem,
        )

    def load_wd(t):
        k, h = far[t]
        return load(wd_hbm.at[:, cols(k * halves + h)], big_v.at[t // 2, :, side(t)], wd_sem.at[2 * t // chunks])

    def load_gu(n, t, segment):
        k, z = shares[t]
        rows = pl.ds(pl.multiple_of((k * tps + z) * share, math.gcd(share, 128)), share)
        return load(
            (wg_hbm, wu_hbm)[n].at[rows],
            gu_v.at[pl.ds(t * share, share), pl.ds(n * hidden_units, hidden_units)],
            gu_sem.at[segment],
        )

    def landed(ref, sem):
        pltpu.make_async_copy(ref, ref, sem).wait()

    def load_segment(segment):
        for t in range(*segments[segment]):
            load_gu(0, t, segment).start(priority=1)
            load_gu(1, t, segment).start(priority=1)

    small = [
        load(nope_hbm, nope_v, in_sem.at[0]),
        load(rope_hbm, rope_v, in_sem.at[1]),
        load(len_hbm, len_v, in_sem.at[2]),
        load(hidden_hbm, hidden_v, in_sem.at[3]),
        load(gain_hbm, gain_v.at[:, pl.ds(0, width)], in_sem.at[4]),
    ]
    uk_load = load(uk_hbm, uk_v, uk_sem)
    cache_load = load(cache_hbm, cache_v, cache_sem)
    uv_load = load(uv_hbm, uv_v, uv_sem)

    barrier = pltpu.get_barrier_semaphore()
    small[0].start()
    uk_load.start()
    small[1].start()

    below = {"kvp": kvp, "tp": lax.rem(tp + tps - 1, tps)}
    above = {"kvp": kvp, "tp": lax.rem(tp + 1, tps)}
    has_below, has_above = tp > 0, tp < tps - 1

    def greet(sem, device):
        pl.semaphore_signal(sem, inc=1, device_id=device, device_id_type=MESH)

    for i in range(1, groups):
        greet(barrier, {"kvp": target_of(i), "tp": tp})

    @pl.when(has_below)
    def _():
        greet(barrier, below)

    @pl.when(has_above)
    def _():
        greet(barrier, above)

    cache_load.start()
    for copy in small[2:]:
        copy.start()

    small[0].wait()
    nope_s[...] = nope_v[...].astype(F32)
    small[1].wait()
    base = 2 * latent
    for b in range(batch):
        first = base + (b % 2) * rope
        q_send[b // 2, :, first : first + rope] = rope_v[b]
    uk_load.wait()
    uv_load.start()
    for t in range(chunks):
        load_wo(t).start()
    for i in range(heads):
        qlat_s[:, i, :] = jnp.dot(
            nope_s[:, i, :].astype(BF16), uk_v[i], preferred_element_type=F32
        )
    for b in range(batch):
        first = (b % 2) * latent
        q_send[b // 2, :, first : first + latent] = qlat_s[b].astype(BF16)
    edges = (tps - tp - 1) // (tps - 1) + tp // (tps - 1)
    pl.semaphore_wait(barrier, groups + 1 - edges)

    def q_copy(i, u):
        other = target_of(i)
        return pltpu.make_async_remote_copy(
            src_ref=q_send.at[pl.ds(u * span // 2, span // 2)],
            dst_ref=q_all.at[kvp, pl.ds(u * span // 2, span // 2)],
            send_sem=q_ss,
            recv_sem=q_rs.at[u],
            device_id={"kvp": other, "tp": tp},
            device_id_type=MESH,
        )

    def part_copy(i, u):
        other = target_of(i)
        some = pl.ds(u * span, span)
        return pltpu.make_async_remote_copy(
            src_ref=part_send.at[other, some],
            dst_ref=part_all.at[kvp, some],
            send_sem=part_ss,
            recv_sem=part_rs.at[u],
            device_id={"kvp": other, "tp": tp},
            device_id_type=MESH,
        )

    def log_copy(i):
        other = target_of(i)
        return pltpu.make_async_remote_copy(
            src_ref=log_send.at[other],
            dst_ref=log_all.at[kvp],
            send_sem=log_ss,
            recv_sem=log_rs,
            device_id={"kvp": other, "tp": tp},
            device_id_type=MESH,
        )

    outward = list(range(2, groups)) + [1]
    for u in range(parts):
        for i in outward:
            q_copy(i, u).start()
    steps = chunks // 2
    early = len(segments) // 2 + 1
    for segment in range(early):
        load_segment(segment)
    def token(sem, arrives, leaves, device):
        @pl.when(arrives)
        def _():
            pl.semaphore_wait(sem, 1)

        @pl.when(leaves)
        def _():
            greet(sem, device)

    up = functools.partial(token, up_sem, has_below, has_above, above)
    down = functools.partial(token, down_sem, has_above, has_below, below)

    @pl.when(half < halves // 2)
    def _():
        up()
        down()

    @pl.when(half >= halves // 2)
    def _():
        down()
        up()

    q_all[kvp] = q_send[...]
    for copy in small[2:]:
        copy.wait()
    for n in range(count):
        piece = slice(n * share, (n + 1) * share)
        gain_s[n] = jnp.broadcast_to(gain_v[:, piece], (batch, share))
        hid_s[n] = hidden_v[:, piece].astype(F32)
    cache_load.wait()

    scale = float(head_dim + rope) ** (-0.5)
    rows = groups * heads
    position = kvp * ctx + lax.broadcasted_iota(jnp.int32, (rows, ctx), 1)
    lane = lax.broadcasted_iota(jnp.int32, (rows, 128), 1)
    logs_acc = jnp.zeros((rows, 128), F32)
    lengths = len_v[...]
    for u in range(parts):
        landed(q_all.at[pl.ds(0, groups - 1), pl.ds(u * span // 2, span // 2)], q_rs.at[u])
        some = range(u * span, (u + 1) * span)
        for b in some:
            lat = (b % 2) * latent
            rot = base + (b % 2) * rope
            q_lat = q_all[:, b // 2, :, lat : lat + latent].astype(F32).reshape(rows, latent)
            q_rot = q_all[:, b // 2, :, rot : rot + rope].astype(F32).reshape(rows, rope)
            score_s[b] = (
                jnp.dot(q_lat.astype(BF16), cache_v[b, :latent], preferred_element_type=F32)
                + jnp.dot(q_rot.astype(BF16), cache_v[b, latent:], preferred_element_type=F32)
            ) * scale
        for b in some:
            visible = position < lengths[:, b : b + 1]
            masked = jnp.where(visible, score_s[b], F32(-1e30))
            top = jnp.max(masked, axis=1, keepdims=True)
            exps = jnp.where(visible, jnp.exp(masked - top), F32(0.0))
            guarded = jnp.maximum(jnp.sum(exps, axis=1, keepdims=True), 1.0)
            logs_acc = jnp.where(lane == b, top + jnp.log(guarded), logs_acc)
            weight_s[b] = (exps / guarded).astype(BF16)
        for b in some:
            part = lax.dot_general(
                weight_s[b], cache_v[b, :latent], (((1,), (1,)), ((), ())),
                preferred_element_type=F32,
            )
            for g in range(groups):
                part_send[g, b] = part[g * heads : (g + 1) * heads].astype(BF16)
        for i in outward:
            part_copy(i, u).start()
    for g in range(groups):
        log_send[g] = logs_acc[g * heads : (g + 1) * heads]
    for i in outward:
        log_copy(i).start()
    for segment in range(early, len(segments)):
        load_segment(segment)
    part_all[kvp] = part_send[kvp]
    log_all[kvp] = log_send[kvp]
    uv_load.wait()
    landed(big_v.at[:, pl.ds(0, out_rows)], wo_sem)
    landed(log_all.at[pl.ds(0, groups - 1)], log_rs)
    logs = [log_all[g] for g in range(groups)]
    highest = functools.reduce(jnp.maximum, logs)
    overall = highest + jnp.log(sum(jnp.exp(x - highest) for x in logs))
    factors = [jnp.exp(x - overall) for x in logs]
    for u in range(parts):
        landed(part_all.at[pl.ds(0, groups - 1), pl.ds(u * span, span)], part_rs.at[u])
        for b in range(u * span, (u + 1) * span):
            olat_s[b] = sum(
                factors[g][:, b : b + 1] * part_all[g, b].astype(F32) for g in range(groups)
            )
    for i in range(heads):
        head_s[:, i * head_dim : (i + 1) * head_dim] = jnp.dot(
            olat_s[:, i, :].astype(BF16), uv_v[i], preferred_element_type=F32
        ).astype(BF16)

    def scatter_sum(lhs, depth, total, send, arrived, ss, rs, after):
        def copy(n, k, z):
            return pltpu.make_async_remote_copy(
                src_ref=send.at[n],
                dst_ref=arrived.at[me],
                send_sem=ss,
                recv_sem=rs,
                device_id={"kvp": k, "tp": z},
                device_id_type=MESH,
            )

        run = steps // halves
        for e in range(halves):
            blocks = range(e * run, (e + 1) * run)
            terms = [
                jnp.dot(lhs, big_v[s, :depth], preferred_element_type=F32) for s in blocks
            ]
            for s, term in zip(blocks, terms):
                for n in range(4):
                    piece = term[:, n * share : (n + 1) * share]
                    send[4 * s + n] = piece.astype(BF16)
                    if 4 * s + n >= count - 2:
                        total = total + jnp.where(lax.rem(tp, 2) == n % 2, piece, F32(0.0))
            for s in blocks:
                for t in (2 * s, 2 * s + 1):
                    k, h = far[t]
                    if t < chunks - 1:
                        p = (h - half + halves) // halves
                        copy(2 * t + p, k, 2 * h + p).start()
                        copy(2 * t + 1 - p, k, 2 * h + 1 - p).start()
                    else:
                        n = 2 * t + 1 - lax.rem(tp, 2)
                        copy(n, k, tp + 1 - 2 * lax.rem(tp, 2)).start()
            for s in blocks:
                after(s)

        landed(arrived.at[pl.ds(0, count - 1)], rs)
        for d in range(1, count):
            total = total + arrived[lax.rem(me + d, count)].astype(F32)
        return total

    def reload(s):
        load_wd(2 * s).start(priority=1)
        load_wd(2 * s + 1).start(priority=1)

    residual = scatter_sum(
        head_s[...], out_rows, hid_s[me], rs_send, rs_all, rs_ss, rs_rs, reload
    )
    own_s[...] = residual
    ag_send[...] = residual.astype(BF16)
    for t in range(1, count):
        k, z = shares[t]
        pltpu.make_async_remote_copy(
            src_ref=ag_send,
            dst_ref=ag_all.at[me],
            send_sem=ag_ss,
            recv_sem=ag_rs.at[0 if t < 2 else 1 if t < groups else 2 + tp],
            device_id={"kvp": k, "tp": z},
            device_id_type=MESH,
        ).start()
    ag_all[me] = ag_send[...]

    square = jnp.zeros((batch, 1), F32)
    products = jnp.zeros((batch, 2 * hidden_units), F32)
    for segment, (low, high) in enumerate(segments):
        landed(gu_v.at[pl.ds(low * share, (high - low) * share)], gu_sem.at[segment])
        if segment == 0:
            landed(ag_all.at[pl.ds(0, 1)], ag_rs.at[0])
        if segment == 1:
            landed(ag_all.at[pl.ds(0, groups - 2)], ag_rs.at[1])
        for n in range(tps):
            if n and low <= n * groups < high:
                landed(ag_all.at[pl.ds(0, groups)], ag_rs.at[2 + planes[n]])
        x = []
        for k, z in shares[low:high]:
            value = ag_all[k * tps + z].astype(F32)
            square = square + jnp.sum(value * value, axis=1, keepdims=True)
            x.append((value * gain_s[k * tps + z]).astype(BF16))
        products = products + jnp.dot(
            jnp.concatenate(x, axis=1),
            gu_v[low * share : high * share],
            preferred_element_type=F32,
        )
    products = products * lax.rsqrt(square / width + 1e-06)
    gate, up = products[:, :hidden_units], products[:, hidden_units:]
    act = (gate / (1.0 + jnp.exp(-gate)) * up).astype(BF16)

    for s in range(2):
        landed(big_v.at[pl.ds(s * steps // 2, steps // 2)], wd_sem.at[s])
    total = scatter_sum(
        act, big_v.shape[1], own_s[...], fs_send, fs_all, fs_ss, fs_rs, lambda s: None
    )
    out_ref[...] = total.astype(BF16)

    others = pl.ds(0, groups - 1)
    landed(q_all.at[others], q_ss)
    landed(part_all.at[others], part_ss)
    landed(log_all.at[others], log_ss)
    everyone = pl.ds(0, count - 1)
    landed(rs_all.at[everyone], rs_ss)
    landed(ag_all.at[everyone], ag_ss)
    landed(fs_all.at[everyone], fs_ss)


def per_device(*operands):
    (hidden_in, queries_nope, queries_rope, cache, lengths, w_uk, w_uv, w_out, norm_gain,
     w_gate, w_up, w_down) = operands
    groups, tps = lax.axis_size("kvp"), lax.axis_size("tp")
    count = groups * tps
    batch, heads, head_dim = queries_nope.shape
    latent, rope, ctx = w_uk.shape[2], queries_rope.shape[2], cache.shape[1]
    width = hidden_in.shape[1]
    share = width // count
    ff = w_gate.shape[1]
    rows = w_out.shape[0]
    chunk = 2 * share
    held = (w_gate.size + w_up.size + max(rows, ff) * width + cache.size + w_uk.size + w_uv.size) * 2
    fits = (
        batch % 8 == 0
        and heads % 8 == 0
        and all(size % 128 == 0 for size in (head_dim, latent, 2 * rope, ctx, chunk, ff))
        and groups % 2 == 0
        and tps % 4 == 0
        and batch <= 128
        and rows <= ff
        and held < VMEM_BYTES - 8 * 2**20
    )
    if not fits:
        return plain_device(*operands)
    chunks = width // chunk
    pairs = batch // 2
    parts = batch // SPAN
    dma = pltpu.SemaphoreType.DMA
    vmem = pl.BlockSpec(memory_space=pltpu.VMEM)
    anywhere = pl.BlockSpec(memory_space=pl.ANY)
    packed = 2 * (latent + rope)
    spread = pltpu.VMEM((count, batch, share), BF16)
    scratch = [
        pltpu.VMEM((batch, width), BF16),
        pltpu.VMEM((batch, heads, head_dim), BF16),
        pltpu.VMEM((batch, heads, rope), BF16),
        pltpu.VMEM((1, batch), jnp.int32),
        pltpu.VMEM((1, width + 1024), F32),
        pltpu.VMEM((count, batch, share), F32),
        pltpu.VMEM((count, batch, share), F32),
        pltpu.VMEM((batch, latent + rope, ctx), BF16),
        pltpu.VMEM(w_uk.shape, BF16),
        pltpu.VMEM(w_uv.shape, BF16),
        pltpu.VMEM((chunks // 2, ff, 2 * chunk), BF16),
        pltpu.VMEM((width, 2 * ff), BF16),
        pltpu.VMEM((batch, heads, head_dim), F32),
        pltpu.VMEM((batch, heads, latent), F32),
        pltpu.VMEM((batch, groups * heads, ctx), F32),
        pltpu.VMEM((batch, groups * heads, ctx), BF16),
        pltpu.VMEM((pairs, heads, packed), BF16),
        pltpu.VMEM((groups, pairs, heads, packed), BF16),
        pltpu.VMEM((groups, batch, heads, latent), BF16),
        pltpu.VMEM((groups, batch, heads, latent), BF16),
        pltpu.VMEM((groups, heads, 128), F32),
        pltpu.VMEM((groups, heads, 128), F32),
        pltpu.VMEM((batch, heads, latent), F32),
        pltpu.VMEM((batch, heads * head_dim), BF16),
        pltpu.VMEM((batch, share), F32),
        spread, spread, pltpu.VMEM((batch, share), BF16), spread, spread, spread,
        dma((5,)), dma, dma, dma,
        dma, dma((tps // 2 + 1,)), dma((2,)),
        dma, dma((parts,)), dma, dma((parts,)), dma, dma,
        dma, dma, dma, dma((tps + 2,)), dma, dma,
        pltpu.SemaphoreType.REGULAR, pltpu.SemaphoreType.REGULAR,
    ]
    return pl.pallas_call(
        functools.partial(layer_kernel, groups, tps, share, chunk, rows, SPAN),
        out_shape=pltpu.VMEM((batch, share), BF16),
        in_specs=[anywhere] * 12,
        out_specs=vmem,
        scratch_shapes=scratch,
        compiler_params=pltpu.CompilerParams(
            collective_id=0, has_side_effects=True, vmem_limit_bytes=VMEM_BYTES - 640 * 1024
        ),
    )(
        hidden_in, queries_nope, queries_rope, lengths.reshape(1, batch), norm_gain.reshape(1, width),
        jnp.swapaxes(cache, 1, 2), w_uk, w_uv, w_out, w_gate, w_up, w_down,
    )


def solution(mesh):
    placed = (
        P("grp", None),
        P("grp", ("kvp", "tp"), None),
        P("grp", ("kvp", "tp"), None),
        P("grp", "kvp", None),
        P("grp"),
        P(("kvp", "tp"), None, None),
        P(("kvp", "tp"), None, None),
        P(("kvp", "tp"), None),
        P(),
        P(None, ("kvp", "tp")),
        P(None, ("kvp", "tp")),
        P(("kvp", "tp"), None),
    )
    return jax.shard_map(
        per_device, mesh=mesh, in_specs=placed, out_specs=P("grp", ("kvp", "tp")), check_vma=False
    )
```

```python
import functools
import math

import jax
import jax.numpy as jnp
from jax import lax
from jax.experimental import pallas as pl
from jax.experimental.pallas import tpu as pltpu
from jax.sharding import PartitionSpec as P


def project(o_lat, w_uv, w_out):
    head_out = jnp.einsum("bhl,hle->bhe", o_lat, w_uv, preferred_element_type=jnp.float32).astype(
        jnp.bfloat16
    )
    return jnp.dot(
        head_out.reshape(head_out.shape[0], -1), w_out, preferred_element_type=jnp.float32
    )


def plain_device(
    hidden_in,
    queries_nope,
    queries_rope,
    cache,
    lengths,
    w_uk,
    w_uv,
    w_out,
    norm_gain,
    w_gate,
    w_up,
    w_down,
):
    batch, heads_dev, head_dim = queries_nope.shape
    latent = w_uk.shape[2]
    ctx_dev = cache.shape[1]
    groups = lax.axis_size("kvp")
    score_scale = float(head_dim + queries_rope.shape[2]) ** (-0.5)
    q_lat = jnp.einsum(
        "bhd,hdl->bhl", queries_nope, w_uk, preferred_element_type=jnp.float32
    ).astype(jnp.bfloat16)
    q_lat_all, rope_all = (
        lax.all_gather(q_lat, "kvp", axis=1, tiled=True),
        lax.all_gather(queries_rope, "kvp", axis=1, tiled=True),
    )
    q_full = jnp.concatenate([q_lat_all, rope_all], axis=2)
    scores = (
        jnp.einsum("bhc,btc->bht", q_full, cache, preferred_element_type=jnp.float32) * score_scale
    )
    offset = lax.axis_index("kvp") * ctx_dev
    visible = ((offset + jnp.arange(ctx_dev, dtype=jnp.int32))[None, :] < lengths[:, None])[
        :, None, :
    ]
    masked = jnp.where(visible, scores, jnp.float32(-1e30))
    block_max = jnp.max(masked, axis=2)
    exponent = jnp.where(visible, jnp.exp(masked - block_max[..., None]), jnp.float32(0.0))
    guarded = jnp.maximum(jnp.sum(exponent, axis=2), 1.0)
    log_total = block_max + jnp.log(guarded)
    weights = (exponent / guarded[..., None]).astype(jnp.bfloat16)
    partial_value = jnp.einsum("bht,btc->bhc", weights, cache, preferred_element_type=jnp.float32)[
        ..., :latent
    ]
    blocks = partial_value.reshape(batch, groups, heads_dev, latent)
    block_logs = log_total.reshape(batch, groups, heads_dev)
    part_blocks = lax.all_to_all(
        blocks.astype(jnp.bfloat16), "kvp", split_axis=1, concat_axis=1, tiled=True
    ).astype(blocks.dtype)
    part_logs = lax.all_to_all(block_logs, "kvp", split_axis=1, concat_axis=1, tiled=True)
    highest = jnp.max(part_logs, axis=1)
    overall = highest + jnp.log(jnp.sum(jnp.exp(part_logs - highest[:, None, :]), axis=1))
    scaled = jnp.exp(part_logs - overall[:, None, :])[..., None] * part_blocks
    o_lat = jnp.sum(scaled, axis=1).astype(jnp.bfloat16)
    attention = project(o_lat, w_uv, w_out)
    model_width = norm_gain.shape[0]
    share_width = model_width // lax.axis_size(("kvp", "tp"))
    share_start = lax.axis_index(("kvp", "tp")) * share_width
    attn_whole = lax.psum(attention, ("kvp", "tp"))
    residual = hidden_in.astype(jnp.float32) + attn_whole
    mean_square = jnp.mean(residual * residual, axis=1)
    normed = (residual * lax.rsqrt(mean_square + 1e-06)[:, None] * norm_gain[None, :]).astype(
        jnp.bfloat16
    )
    residual_share = lax.dynamic_slice_in_dim(residual, share_start, share_width, 1)
    gate_proj = jnp.dot(normed, w_gate, preferred_element_type=jnp.float32)
    up_proj = jnp.dot(normed, w_up, preferred_element_type=jnp.float32)
    act = (jax.nn.silu(gate_proj) * up_proj).astype(jnp.bfloat16)
    ffn_terms = jnp.dot(act, w_down, preferred_element_type=jnp.float32)
    ffn_share = lax.psum_scatter(ffn_terms, ("kvp", "tp"), scatter_dimension=1, tiled=True)
    return (residual_share + ffn_share).astype(jnp.bfloat16)


MESH = pl.DeviceIdType.MESH
F32 = jnp.float32
BF16 = jnp.bfloat16
VMEM_BYTES = 67043328


SPAN = 2


def layer_kernel(
    groups, tps, share, chunk, out_rows, span,
    hidden_hbm, nope_hbm, rope_hbm, len_hbm, gain_hbm,
    cache_hbm, uk_hbm, uv_hbm, wo_hbm, wg_hbm, wu_hbm, wd_hbm,
    out_ref,
    hidden_v, nope_v, rope_v, len_v, gain_v, gain_s, hid_s,
    cache_v, uk_v, uv_v, big_v, gu_v,
    nope_s, qlat_s, score_s, weight_s, q_send, q_all, part_send, part_all, log_send, log_all,
    olat_s, head_s, own_s, rs_send, rs_all, ag_send, ag_all, fs_send, fs_all,
    in_sem, uk_sem, cache_sem, uv_sem, wo_sem, gu_sem, wd_sem,
    q_ss, q_rs, part_ss, part_rs, log_ss, log_rs, rs_ss, rs_rs, ag_ss, ag_rs, fs_ss, fs_rs, up_sem, down_sem,
):
    count = groups * tps
    kvp = lax.axis_index("kvp")
    tp = lax.axis_index("tp")
    me = kvp * tps + tp
    batch, heads, head_dim = nope_v.shape
    latent = uk_v.shape[2]
    rope = rope_v.shape[2]
    ctx = cache_v.shape[2]
    width = hidden_v.shape[1]
    chunks = width // chunk
    hidden_units = gu_v.shape[1] // 2
    parts = batch // span
    halves = tps // 2
    half = tp // 2
    chips = groups // 2

    def peer(index):
        return {"kvp": index // tps, "tp": lax.rem(index, tps)}

    def target_of(i):
        return lax.rem(kvp // 2 + i // 2, chips) * 2 + lax.rem(kvp + i, 2)

    near = [
        (target_of(i), lax.rem(half + e, halves)) for e in range(halves) for i in range(groups)
    ]
    far = near[::-1]
    planes = [tp, tp + 1 - 2 * lax.rem(tp, 2)]
    for e in range(1, halves):
        h = lax.rem(half + e, halves)
        p = (half - h + halves - 1) // halves
        planes += [2 * h + p, 2 * h + 1 - p]
    shares = [(target_of(i), z) for z in planes for i in range(groups)]
    bounds = [0, 2] + list(range(groups, count + 1, groups))
    segments = list(zip(bounds[:-1], bounds[1:]))

    def load(source, target, sem):
        return pltpu.make_async_copy(source, target, sem)

    def cols(j):
        return pl.ds(pl.multiple_of(j * chunk, 128), chunk)

    def side(t):
        return pl.ds((t % groups) * chunk, chunk)

    def load_wo(t):
        k, h = far[t]
        return load(
            wo_hbm.at[:, cols(k * halves + h)],
            big_v.at[t // groups, pl.ds(0, out_rows), side(t)],
            wo_sem,
        )

    def load_wd(t):
        k, h = far[t]
        return load(wd_hbm.at[:, cols(k * halves + h)], big_v.at[t // groups, :, side(t)], wd_sem.at[2 * t // chunks])

    def load_gu(n, t, segment):
        k, z = shares[t]
        rows = pl.ds(pl.multiple_of((k * tps + z) * share, math.gcd(share, 128)), share)
        return load(
            (wg_hbm, wu_hbm)[n].at[rows],
            gu_v.at[pl.ds(t * share, share), pl.ds(n * hidden_units, hidden_units)],
            gu_sem.at[segment],
        )

    def landed(ref, sem):
        pltpu.make_async_copy(ref, ref, sem).wait()

    def load_segment(segment):
        for t in range(*segments[segment]):
            load_gu(0, t, segment).start(priority=1)
            load_gu(1, t, segment).start(priority=1)

    small = [
        load(nope_hbm, nope_v, in_sem.at[0]),
        load(rope_hbm, rope_v, in_sem.at[1]),
        load(len_hbm, len_v, in_sem.at[2]),
        load(hidden_hbm, hidden_v, in_sem.at[3]),
        load(gain_hbm, gain_v.at[:, pl.ds(0, width)], in_sem.at[4]),
    ]
    uk_load = load(uk_hbm, uk_v, uk_sem)
    cache_load = load(cache_hbm, cache_v, cache_sem)
    uv_load = load(uv_hbm, uv_v, uv_sem)

    barrier = pltpu.get_barrier_semaphore()
    small[0].start()
    uk_load.start()
    small[1].start()

    below = {"kvp": kvp, "tp": lax.rem(tp + tps - 1, tps)}
    above = {"kvp": kvp, "tp": lax.rem(tp + 1, tps)}
    has_below, has_above = tp > 0, tp < tps - 1

    def greet(sem, device):
        pl.semaphore_signal(sem, inc=1, device_id=device, device_id_type=MESH)

    for i in range(1, groups):
        greet(barrier, {"kvp": target_of(i), "tp": tp})

    @pl.when(has_below)
    def _():
        greet(barrier, below)

    @pl.when(has_above)
    def _():
        greet(barrier, above)

    cache_load.start()
    for copy in small[2:]:
        copy.start()

    small[0].wait()
    nope_s[...] = nope_v[...].astype(F32)
    small[1].wait()
    base = 2 * latent
    for b in range(batch):
        first = base + (b % 2) * rope
        q_send[b // 2, :, first : first + rope] = rope_v[b]
    uk_load.wait()
    uv_load.start()
    for t in range(chunks):
        load_wo(t).start()
    for i in range(heads):
        qlat_s[:, i, :] = jnp.dot(
            nope_s[:, i, :].astype(BF16), uk_v[i], preferred_element_type=F32
        )
    for b in range(batch):
        first = (b % 2) * latent
        q_send[b // 2, :, first : first + latent] = qlat_s[b].astype(BF16)
    edges = (tps - tp - 1) // (tps - 1) + tp // (tps - 1)
    pl.semaphore_wait(barrier, groups + 1 - edges)

    def q_copy(i, u):
        other = target_of(i)
        return pltpu.make_async_remote_copy(
            src_ref=q_send.at[pl.ds(u * span // 2, span // 2)],
            dst_ref=q_all.at[kvp, pl.ds(u * span // 2, span // 2)],
            send_sem=q_ss,
            recv_sem=q_rs.at[u],
            device_id={"kvp": other, "tp": tp},
            device_id_type=MESH,
        )

    def part_copy(i, u):
        other = target_of(i)
        some = pl.ds(u * span, span)
        return pltpu.make_async_remote_copy(
            src_ref=part_send.at[other, some],
            dst_ref=part_all.at[kvp, some],
            send_sem=part_ss,
            recv_sem=part_rs.at[u],
            device_id={"kvp": other, "tp": tp},
            device_id_type=MESH,
        )

    def log_copy(i):
        other = target_of(i)
        return pltpu.make_async_remote_copy(
            src_ref=log_send.at[other],
            dst_ref=log_all.at[kvp],
            send_sem=log_ss,
            recv_sem=log_rs,
            device_id={"kvp": other, "tp": tp},
            device_id_type=MESH,
        )

    outward = list(range(2, groups)) + [1]
    for u in range(parts):
        for i in outward:
            q_copy(i, u).start()
    steps = chunks // 2
    early = len(segments) // 2 + 1
    for segment in range(early):
        load_segment(segment)
    def token(sem, arrives, leaves, device):
        @pl.when(arrives)
        def _():
            pl.semaphore_wait(sem, 1)

        @pl.when(leaves)
        def _():
            greet(sem, device)

    up = functools.partial(token, up_sem, has_below, has_above, above)
    down = functools.partial(token, down_sem, has_above, has_below, below)

    @pl.when(half < halves // 2)
    def _():
        up()
        down()

    @pl.when(half >= halves // 2)
    def _():
        down()
        up()

    q_all[kvp] = q_send[...]
    for copy in small[2:]:
        copy.wait()
    for n in range(count):
        piece = slice(n * share, (n + 1) * share)
        gain_s[n] = jnp.broadcast_to(gain_v[:, piece], (batch, share))
        hid_s[n] = hidden_v[:, piece].astype(F32)
    cache_load.wait()

    scale = float(head_dim + rope) ** (-0.5)
    rows = groups * heads
    position = kvp * ctx + lax.broadcasted_iota(jnp.int32, (rows, ctx), 1)
    lane = lax.broadcasted_iota(jnp.int32, (rows, 128), 1)
    logs_acc = jnp.zeros((rows, 128), F32)
    lengths = len_v[...]
    for u in range(parts):
        landed(q_all.at[pl.ds(0, groups - 1), pl.ds(u * span // 2, span // 2)], q_rs.at[u])
        some = range(u * span, (u + 1) * span)
        for b in some:
            lat = (b % 2) * latent
            rot = base + (b % 2) * rope
            q_lat = q_all[:, b // 2, :, lat : lat + latent].astype(F32).reshape(rows, latent)
            q_rot = q_all[:, b // 2, :, rot : rot + rope].astype(F32).reshape(rows, rope)
            score_s[b] = (
                jnp.dot(q_lat.astype(BF16), cache_v[b, :latent], preferred_element_type=F32)
                + jnp.dot(q_rot.astype(BF16), cache_v[b, latent:], preferred_element_type=F32)
            ) * scale
        for b in some:
            visible = position < lengths[:, b : b + 1]
            masked = jnp.where(visible, score_s[b], F32(-1e30))
            top = jnp.max(masked, axis=1, keepdims=True)
            exps = jnp.where(visible, jnp.exp(masked - top), F32(0.0))
            guarded = jnp.maximum(jnp.sum(exps, axis=1, keepdims=True), 1.0)
            logs_acc = jnp.where(lane == b, top + jnp.log(guarded), logs_acc)
            weight_s[b] = (exps / guarded).astype(BF16)
        for b in some:
            part = lax.dot_general(
                weight_s[b], cache_v[b, :latent], (((1,), (1,)), ((), ())),
                preferred_element_type=F32,
            )
            for g in range(groups):
                part_send[g, b] = part[g * heads : (g + 1) * heads].astype(BF16)
        for i in outward:
            part_copy(i, u).start()
    for g in range(groups):
        log_send[g] = logs_acc[g * heads : (g + 1) * heads]
    for i in outward:
        log_copy(i).start()
    for segment in range(early, len(segments)):
        load_segment(segment)
    part_all[kvp] = part_send[kvp]
    log_all[kvp] = log_send[kvp]
    uv_load.wait()
    landed(big_v.at[:, pl.ds(0, out_rows)], wo_sem)
    landed(log_all.at[pl.ds(0, groups - 1)], log_rs)
    for u in range(parts):
        landed(part_all.at[pl.ds(0, groups - 1), pl.ds(u * span, span)], part_rs.at[u])
    logs = [log_all[g] for g in range(groups)]
    highest = functools.reduce(jnp.maximum, logs)
    overall = highest + jnp.log(sum(jnp.exp(x - highest) for x in logs))
    factors = [jnp.exp(x - overall) for x in logs]
    for b in range(batch):
        olat_s[b] = sum(
            factors[g][:, b : b + 1] * part_all[g, b].astype(F32) for g in range(groups)
        )
    for i in range(heads):
        head_s[:, i * head_dim : (i + 1) * head_dim] = jnp.dot(
            olat_s[:, i, :].astype(BF16), uv_v[i], preferred_element_type=F32
        ).astype(BF16)

    def scatter_sum(lhs, depth, total, send, arrived, ss, rs, after):
        def copy(n, k, z):
            return pltpu.make_async_remote_copy(
                src_ref=send.at[n],
                dst_ref=arrived.at[me],
                send_sem=ss,
                recv_sem=rs,
                device_id={"kvp": k, "tp": z},
                device_id_type=MESH,
            )

        def leave(source, low, high, origin):
            for t in range(low // 2, high // 2):
                k, h = far[t]
                pieces = []
                for n in (2 * t, 2 * t + 1):
                    start = (n - origin) * share
                    pieces.append(source[:, start : start + share])
                    send[n] = pieces[-1].astype(BF16)
                if t < chunks - 1:
                    p = (h - half + halves) // halves
                    copy(2 * t + p, k, 2 * h + p).start()
                    copy(2 * t + 1 - p, k, 2 * h + 1 - p).start()
                else:
                    for p in range(2):
                        @pl.when(lax.rem(tp, 2) != p)
                        def _():
                            copy(2 * t + p, k, 2 * h + p).start()
            return pieces

        held = 2 * groups
        wide = groups * chunk
        for e in range(halves):
            cut = wide if e == halves - 1 else (wide // 2 + 511) // 512 * 512
            done = cut // share // 2 * 2
            first = jnp.dot(lhs, big_v[e, :depth, :cut], preferred_element_type=F32)
            last = leave(first, e * held, e * held + done, e * held)
            if done < held:
                rest = jnp.dot(lhs, big_v[e, :depth, cut:], preferred_element_type=F32)
                rest = jnp.concatenate([first[:, done * share :], rest], axis=1)
                leave(rest, e * held + done, (e + 1) * held, e * held + done)
        for p in range(2):
            total = total + jnp.where(lax.rem(tp, 2) == p, last[p], F32(0.0))
        for s in range(steps):
            after(s)
        landed(arrived.at[pl.ds(0, count - 1)], rs)
        for d in range(1, count):
            total = total + arrived[lax.rem(me + d, count)].astype(F32)
        return total

    def reload(s):
        load_wd(2 * s).start(priority=1)
        load_wd(2 * s + 1).start(priority=1)

    residual = scatter_sum(
        head_s[...], out_rows, hid_s[me], rs_send, rs_all, rs_ss, rs_rs, reload
    )
    own_s[...] = residual
    ag_send[...] = residual.astype(BF16)
    for t in range(1, count):
        k, z = shares[t]
        pltpu.make_async_remote_copy(
            src_ref=ag_send,
            dst_ref=ag_all.at[me],
            send_sem=ag_ss,
            recv_sem=ag_rs.at[0 if t < 2 else 1 if t < groups else 2 + tp],
            device_id={"kvp": k, "tp": z},
            device_id_type=MESH,
        ).start()
    ag_all[me] = ag_send[...]

    square = jnp.zeros((batch, 1), F32)
    even = 2 * hidden_units // 512 * 512
    main = jnp.zeros((batch, even), F32)
    tail = jnp.zeros((batch, 2 * hidden_units - even), F32)
    for segment, (low, high) in enumerate(segments):
        landed(gu_v.at[pl.ds(low * share, (high - low) * share)], gu_sem.at[segment])
        came = high - low - (segment == 0)
        landed(
            ag_all.at[pl.ds(0, came)],
            ag_rs.at[segment if segment < 2 else 2 + planes[segment - 1]],
        )
        x = []
        for k, z in shares[low:high]:
            value = ag_all[k * tps + z].astype(F32)
            square = square + jnp.sum(value * value, axis=1, keepdims=True)
            x.append((value * gain_s[k * tps + z]).astype(BF16))
        main = main + jnp.dot(
            jnp.concatenate(x, axis=1),
            gu_v[low * share : high * share, :even],
            preferred_element_type=F32,
        )
        middle = (low + high) // 2
        for part, a, b in ((x[: middle - low], low, middle), (x[middle - low :], middle, high)):
            tail = tail + jnp.dot(
                jnp.concatenate(part, axis=1),
                gu_v[a * share : b * share, even:],
                preferred_element_type=F32,
            )
    products = jnp.concatenate([main, tail], axis=1)
    products = products * lax.rsqrt(square / width + 1e-06)
    gate, up = products[:, :hidden_units], products[:, hidden_units:]
    act = (gate / (1.0 + jnp.exp(-gate)) * up).astype(BF16)

    for s in range(2):
        landed(big_v.at[pl.ds(s * halves // 2, halves // 2)], wd_sem.at[s])
    total = scatter_sum(
        act, big_v.shape[1], own_s[...], fs_send, fs_all, fs_ss, fs_rs, lambda s: None
    )
    out_ref[...] = total.astype(BF16)

    others = pl.ds(0, groups - 1)
    landed(q_all.at[others], q_ss)
    landed(part_all.at[others], part_ss)
    landed(log_all.at[others], log_ss)
    everyone = pl.ds(0, count - 1)
    landed(rs_all.at[everyone], rs_ss)
    landed(ag_all.at[everyone], ag_ss)
    landed(fs_all.at[everyone], fs_ss)


def per_device(*operands):
    (hidden_in, queries_nope, queries_rope, cache, lengths, w_uk, w_uv, w_out, norm_gain,
     w_gate, w_up, w_down) = operands
    groups, tps = lax.axis_size("kvp"), lax.axis_size("tp")
    count = groups * tps
    batch, heads, head_dim = queries_nope.shape
    latent, rope, ctx = w_uk.shape[2], queries_rope.shape[2], cache.shape[1]
    width = hidden_in.shape[1]
    share = width // count
    ff = w_gate.shape[1]
    rows = w_out.shape[0]
    chunk = 2 * share
    held = (w_gate.size + w_up.size + max(rows, ff) * width + cache.size + w_uk.size + w_uv.size) * 2
    fits = (
        batch % 8 == 0
        and heads % 8 == 0
        and all(size % 128 == 0 for size in (head_dim, latent, 2 * rope, ctx, chunk, ff))
        and groups % 2 == 0
        and tps % 4 == 0
        and batch <= 128
        and rows <= ff
        and held < VMEM_BYTES - 8 * 2**20
    )
    if not fits:
        return plain_device(*operands)
    chunks = width // chunk
    pairs = batch // 2
    parts = batch // SPAN
    dma = pltpu.SemaphoreType.DMA
    vmem = pl.BlockSpec(memory_space=pltpu.VMEM)
    anywhere = pl.BlockSpec(memory_space=pl.ANY)
    packed = 2 * (latent + rope)
    spread = pltpu.VMEM((count, batch, share), BF16)
    scratch = [
        pltpu.VMEM((batch, width), BF16),
        pltpu.VMEM((batch, heads, head_dim), BF16),
        pltpu.VMEM((batch, heads, rope), BF16),
        pltpu.VMEM((1, batch), jnp.int32),
        pltpu.VMEM((1, width + 1024), F32),
        pltpu.VMEM((count, batch, share), F32),
        pltpu.VMEM((count, batch, share), F32),
        pltpu.VMEM((batch, latent + rope, ctx), BF16),
        pltpu.VMEM(w_uk.shape, BF16),
        pltpu.VMEM(w_uv.shape, BF16),
        pltpu.VMEM((tps // 2, ff, groups * chunk), BF16),
        pltpu.VMEM((width, 2 * ff), BF16),
        pltpu.VMEM((batch, heads, head_dim), F32),
        pltpu.VMEM((batch, heads, latent), F32),
        pltpu.VMEM((batch, groups * heads, ctx), F32),
        pltpu.VMEM((batch, groups * heads, ctx), BF16),
        pltpu.VMEM((pairs, heads, packed), BF16),
        pltpu.VMEM((groups, pairs, heads, packed), BF16),
        pltpu.VMEM((groups, batch, heads, latent), BF16),
        pltpu.VMEM((groups, batch, heads, latent), BF16),
        pltpu.VMEM((groups, heads, 128), F32),
        pltpu.VMEM((groups, heads, 128), F32),
        pltpu.VMEM((batch, heads, latent), F32),
        pltpu.VMEM((batch, heads * head_dim), BF16),
        pltpu.VMEM((batch, share), F32),
        spread, spread, pltpu.VMEM((batch, share), BF16), spread, spread, spread,
        dma((5,)), dma, dma, dma,
        dma, dma((tps + 1,)), dma((2,)),
        dma, dma((parts,)), dma, dma((parts,)), dma, dma,
        dma, dma, dma, dma((tps + 2,)), dma, dma,
        pltpu.SemaphoreType.REGULAR, pltpu.SemaphoreType.REGULAR,
    ]
    return pl.pallas_call(
        functools.partial(layer_kernel, groups, tps, share, chunk, rows, SPAN),
        out_shape=pltpu.VMEM((batch, share), BF16),
        in_specs=[anywhere] * 12,
        out_specs=vmem,
        scratch_shapes=scratch,
        compiler_params=pltpu.CompilerParams(
            collective_id=0, has_side_effects=True, vmem_limit_bytes=VMEM_BYTES - 640 * 1024
        ),
    )(
        hidden_in, queries_nope, queries_rope, lengths.reshape(1, batch), norm_gain.reshape(1, width),
        jnp.swapaxes(cache, 1, 2), w_uk, w_uv, w_out, w_gate, w_up, w_down,
    )


def solution(mesh):
    placed = (
        P("grp", None),
        P("grp", ("kvp", "tp"), None),
        P("grp", ("kvp", "tp"), None),
        P("grp", "kvp", None),
        P("grp"),
        P(("kvp", "tp"), None, None),
        P(("kvp", "tp"), None, None),
        P(("kvp", "tp"), None),
        P(),
        P(None, ("kvp", "tp")),
        P(None, ("kvp", "tp")),
        P(("kvp", "tp"), None),
    )
    return jax.shard_map(
        per_device, mesh=mesh, in_specs=placed, out_specs=P("grp", ("kvp", "tp")), check_vma=False
    )
```

```python
import functools
import math

import jax
import jax.numpy as jnp
from jax import lax
from jax.experimental import pallas as pl
from jax.experimental.pallas import tpu as pltpu
from jax.sharding import PartitionSpec as P


def project(o_lat, w_uv, w_out):
    head_out = jnp.einsum("bhl,hle->bhe", o_lat, w_uv, preferred_element_type=jnp.float32).astype(
        jnp.bfloat16
    )
    return jnp.dot(
        head_out.reshape(head_out.shape[0], -1), w_out, preferred_element_type=jnp.float32
    )


def plain_device(
    hidden_in,
    queries_nope,
    queries_rope,
    cache,
    lengths,
    w_uk,
    w_uv,
    w_out,
    norm_gain,
    w_gate,
    w_up,
    w_down,
):
    batch, heads_dev, head_dim = queries_nope.shape
    latent = w_uk.shape[2]
    ctx_dev = cache.shape[1]
    groups = lax.axis_size("kvp")
    score_scale = float(head_dim + queries_rope.shape[2]) ** (-0.5)
    q_lat = jnp.einsum(
        "bhd,hdl->bhl", queries_nope, w_uk, preferred_element_type=jnp.float32
    ).astype(jnp.bfloat16)
    q_lat_all, rope_all = (
        lax.all_gather(q_lat, "kvp", axis=1, tiled=True),
        lax.all_gather(queries_rope, "kvp", axis=1, tiled=True),
    )
    q_full = jnp.concatenate([q_lat_all, rope_all], axis=2)
    scores = (
        jnp.einsum("bhc,btc->bht", q_full, cache, preferred_element_type=jnp.float32) * score_scale
    )
    offset = lax.axis_index("kvp") * ctx_dev
    visible = ((offset + jnp.arange(ctx_dev, dtype=jnp.int32))[None, :] < lengths[:, None])[
        :, None, :
    ]
    masked = jnp.where(visible, scores, jnp.float32(-1e30))
    block_max = jnp.max(masked, axis=2)
    exponent = jnp.where(visible, jnp.exp(masked - block_max[..., None]), jnp.float32(0.0))
    guarded = jnp.maximum(jnp.sum(exponent, axis=2), 1.0)
    log_total = block_max + jnp.log(guarded)
    weights = (exponent / guarded[..., None]).astype(jnp.bfloat16)
    partial_value = jnp.einsum("bht,btc->bhc", weights, cache, preferred_element_type=jnp.float32)[
        ..., :latent
    ]
    blocks = partial_value.reshape(batch, groups, heads_dev, latent)
    block_logs = log_total.reshape(batch, groups, heads_dev)
    part_blocks = lax.all_to_all(
        blocks.astype(jnp.bfloat16), "kvp", split_axis=1, concat_axis=1, tiled=True
    ).astype(blocks.dtype)
    part_logs = lax.all_to_all(block_logs, "kvp", split_axis=1, concat_axis=1, tiled=True)
    highest = jnp.max(part_logs, axis=1)
    overall = highest + jnp.log(jnp.sum(jnp.exp(part_logs - highest[:, None, :]), axis=1))
    scaled = jnp.exp(part_logs - overall[:, None, :])[..., None] * part_blocks
    o_lat = jnp.sum(scaled, axis=1).astype(jnp.bfloat16)
    attention = project(o_lat, w_uv, w_out)
    model_width = norm_gain.shape[0]
    share_width = model_width // lax.axis_size(("kvp", "tp"))
    share_start = lax.axis_index(("kvp", "tp")) * share_width
    attn_whole = lax.psum(attention, ("kvp", "tp"))
    residual = hidden_in.astype(jnp.float32) + attn_whole
    mean_square = jnp.mean(residual * residual, axis=1)
    normed = (residual * lax.rsqrt(mean_square + 1e-06)[:, None] * norm_gain[None, :]).astype(
        jnp.bfloat16
    )
    residual_share = lax.dynamic_slice_in_dim(residual, share_start, share_width, 1)
    gate_proj = jnp.dot(normed, w_gate, preferred_element_type=jnp.float32)
    up_proj = jnp.dot(normed, w_up, preferred_element_type=jnp.float32)
    act = (jax.nn.silu(gate_proj) * up_proj).astype(jnp.bfloat16)
    ffn_terms = jnp.dot(act, w_down, preferred_element_type=jnp.float32)
    ffn_share = lax.psum_scatter(ffn_terms, ("kvp", "tp"), scatter_dimension=1, tiled=True)
    return (residual_share + ffn_share).astype(jnp.bfloat16)


MESH = pl.DeviceIdType.MESH
F32 = jnp.float32
BF16 = jnp.bfloat16
VMEM_BYTES = 67043328


SPAN = 2


def layer_kernel(
    groups, tps, share, chunk, out_rows, span,
    hidden_hbm, nope_hbm, rope_hbm, len_hbm, gain_hbm,
    cache_hbm, uk_hbm, uv_hbm, wo_hbm, wg_hbm, wu_hbm, wd_hbm,
    out_ref,
    hidden_v, nope_v, rope_v, len_v, gain_v, gain_s, hid_s,
    cache_v, uk_v, uv_v, big_v, gu_v,
    nope_s, qlat_s, score_s, weight_s, q_send, q_all, part_send, part_all, log_send, log_all,
    olat_s, head_s, own_s, rs_send, rs_all, ag_send, ag_all, fs_send, fs_all,
    in_sem, uk_sem, cache_sem, uv_sem, wo_sem, gu_sem, wd_sem,
    q_ss, q_rs, part_ss, part_rs, log_ss, log_rs, rs_ss, rs_rs, ag_ss, ag_rs, fs_ss, fs_rs, up_sem, down_sem,
):
    count = groups * tps
    kvp = lax.axis_index("kvp")
    tp = lax.axis_index("tp")
    me = kvp * tps + tp
    batch, heads, head_dim = nope_v.shape
    latent = uk_v.shape[2]
    rope = rope_v.shape[2]
    ctx = cache_v.shape[2]
    width = hidden_v.shape[1]
    chunks = width // chunk
    hidden_units = gu_v.shape[1] // 2
    parts = batch // span
    halves = tps // 2
    half = tp // 2
    chips = groups // 2

    def peer(index):
        return {"kvp": index // tps, "tp": lax.rem(index, tps)}

    def target_of(i):
        return lax.rem(kvp // 2 + i // 2, chips) * 2 + lax.rem(kvp + i, 2)

    near = [
        (target_of(i), lax.rem(half + e, halves)) for e in range(halves) for i in range(groups)
    ]
    far = near[::-1]
    planes = [tp, tp + 1 - 2 * lax.rem(tp, 2)]
    for e in range(1, halves):
        h = lax.rem(half + e, halves)
        p = (half - h + halves - 1) // halves
        planes += [2 * h + p, 2 * h + 1 - p]
    shares = [(target_of(i), z) for z in planes for i in range(groups)]
    bounds = [0, 2] + list(range(groups, count + 1, groups))
    segments = list(zip(bounds[:-1], bounds[1:]))

    def load(source, target, sem):
        return pltpu.make_async_copy(source, target, sem)

    def cols(j):
        return pl.ds(pl.multiple_of(j * chunk, 128), chunk)

    def side(t):
        return pl.ds((t % groups) * chunk, chunk)

    def load_wo(t):
        k, h = far[t]
        return load(
            wo_hbm.at[:, cols(k * halves + h)],
            big_v.at[t // groups, pl.ds(0, out_rows), side(t)],
            wo_sem,
        )

    def load_wd(t):
        k, h = far[t]
        return load(wd_hbm.at[:, cols(k * halves + h)], big_v.at[t // groups, :, side(t)], wd_sem.at[2 * t // chunks])

    def load_gu(n, t, segment):
        k, z = shares[t]
        rows = pl.ds(pl.multiple_of((k * tps + z) * share, math.gcd(share, 128)), share)
        return load(
            (wg_hbm, wu_hbm)[n].at[rows],
            gu_v.at[pl.ds(t * share, share), pl.ds(n * hidden_units, hidden_units)],
            gu_sem.at[segment],
        )

    def landed(ref, sem):
        pltpu.make_async_copy(ref, ref, sem).wait()

    def load_segment(segment):
        for t in range(*segments[segment]):
            load_gu(0, t, segment).start(priority=1)
            load_gu(1, t, segment).start(priority=1)

    small = [
        load(nope_hbm, nope_v, in_sem.at[0]),
        load(rope_hbm, rope_v, in_sem.at[1]),
        load(len_hbm, len_v, in_sem.at[2]),
        load(hidden_hbm, hidden_v, in_sem.at[3]),
        load(gain_hbm, gain_v.at[:, pl.ds(0, width)], in_sem.at[4]),
    ]
    uk_load = load(uk_hbm, uk_v, uk_sem)
    cache_load = load(cache_hbm, cache_v, cache_sem)
    uv_load = load(uv_hbm, uv_v, uv_sem)

    barrier = pltpu.get_barrier_semaphore()
    small[0].start()
    uk_load.start()
    small[1].start()

    below = {"kvp": kvp, "tp": lax.rem(tp + tps - 1, tps)}
    above = {"kvp": kvp, "tp": lax.rem(tp + 1, tps)}
    has_below, has_above = tp > 0, tp < tps - 1

    def greet(sem, device):
        pl.semaphore_signal(sem, inc=1, device_id=device, device_id_type=MESH)

    for i in range(1, groups):
        greet(barrier, {"kvp": target_of(i), "tp": tp})

    @pl.when(has_below)
    def _():
        greet(barrier, below)

    @pl.when(has_above)
    def _():
        greet(barrier, above)

    cache_load.start()
    for copy in small[2:]:
        copy.start()

    small[0].wait()
    nope_s[...] = nope_v[...].astype(F32)
    small[1].wait()
    base = 2 * latent
    for b in range(batch):
        first = base + (b % 2) * rope
        q_send[b // 2, :, first : first + rope] = rope_v[b]
    uk_load.wait()
    uv_load.start()
    for t in range(chunks):
        load_wo(t).start()
    for i in range(heads):
        qlat_s[:, i, :] = jnp.dot(
            nope_s[:, i, :].astype(BF16), uk_v[i], preferred_element_type=F32
        )
    for b in range(batch):
        first = (b % 2) * latent
        q_send[b // 2, :, first : first + latent] = qlat_s[b].astype(BF16)
    edges = (tps - tp - 1) // (tps - 1) + tp // (tps - 1)
    pl.semaphore_wait(barrier, groups + 1 - edges)

    def q_copy(i, u):
        other = target_of(i)
        return pltpu.make_async_remote_copy(
            src_ref=q_send.at[pl.ds(u * span // 2, span // 2)],
            dst_ref=q_all.at[kvp, pl.ds(u * span // 2, span // 2)],
            send_sem=q_ss,
            recv_sem=q_rs.at[u],
            device_id={"kvp": other, "tp": tp},
            device_id_type=MESH,
        )

    def part_copy(i, u):
        other = target_of(i)
        some = pl.ds(u * span, span)
        return pltpu.make_async_remote_copy(
            src_ref=part_send.at[other, some],
            dst_ref=part_all.at[kvp, some],
            send_sem=part_ss,
            recv_sem=part_rs.at[u],
            device_id={"kvp": other, "tp": tp},
            device_id_type=MESH,
        )

    def log_copy(i):
        other = target_of(i)
        return pltpu.make_async_remote_copy(
            src_ref=log_send.at[other],
            dst_ref=log_all.at[kvp],
            send_sem=log_ss,
            recv_sem=log_rs,
            device_id={"kvp": other, "tp": tp},
            device_id_type=MESH,
        )

    outward = list(range(2, groups)) + [1]
    for u in range(parts):
        for i in outward:
            q_copy(i, u).start()
    steps = chunks // 2
    early = len(segments) // 2 + 1
    for segment in range(early):
        load_segment(segment)
    def token(sem, arrives, leaves, device):
        @pl.when(arrives)
        def _():
            pl.semaphore_wait(sem, 1)

        @pl.when(leaves)
        def _():
            greet(sem, device)

    up = functools.partial(token, up_sem, has_below, has_above, above)
    down = functools.partial(token, down_sem, has_above, has_below, below)

    @pl.when(half < halves // 2)
    def _():
        up()
        down()

    @pl.when(half >= halves // 2)
    def _():
        down()
        up()

    q_all[kvp] = q_send[...]
    for copy in small[2:]:
        copy.wait()
    for n in range(count):
        piece = slice(n * share, (n + 1) * share)
        gain_s[n] = jnp.broadcast_to(gain_v[:, piece], (batch, share))
        hid_s[n] = hidden_v[:, piece].astype(F32)
    cache_load.wait()

    scale = float(head_dim + rope) ** (-0.5)
    rows = groups * heads
    position = kvp * ctx + lax.broadcasted_iota(jnp.int32, (rows, ctx), 1)
    lane = lax.broadcasted_iota(jnp.int32, (rows, 128), 1)
    logs_acc = jnp.zeros((rows, 128), F32)
    lengths = len_v[...]
    for u in range(parts):
        landed(q_all.at[pl.ds(0, groups - 1), pl.ds(u * span // 2, span // 2)], q_rs.at[u])
        some = range(u * span, (u + 1) * span)
        for b in some:
            lat = (b % 2) * latent
            rot = base + (b % 2) * rope
            q_lat = q_all[:, b // 2, :, lat : lat + latent].astype(F32).reshape(rows, latent)
            q_rot = q_all[:, b // 2, :, rot : rot + rope].astype(F32).reshape(rows, rope)
            score_s[b] = (
                jnp.dot(q_lat.astype(BF16), cache_v[b, :latent], preferred_element_type=F32)
                + jnp.dot(q_rot.astype(BF16), cache_v[b, latent:], preferred_element_type=F32)
            ) * scale
        for b in some:
            visible = position < lengths[:, b : b + 1]
            masked = jnp.where(visible, score_s[b], F32(-1e30))
            top = jnp.max(masked, axis=1, keepdims=True)
            exps = jnp.where(visible, jnp.exp(masked - top), F32(0.0))
            guarded = jnp.maximum(jnp.sum(exps, axis=1, keepdims=True), 1.0)
            logs_acc = jnp.where(lane == b, top + jnp.log(guarded), logs_acc)
            weight_s[b] = (exps / guarded).astype(BF16)
        for b in some:
            part = lax.dot_general(
                weight_s[b], cache_v[b, :latent], (((1,), (1,)), ((), ())),
                preferred_element_type=F32,
            )
            for g in range(groups):
                part_send[g, b] = part[g * heads : (g + 1) * heads].astype(BF16)
        for i in outward:
            part_copy(i, u).start()
    for g in range(groups):
        log_send[g] = logs_acc[g * heads : (g + 1) * heads]
    for i in outward:
        log_copy(i).start()
    for segment in range(early, len(segments)):
        load_segment(segment)
    part_all[kvp] = part_send[kvp]
    log_all[kvp] = log_send[kvp]
    uv_load.wait()
    landed(big_v.at[:, pl.ds(0, out_rows)], wo_sem)
    landed(log_all.at[pl.ds(0, groups - 1)], log_rs)
    for u in range(parts):
        landed(part_all.at[pl.ds(0, groups - 1), pl.ds(u * span, span)], part_rs.at[u])
    logs = [log_all[g] for g in range(groups)]
    highest = functools.reduce(jnp.maximum, logs)
    overall = highest + jnp.log(sum(jnp.exp(x - highest) for x in logs))
    factors = [jnp.exp(x - overall) for x in logs]
    for b in range(batch):
        olat_s[b] = sum(
            factors[g][:, b : b + 1] * part_all[g, b].astype(F32) for g in range(groups)
        )
    for i in range(heads):
        head_s[:, i * head_dim : (i + 1) * head_dim] = jnp.dot(
            olat_s[:, i, :].astype(BF16), uv_v[i], preferred_element_type=F32
        ).astype(BF16)

    def scatter_sum(lhs, depth, total, send, arrived, ss, rs, after):
        def copy(n, k, z):
            return pltpu.make_async_remote_copy(
                src_ref=send.at[n],
                dst_ref=arrived.at[me],
                send_sem=ss,
                recv_sem=rs,
                device_id={"kvp": k, "tp": z},
                device_id_type=MESH,
            )

        def leave(source, low, high, origin):
            for t in range(low // 2, high // 2):
                k, h = far[t]
                pieces = []
                for n in (2 * t, 2 * t + 1):
                    start = (n - origin) * share
                    pieces.append(source[:, start : start + share])
                    send[n] = pieces[-1].astype(BF16)
                if t < chunks - 1:
                    p = (h - half + halves) // halves
                    copy(2 * t + p, k, 2 * h + p).start()
                    copy(2 * t + 1 - p, k, 2 * h + 1 - p).start()
                else:
                    for p in range(2):
                        @pl.when(lax.rem(tp, 2) != p)
                        def _():
                            copy(2 * t + p, k, 2 * h + p).start()
            return pieces

        held = 2 * groups
        wide = groups * chunk
        for e in range(halves):
            cut = wide if e == halves - 1 else (wide // 2 + 511) // 512 * 512
            done = cut // share // 2 * 2
            first = jnp.dot(lhs, big_v[e, :depth, :cut], preferred_element_type=F32)
            last = leave(first, e * held, e * held + done, e * held)
            if done < held:
                rest = jnp.dot(lhs, big_v[e, :depth, cut:], preferred_element_type=F32)
                rest = jnp.concatenate([first[:, done * share :], rest], axis=1)
                leave(rest, e * held + done, (e + 1) * held, e * held + done)
        for p in range(2):
            total = total + jnp.where(lax.rem(tp, 2) == p, last[p], F32(0.0))
        for s in range(steps):
            after(s)
        landed(arrived.at[pl.ds(0, count - 1)], rs)
        for d in range(1, count):
            total = total + arrived[lax.rem(me + d, count)].astype(F32)
        return total

    def reload(s):
        load_wd(2 * s).start(priority=1)
        load_wd(2 * s + 1).start(priority=1)

    residual = scatter_sum(
        head_s[...], out_rows, hid_s[me], rs_send, rs_all, rs_ss, rs_rs, reload
    )
    own_s[...] = residual
    ag_send[...] = residual.astype(BF16)
    for t in range(1, count):
        k, z = shares[t]
        pltpu.make_async_remote_copy(
            src_ref=ag_send,
            dst_ref=ag_all.at[me],
            send_sem=ag_ss,
            recv_sem=ag_rs.at[0 if t < 2 else 1 if t < groups else 2 + tp],
            device_id={"kvp": k, "tp": z},
            device_id_type=MESH,
        ).start()
    ag_all[me] = ag_send[...]

    square = jnp.zeros((batch, 1), F32)
    gate = jnp.zeros((batch, hidden_units), F32)
    up = jnp.zeros((batch, hidden_units), F32)
    for segment, (low, high) in enumerate(segments):
        landed(gu_v.at[pl.ds(low * share, (high - low) * share)], gu_sem.at[segment])
        came = high - low - (segment == 0)
        landed(
            ag_all.at[pl.ds(0, came)],
            ag_rs.at[segment if segment < 2 else 2 + planes[segment - 1]],
        )
        x = []
        for k, z in shares[low:high]:
            value = ag_all[k * tps + z].astype(F32)
            square = square + jnp.sum(value * value, axis=1, keepdims=True)
            x.append((value * gain_s[k * tps + z]).astype(BF16))
        x = jnp.concatenate(x, axis=1)
        rows_used = slice(low * share, high * share)
        gate = gate + jnp.dot(x, gu_v[rows_used, :hidden_units], preferred_element_type=F32)
        up = up + jnp.dot(x, gu_v[rows_used, hidden_units:], preferred_element_type=F32)
    products = jnp.concatenate([gate, up], axis=1)
    products = products * lax.rsqrt(square / width + 1e-06)
    gate, up = products[:, :hidden_units], products[:, hidden_units:]
    act = (gate / (1.0 + jnp.exp(-gate)) * up).astype(BF16)

    for s in range(2):
        landed(big_v.at[pl.ds(s * halves // 2, halves // 2)], wd_sem.at[s])
    total = scatter_sum(
        act, big_v.shape[1], own_s[...], fs_send, fs_all, fs_ss, fs_rs, lambda s: None
    )
    out_ref[...] = total.astype(BF16)

    others = pl.ds(0, groups - 1)
    landed(q_all.at[others], q_ss)
    landed(part_all.at[others], part_ss)
    landed(log_all.at[others], log_ss)
    everyone = pl.ds(0, count - 1)
    landed(rs_all.at[everyone], rs_ss)
    landed(ag_all.at[everyone], ag_ss)
    landed(fs_all.at[everyone], fs_ss)


def per_device(*operands):
    (hidden_in, queries_nope, queries_rope, cache, lengths, w_uk, w_uv, w_out, norm_gain,
     w_gate, w_up, w_down) = operands
    groups, tps = lax.axis_size("kvp"), lax.axis_size("tp")
    count = groups * tps
    batch, heads, head_dim = queries_nope.shape
    latent, rope, ctx = w_uk.shape[2], queries_rope.shape[2], cache.shape[1]
    width = hidden_in.shape[1]
    share = width // count
    ff = w_gate.shape[1]
    rows = w_out.shape[0]
    chunk = 2 * share
    held = (w_gate.size + w_up.size + max(rows, ff) * width + cache.size + w_uk.size + w_uv.size) * 2
    fits = (
        batch % 8 == 0
        and heads % 8 == 0
        and all(size % 128 == 0 for size in (head_dim, latent, 2 * rope, ctx, chunk, ff))
        and groups % 2 == 0
        and tps % 4 == 0
        and batch <= 128
        and rows <= ff
        and held < VMEM_BYTES - 8 * 2**20
    )
    if not fits:
        return plain_device(*operands)
    chunks = width // chunk
    pairs = batch // 2
    parts = batch // SPAN
    dma = pltpu.SemaphoreType.DMA
    vmem = pl.BlockSpec(memory_space=pltpu.VMEM)
    anywhere = pl.BlockSpec(memory_space=pl.ANY)
    packed = 2 * (latent + rope)
    spread = pltpu.VMEM((count, batch, share), BF16)
    scratch = [
        pltpu.VMEM((batch, width), BF16),
        pltpu.VMEM((batch, heads, head_dim), BF16),
        pltpu.VMEM((batch, heads, rope), BF16),
        pltpu.VMEM((1, batch), jnp.int32),
        pltpu.VMEM((1, width + 1024), F32),
        pltpu.VMEM((count, batch, share), F32),
        pltpu.VMEM((count, batch, share), F32),
        pltpu.VMEM((batch, latent + rope, ctx), BF16),
        pltpu.VMEM(w_uk.shape, BF16),
        pltpu.VMEM(w_uv.shape, BF16),
        pltpu.VMEM((tps // 2, ff, groups * chunk), BF16),
        pltpu.VMEM((width, 2 * ff), BF16),
        pltpu.VMEM((batch, heads, head_dim), F32),
        pltpu.VMEM((batch, heads, latent), F32),
        pltpu.VMEM((batch, groups * heads, ctx), F32),
        pltpu.VMEM((batch, groups * heads, ctx), BF16),
        pltpu.VMEM((pairs, heads, packed), BF16),
        pltpu.VMEM((groups, pairs, heads, packed), BF16),
        pltpu.VMEM((groups, batch, heads, latent), BF16),
        pltpu.VMEM((groups, batch, heads, latent), BF16),
        pltpu.VMEM((groups, heads, 128), F32),
        pltpu.VMEM((groups, heads, 128), F32),
        pltpu.VMEM((batch, heads, latent), F32),
        pltpu.VMEM((batch, heads * head_dim), BF16),
        pltpu.VMEM((batch, share), F32),
        spread, spread, pltpu.VMEM((batch, share), BF16), spread, spread, spread,
        dma((5,)), dma, dma, dma,
        dma, dma((tps + 1,)), dma((2,)),
        dma, dma((parts,)), dma, dma((parts,)), dma, dma,
        dma, dma, dma, dma((tps + 2,)), dma, dma,
        pltpu.SemaphoreType.REGULAR, pltpu.SemaphoreType.REGULAR,
    ]
    return pl.pallas_call(
        functools.partial(layer_kernel, groups, tps, share, chunk, rows, SPAN),
        out_shape=pltpu.VMEM((batch, share), BF16),
        in_specs=[anywhere] * 12,
        out_specs=vmem,
        scratch_shapes=scratch,
        compiler_params=pltpu.CompilerParams(
            collective_id=0, has_side_effects=True, vmem_limit_bytes=VMEM_BYTES - 640 * 1024
        ),
    )(
        hidden_in, queries_nope, queries_rope, lengths.reshape(1, batch), norm_gain.reshape(1, width),
        jnp.swapaxes(cache, 1, 2), w_uk, w_uv, w_out, w_gate, w_up, w_down,
    )


def solution(mesh):
    placed = (
        P("grp", None),
        P("grp", ("kvp", "tp"), None),
        P("grp", ("kvp", "tp"), None),
        P("grp", "kvp", None),
        P("grp"),
        P(("kvp", "tp"), None, None),
        P(("kvp", "tp"), None, None),
        P(("kvp", "tp"), None),
        P(),
        P(None, ("kvp", "tp")),
        P(None, ("kvp", "tp")),
        P(("kvp", "tp"), None),
    )
    return jax.shard_map(
        per_device, mesh=mesh, in_specs=placed, out_specs=P("grp", ("kvp", "tp")), check_vma=False
    )
```
